32 devices in a mesh: boxes: 32 (over z, y, x, core).
Axes of the slice: x: 2, y: 2, z: 4, core: 2. Of those that a mesh axis runs over, the one named last changes fastest.
Arguments:
- conserved: float32 [32, 5, 16, 32, 128], P('boxes'), may hold values from -6 to 6
- volume_fraction: float32 [32, 16, 32, 128], P('boxes'), may hold values from 0.05 to 1
- cut_mask: int32 [32, 16, 32, 128], P('boxes'), may hold values 0 or 1
- merge_code: int32 [32, 16, 32, 128], P('boxes'), may hold values from 0 to 26
Outputs:
- redistributed: float32 [32, 5, 16, 32, 128], P('boxes')
The draws below stay inside these ranges and needn't reach their ends.
All inputs are finite; a program needn't handle non-finite values. No bound on the sum of `cut_mask` on one device may be relied on, other than what follows from the above.
Results may differ from the reference program's by a relative error of at most 0.0003.
Values sent between devices are 32-bit elements; how exact they have to be, the bound alone decides.
A program may use at most 64 MiB of HBM per device.

```python
import math
import jax
import jax.numpy as jnp
from jax import lax

FIELDS = 5
CX = 16
CY = 32
CZ = 128
NBY = 4
NBZ = 4
NBOXES = 32
NBX = 2
NX = 32
NY = 128
NZ = 512


def plant(array, stream_key, least, high):
    shape = array.shape
    spot = [jax.random.randint(jax.random.fold_in(stream_key, axis), (), 0, shape[axis]) for axis in range(len(shape))]
    array = array.at[tuple(spot)].set(least)
    longest = shape.index(max(shape))
    spot[longest] = (spot[longest] + 1) % shape[longest]
    return array.at[tuple(spot)].set(high)


def levels(key, dims, split, least, high):
    loudness, own = 1.0, jax.random.fold_in(key, 6)
    for dim, parts in split:
        steps = jnp.exp(jax.random.uniform(jax.random.fold_in(own, dim), (parts,), jnp.float32, least / len(split), high / len(split)))
        loudness = loudness * jnp.repeat(steps, dims[dim] // parts).reshape([-1 if axis == dim else 1 for axis in range(len(dims))])
    return loudness


def bell_draw(key, shape, width, limit, cuts=(), held_as=jnp.bfloat16):
    gain = levels(key, shape, cuts, -0.22, 0.18) if cuts else 1.0
    array = jax.random.normal(key, shape, jnp.float32) * width * gain
    return jnp.minimum(jnp.maximum(array, -limit), limit).astype(held_as)


def setup_inputs(seed: int = 0) -> dict:
    arg_keys = jax.random.split(jax.random.key(seed), 5)
    return {
        "conserved": bell_draw(arg_keys[0], (NBOXES, FIELDS, CX, CY, CZ), 1.0, 6.0, ((0, 32),), jnp.float32),
        "volume_fraction": jnp.clip(jnp.exp(math.log(1.0) - 2.9957323 * jax.random.uniform(arg_keys[1], (NBOXES, CX, CY, CZ), jnp.float32) ** levels(arg_keys[1], (NBOXES, CX, CY, CZ), ((0, 32),), -0.2, 0.2)), 0.05, 1.0),
        "cut_mask": plant((jax.random.randint(arg_keys[2], (NBOXES, CX, CY, CZ), 0, 2) < 1).astype(jnp.int32), jax.random.fold_in(arg_keys[2], 1), 0, 1),
        "merge_code": plant(jax.random.randint(arg_keys[3], (NBOXES, CX, CY, CZ), 0, 27), jax.random.fold_in(arg_keys[3], 1), 0, 26).astype(jnp.int32),
    }


OFFSETS = [(first, second, third) for first in (-1, 0, 1) for second in (-1, 0, 1) for third in (-1, 0, 1) if (first, second, third) != (0, 0, 0)]


def decode(code_field):
    sign_parts = (code_field // 9 - 1, (code_field // 3) % 3 - 1, code_field % 3 - 1)
    members = []
    for offset in OFFSETS:
        inside = jnp.ones(code_field.shape, jnp.bool_)
        for direction, component in zip(sign_parts, offset):
            if component != 0:
                inside = inside & (direction == component)
        members.append(inside)
    return members


def placed(values, offset):
    spread = [(0, 0)] * (values.ndim - 3) + [(1 + component, 1 - component) for component in offset]
    return jnp.pad(values, spread)


def count_members(members):
    running = placed(jnp.ones(members[0].shape, jnp.float32), (0, 0, 0))
    for offset, inside in zip(OFFSETS, members):
        running = running + placed(inside.astype(jnp.float32), offset)
    return running


def window(weighted, offset, interior):
    starts = [0] + [1 + component for component in offset]
    limits = [weighted.shape[0]] + [anchor + extent for anchor, extent in zip(starts[1:], interior)]
    return lax.slice(weighted, starts, limits)


def neighbour_average(weighted, members):
    interior = [extent - 2 for extent in weighted.shape[1:]]
    running = window(weighted, (0, 0, 0), interior)
    for offset, inside in zip(OFFSETS, members):
        running = running + jnp.where(inside[None], window(weighted, offset, interior), 0.0)
    return running[1:] / running[0:1]


def spread_back(average, members):
    running = placed(average, (0, 0, 0))
    for offset, inside in zip(OFFSETS, members):
        running = running + placed(jnp.where(inside[None], average, 0.0), offset)
    return running


def to_grid(boxed):
    channels = boxed.shape[1]
    shaped = boxed.reshape(NBX, NBY, NBZ, channels, CX, CY, CZ)
    return shaped.transpose(3, 0, 4, 1, 5, 2, 6).reshape(channels, NX, NY, NZ)


def from_grid(gridded):
    channels = gridded.shape[0]
    shaped = gridded.reshape(channels, NBX, CX, NBY, CY, NBZ, CZ)
    return shaped.transpose(1, 3, 5, 0, 2, 4, 6).reshape(NBOXES, channels, CX, CY, CZ)


def reference(conserved, volume_fraction, cut_mask, merge_code):
    fields = to_grid(conserved)
    fraction = to_grid(volume_fraction[:, None])[0]
    code_field = jnp.where(to_grid(cut_mask[:, None])[0] == 1, to_grid(merge_code[:, None])[0], 13)
    members = decode(code_field)
    counts = count_members(members)[1:-1, 1:-1, 1:-1]
    weight = fraction / counts
    weighted = jnp.concatenate([weight[None], weight[None] * fields], axis=0)
    weighted = jnp.pad(weighted, ((0, 0), (1, 1), (1, 1), (1, 1)))
    average = neighbour_average(weighted, members)
    gathered = spread_back(average, members)[:, 1:-1, 1:-1, 1:-1]
    return from_grid(gathered / counts[None])
```

```python
import functools

import jax
import jax.numpy as jnp
from jax import lax
from jax.experimental import pallas as pl
from jax.experimental.pallas import tpu as pltpu
from jax.sharding import PartitionSpec as P

NBY = 4
NBZ = 4
MESH = pl.DeviceIdType.MESH
XP, XM, YP, YM, ZP, ZM = 1, 2, 4, 8, 16, 32
ONE, UP, DOWN = 10, 14, 18
PX, PY = 2, 8


def flag(ax, ay, az):
    return (
        {1: XP, -1: XM, 0: 0}[ax] | {1: YP, -1: YM, 0: 0}[ay] | {1: ZP, -1: ZM, 0: 0}[az]
    )


def holds(e, bits):
    return (e & bits) == bits


def kernel(n, dims, u_ref, vf_ref, mask_ref, code_ref, out_ref, ext_e, ext_f, cnt, w0, wp, wm, avg,
           raw_m, raw_c, ys_e, ys_f, yr_e, yr_f, cr_e, cr_f, zs, zr, load_sem, send_sem, recv_sem):
    fields, cx, cy, cz = dims
    chans = fields + 1
    me = lax.axis_index("boxes")
    bx, by, bz = me // (NBY * NBZ), me // NBZ % NBY, me % NBZ
    axes = {
        "x": (NBY * NBZ, bx > 0, bx < n // (NBY * NBZ) - 1),
        "y": (NBZ, by > 0, by < NBY - 1),
        "z": (1, bz > 0, bz < NBZ - 1),
    }
    lane = lax.broadcasted_iota(jnp.int32, (8, cz), 1)
    nyb = (cy + 8) // 8

    loads = [
        pltpu.make_async_copy(mask_ref.at[0], raw_m, load_sem.at[0]),
        pltpu.make_async_copy(code_ref.at[0], raw_c, load_sem.at[1]),
        pltpu.make_async_copy(vf_ref.at[0], ext_f.at[0, PX:PX + cx, PY:PY + cy], load_sem.at[2]),
        pltpu.make_async_copy(u_ref.at[0], ext_f.at[1:chans, PX:PX + cx, PY:PY + cy], load_sem.at[3]),
    ]
    for copy in loads:
        copy.start()

    barrier = pltpu.get_barrier_semaphore()
    total = jnp.int32(0)
    for stride, low, high in axes.values():
        for has, there in ((low, me - stride), (high, me + stride)):
            @pl.when(has)
            def _():
                pl.semaphore_signal(barrier, inc=1, device_id=(there,), device_id_type=MESH)
            total = total + has.astype(jnp.int32)
    pl.semaphore_wait(barrier, total)

    def copies(axis, ident, up, down):
        stride = axes[axis][0]
        out = []
        for d, (pair, there) in enumerate(((up, me + stride), (down, me - stride))):
            out.append(pltpu.make_async_remote_copy(
                src_ref=pair[0], dst_ref=pair[1], send_sem=send_sem.at[2 * ident + d],
                recv_sem=recv_sem.at[2 * ident + d], device_id=(there,), device_id_type=MESH))
        return axis, out

    def start(c):
        axis, (up, down) = c
        _, low, high = axes[axis]
        pl.when(high)(lambda: up.start())
        pl.when(low)(lambda: down.start())

    def recv(c):
        axis, (up, down) = c
        _, low, high = axes[axis]
        pl.when(low)(lambda: up.wait_recv())
        pl.when(high)(lambda: down.wait_recv())

    def sent(c):
        axis, (up, down) = c
        _, low, high = axes[axis]
        pl.when(high)(lambda: up.wait_send())
        pl.when(low)(lambda: down.wait_send())

    def x_face(ident, ref, lead, depth):
        box = slice(PY, PY + cy)
        at = lambda a, b: ref.at[lead + (slice(a, b), box)]
        end = PX + cx
        return copies("x", ident, (at(end - depth, end), at(PX - depth, PX)),
                      (at(PX, PX + depth), at(end, end + depth)))

    x_e = x_face(0, ext_e, (), 2)
    x_vf = x_face(1, ext_f, (slice(0, 1),), 1)
    x_u = x_face(2, ext_f, (slice(1, chans),), 1)
    y_e = copies("y", 3, (ys_e.at[0], yr_e.at[0]), (ys_e.at[1], yr_e.at[1]))
    y_f = copies("y", 4, (ys_f.at[0], yr_f.at[0]), (ys_f.at[1], yr_f.at[1]))
    c_e = copies("x", 5, (yr_e.at[:, cx - 2:cx], cr_e.at[0]), (yr_e.at[:, 0:2], cr_e.at[1]))
    c_f = copies("x", 6, (yr_f.at[:, :, cx - 1:cx], cr_f.at[0]), (yr_f.at[:, :, 0:1], cr_f.at[1]))
    last = 1 + 2 * chans
    spans = ((0, 1), (1, 1 + chans), (1 + chans, last), (last, last + fields))
    z_c = [copies("z", 7 + i, (zs.at[0, a:b], zr.at[0, a:b]), (zs.at[1, a:b], zr.at[1, a:b]))
           for i, (a, b) in enumerate(spans)]
    everything = [x_e, x_vf, x_u, y_e, y_f, c_e, c_f] + z_c

    loads[2].wait()
    loads[3].wait()
    start(x_vf)
    start(x_u)
    loads[0].wait()
    loads[1].wait()

    def encode(p, _):
        c = raw_c[p]
        cut = raw_m[p] == 1
        third = (c * 171) >> 9
        sz = c - 3 * third
        ninth = (third * 171) >> 9
        sy = third - 3 * ninth
        bit = lambda test, value: jnp.where(test, value, 0)
        e = (bit(ninth == 2, XP) + bit(ninth == 0, XM) + bit(sy == 2, YP) + bit(sy == 0, YM)
             + bit(sz == 2, ZP + (1 << UP)) + bit(sz == 0, ZM + (1 << DOWN)))
        ext_e[PX + p, PY:PY + cy, :] = jnp.where(cut, e, 0) + (1 << ONE)
        return 0

    lax.fori_loop(0, cx, encode, 0)
    start(x_e)
    ys_e[0] = ext_e[PX:PX + cx, PY + cy - 2:PY + cy, :]
    ys_e[1] = ext_e[PX:PX + cx, PY:PY + 2, :]
    start(y_e)
    for c in range(chans):
        ys_f[0, c] = ext_f[c, PX:PX + cx, PY + cy - 1:PY + cy, :]
        ys_f[1, c] = ext_f[c, PX:PX + cx, PY:PY + 1, :]
    start(y_f)

    end = PX + cx
    _, low, high = axes["x"]
    for has, (e0, e1), (f0, f1) in ((low, (0, 2), (1, 2)), (high, (end, end + 2), (end, end + 1))):
        @pl.when(jnp.logical_not(has))
        def _():
            ext_e[e0:e1, :, :] = jnp.full((e1 - e0,) + ext_e.shape[1:], 1 << ONE, jnp.int32)
            for c in range(chans):
                ext_f[c, f0:f1, :, :] = jnp.zeros((f1 - f0,) + ext_f.shape[2:], jnp.float32)
    _, low, high = axes["y"]
    for side, has in enumerate((low, high)):
        @pl.when(jnp.logical_not(has))
        def _():
            yr_e[side] = jnp.full(yr_e.shape[1:], 1 << ONE, jnp.int32)
            yr_f[side] = jnp.zeros(yr_f.shape[1:], jnp.float32)
    _, low, high = axes["z"]
    for side, has in enumerate((low, high)):
        @pl.when(jnp.logical_not(has))
        def _():
            zr[side] = jnp.zeros(zr.shape[1:], jnp.float32)

    recv(y_e)
    start(c_e)
    ext_e[PX:PX + cx, PY - 2:PY, :] = yr_e[0]
    ext_e[PX:PX + cx, PY + cy:PY + cy + 2, :] = yr_e[1]
    recv(x_e)
    recv(c_e)
    x_sides = [(side, has, at) for side, (has, at) in enumerate(zip(axes["x"][1:], (PX, end)))]
    for side, has, at in x_sides:
        @pl.when(has)
        def _():
            e0 = at - 2 if side == 0 else at
            for ys, er in ((0, PY - 2), (1, PY + cy)):
                ext_e[e0:e0 + 2, er:er + 2, :] = cr_e[side, ys]

    zero = me // n

    def blocks(planes, p0, count, row0, body):
        steps, plane_of = planes
        group = count

        def several(p, b0, size):
            packs = []
            for i in range(size):
                b = b0 + i
                k = (p - p0) * count + b
                packs.append((k, body(p, row0 + zero + 8 * b, k)))
            for j in range(len(packs[0][1])):
                slot = packs[0][1][j][0]
                upper, lower = zs[0, slot], zs[1, slot]
                for k, found in packs:
                    _, to_upper, to_lower = found[j]
                    here = lane == k
                    upper = jnp.where(here, pltpu.roll(to_upper, lax.rem(k + 1, cz), 1), upper)
                    lower = jnp.where(here, pltpu.roll(to_lower, k, 1), lower)
                zs[0, slot] = upper
                zs[1, slot] = lower

        def plane(i, _):
            several(plane_of(i), 0, count)
            return 0

        lax.fori_loop(0, steps, plane, 0)

    def span(p0, p1):
        return p1 - p0, lambda i: i + p0

    def both_ends(p0, p1, depth):
        return 2 * depth, lambda i: i + p0 + i // depth * (p1 - p0 - 2 * depth)

    def rows(ref, lead, p, r):
        return ref[lead + (p, pl.ds(r, 8), slice(None))]

    def from_lower(slot, k):
        return pltpu.roll(zr[0, slot], lax.rem(cz - k, cz), 1)

    def from_upper(slot, k):
        return pltpu.roll(zr[1, slot], cz - 1 - k, 1)

    pairs = [(ax, ay) for ax in (-1, 0, 1) for ay in (-1, 0, 1)]

    def count_body(p, r, k):
        acc = rows(ext_e, (), p, r)
        for ax, ay in pairs:
            if (ax, ay) != (0, 0):
                e = rows(ext_e, (), p - ax, r - ay)
                acc = acc + jnp.where(holds(e, flag(ax, ay, 0)), e, 0)
        up, down = (acc >> UP) & 15, (acc >> DOWN) & 15
        inner = ((acc >> ONE) & 15) + jnp.where(lane == 0, 0, pltpu.roll(up, 1, 1))
        inner = inner + jnp.where(lane == cz - 1, 0, pltpu.roll(down, cz - 1, 1))
        cnt[p, pl.ds(r, 8), :] = inner.astype(jnp.float32)
        return [(0, up.astype(jnp.float32), down.astype(jnp.float32))]

    blocks(span(PX - 1, end + 1), PX - 1, nyb, PY - 4, count_body)
    start(z_c[0])
    recv(y_f)
    start(c_f)
    for c in range(chans):
        ext_f[c, PX:PX + cx, PY - 1:PY, :] = yr_f[0, c]
        ext_f[c, PX:PX + cx, PY + cy:PY + cy + 1, :] = yr_f[1, c]
    recv(z_c[0])

    def weight_body(slot, p, r, k):
        c = rows(cnt, (), p, r)
        c = c + jnp.where(lane == 0, from_lower(0, k), 0.0)
        c = c + jnp.where(lane == cz - 1, from_upper(0, k), 0.0)
        cnt[p, pl.ds(r, 8), :] = c
        w = rows(ext_f, (0,), p, r) / c
        packs = []
        for ch in range(chans):
            v = w if ch == 0 else w * rows(ext_f, (ch,), p, r)
            w0[ch, p, pl.ds(r, 8), :] = v
            packs.append((slot + ch, v, v))
        return packs

    def shift_body(slot, p, r, k):
        for ch in range(chans):
            v = rows(w0, (ch,), p, r)
            wp[ch, p, pl.ds(r, 8), :] = jnp.where(
                lane == cz - 1, from_upper(slot + ch, k), pltpu.roll(v, cz - 1, 1))
            wm[ch, p, pl.ds(r, 8), :] = jnp.where(
                lane == 0, from_lower(slot + ch, k), pltpu.roll(v, 1, 1))
        return []

    def average_body(p, r, k):
        e = rows(ext_e, (), p, r)
        m = {b: holds(e, b) for b in (XP, XM, YP, YM, ZP, ZM)}

        def along_z(ch, q, s):
            side = jnp.where(m[ZP], rows(wp, (ch,), q, s), jnp.where(m[ZM], rows(wm, (ch,), q, s), 0.0))
            return rows(w0, (ch,), q, s) + side

        def along_y(ch, q):
            side = jnp.where(m[YP], along_z(ch, q, r + 1), jnp.where(m[YM], along_z(ch, q, r - 1), 0.0))
            return along_z(ch, q, r) + side

        def whole(ch):
            side = jnp.where(m[XP], along_y(ch, p + 1), jnp.where(m[XM], along_y(ch, p - 1), 0.0))
            return along_y(ch, p) + side

        inverse = 1.0 / whole(0)
        for ch in range(1, chans):
            avg[ch - 1, p, pl.ds(r, 8), :] = whole(ch) * inverse
        return []

    def deposit_body(p, r, k):
        acc = [[None] * 3 for _ in range(fields)]
        for ax, ay in pairs:
            e = rows(ext_e, (), p - ax, r - ay)
            ms = [holds(e, flag(ax, ay, az)) for az in (0, 1, -1)]
            for f in range(fields):
                v = rows(avg, (f,), p - ax, r - ay)
                for i in range(3):
                    term = v if (ax, ay, i) == (0, 0, 0) else jnp.where(ms[i], v, 0.0)
                    acc[f][i] = term if acc[f][i] is None else acc[f][i] + term
        packs = []
        for f in range(fields):
            here, up, down = acc[f]
            here = here + jnp.where(lane == 0, 0.0, pltpu.roll(up, 1, 1))
            here = here + jnp.where(lane == cz - 1, 0.0, pltpu.roll(down, cz - 1, 1))
            out_ref[0, f, p - PX, pl.ds(r - PY, 8), :] = here
            packs.append((1 + 2 * chans + f, up, down))
        return packs

    weight = lambda planes, slot: blocks(
        planes, PX - 1, nyb, PY - 4, functools.partial(weight_body, slot))
    shift = lambda planes, slot: blocks(
        planes, PX - 1, nyb, PY - 4, functools.partial(shift_body, slot))
    average = lambda planes: blocks(planes, PX - 1, nyb, PY - 4, average_body)
    deposit = lambda planes: blocks(planes, PX, cy // 8, PY, deposit_body)

    own, ghosts = span(PX, end), both_ends(PX - 1, end + 1, 1)
    weight(own, 1)
    start(z_c[1])
    recv(z_c[1])
    shift(own, 1)
    average(span(PX + 1, end - 1))
    for c in (x_vf, x_u, c_f):
        recv(c)
    for side, has, at in x_sides:
        @pl.when(has)
        def _():
            f0 = at - 1 if side == 0 else at
            for ys, fr in ((0, PY - 1), (1, PY + cy)):
                for c in range(chans):
                    ext_f[c, f0:f0 + 1, fr:fr + 1, :] = cr_f[side, ys, c]
    weight(ghosts, 1 + chans)
    start(z_c[2])
    deposit(span(PX + 2, end - 2))
    recv(z_c[2])
    shift(ghosts, 1 + chans)
    average(both_ends(PX - 1, end + 1, 2))
    deposit(both_ends(PX, end, 2))
    start(z_c[3])
    recv(z_c[3])

    def final_body(p, r, k):
        inverse = 1.0 / rows(cnt, (), p, r)
        for f in range(fields):
            v = out_ref[0, f, p - PX, pl.ds(r - PY, 8), :]
            v = v + jnp.where(lane == 0, from_lower(1 + 2 * chans + f, k), 0.0)
            v = v + jnp.where(lane == cz - 1, from_upper(1 + 2 * chans + f, k), 0.0)
            out_ref[0, f, p - PX, pl.ds(r - PY, 8), :] = v * inverse
        return []

    blocks(own, PX, cy // 8, PY, final_body)
    for c in everything:
        sent(c)


def per_device(n, conserved, volume_fraction, cut_mask, merge_code):
    fields, cx, cy, cz = conserved.shape[1:]
    chans = fields + 1
    ext = (cx + 5, cy + 24, cz)
    f32, i32 = jnp.float32, jnp.int32
    scratch = [
        pltpu.VMEM(ext, i32), pltpu.VMEM((chans,) + ext, f32), pltpu.VMEM(ext, f32),
        pltpu.VMEM((chans,) + ext, f32), pltpu.VMEM((chans,) + ext, f32), pltpu.VMEM((chans,) + ext, f32),
        pltpu.VMEM((fields,) + ext, f32),
        pltpu.VMEM((cx, cy, cz), i32), pltpu.VMEM((cx, cy, cz), i32),
        pltpu.VMEM((2, cx, 2, cz), i32), pltpu.VMEM((2, chans, cx, 1, cz), f32),
        pltpu.VMEM((2, cx, 2, cz), i32), pltpu.VMEM((2, chans, cx, 1, cz), f32),
        pltpu.VMEM((2, 2, 2, 2, cz), i32), pltpu.VMEM((2, 2, chans, 1, 1, cz), f32),
        pltpu.VMEM((2, 1 + 2 * chans + fields, 8, cz), f32), pltpu.VMEM((2, 1 + 2 * chans + fields, 8, cz), f32),
        pltpu.SemaphoreType.DMA((4,)), pltpu.SemaphoreType.DMA((22,)), pltpu.SemaphoreType.DMA((22,)),
    ]
    return pl.pallas_call(
        functools.partial(kernel, n, (fields, cx, cy, cz)),
        out_shape=jax.ShapeDtypeStruct(conserved.shape, f32),
        in_specs=[pl.BlockSpec(memory_space=pl.ANY)] * 4,
        out_specs=pl.BlockSpec(memory_space=pltpu.VMEM),
        scratch_shapes=scratch,
        compiler_params=pltpu.CompilerParams(
            collective_id=0, has_side_effects=True, vmem_limit_bytes=60 * 1024 * 1024),
        name="redistribute",
    )(conserved, volume_fraction, cut_mask, merge_code)


def solution(mesh):
    return jax.shard_map(
        functools.partial(per_device, mesh.shape["boxes"]),
        mesh=mesh,
        in_specs=(
            P("boxes", None, None, None, None),
            P("boxes", None, None, None),
            P("boxes", None, None, None),
            P("boxes", None, None, None),
        ),
        out_specs=P("boxes", None, None, None, None),
        check_vma=False,
    )
```

```python
import functools

import jax
import jax.numpy as jnp
from jax import lax
from jax.experimental import pallas as pl
from jax.experimental.pallas import tpu as pltpu
from jax.sharding import PartitionSpec as P

NBY = 4
NBZ = 4
MESH = pl.DeviceIdType.MESH
XP, XM, YP, YM, ZP, ZM = 1, 2, 4, 8, 16, 32
ONE, UP, DOWN = 10, 14, 18
PX, PY = 2, 8


def flag(ax, ay, az):
    return (
        {1: XP, -1: XM, 0: 0}[ax] | {1: YP, -1: YM, 0: 0}[ay] | {1: ZP, -1: ZM, 0: 0}[az]
    )


def holds(e, bits):
    return (e & bits) == bits


def kernel(n, dims, u_ref, vf_ref, mask_ref, code_ref, out_ref, ext_e, ext_f, cnt, w0, wp, wm, avg,
           raw_m, raw_c, ys_e, ys_f, yr_e, yr_f, cr_e, cr_f, zs, zr, load_sem, send_sem, recv_sem):
    fields, cx, cy, cz = dims
    chans = fields + 1
    me = lax.axis_index("boxes")
    bx, by, bz = me // (NBY * NBZ), me // NBZ % NBY, me % NBZ
    axes = {
        "x": (NBY * NBZ, bx > 0, bx < n // (NBY * NBZ) - 1),
        "y": (NBZ, by > 0, by < NBY - 1),
        "z": (1, bz > 0, bz < NBZ - 1),
    }
    lane = lax.broadcasted_iota(jnp.int32, (8, cz), 1)
    nyb = (cy + 8) // 8

    loads = [
        pltpu.make_async_copy(mask_ref.at[0], raw_m, load_sem.at[0]),
        pltpu.make_async_copy(code_ref.at[0], raw_c, load_sem.at[1]),
        pltpu.make_async_copy(vf_ref.at[0], ext_f.at[0, PX:PX + cx, PY:PY + cy], load_sem.at[2]),
        pltpu.make_async_copy(u_ref.at[0], ext_f.at[1:chans, PX:PX + cx, PY:PY + cy], load_sem.at[3]),
    ]
    for copy in loads:
        copy.start()

    barrier = pltpu.get_barrier_semaphore()
    total = jnp.int32(0)
    for stride, low, high in axes.values():
        for has, there in ((low, me - stride), (high, me + stride)):
            @pl.when(has)
            def _():
                pl.semaphore_signal(barrier, inc=1, device_id=(there,), device_id_type=MESH)
            total = total + has.astype(jnp.int32)
    pl.semaphore_wait(barrier, total)

    def copies(axis, ident, up, down):
        stride = axes[axis][0]
        out = []
        for d, (pair, there) in enumerate(((up, me + stride), (down, me - stride))):
            out.append(pltpu.make_async_remote_copy(
                src_ref=pair[0], dst_ref=pair[1], send_sem=send_sem.at[2 * ident + d],
                recv_sem=recv_sem.at[2 * ident + d], device_id=(there,), device_id_type=MESH))
        return axis, out

    def start(c):
        axis, (up, down) = c
        _, low, high = axes[axis]
        pl.when(high)(lambda: up.start())
        pl.when(low)(lambda: down.start())

    def recv(c):
        axis, (up, down) = c
        _, low, high = axes[axis]
        pl.when(low)(lambda: up.wait_recv())
        pl.when(high)(lambda: down.wait_recv())

    def sent(c):
        axis, (up, down) = c
        _, low, high = axes[axis]
        pl.when(high)(lambda: up.wait_send())
        pl.when(low)(lambda: down.wait_send())

    def x_face(ident, ref, lead, depth):
        box = slice(PY, PY + cy)
        at = lambda a, b: ref.at[lead + (slice(a, b), box)]
        end = PX + cx
        return copies("x", ident, (at(end - depth, end), at(PX - depth, PX)),
                      (at(PX, PX + depth), at(end, end + depth)))

    x_e = x_face(0, ext_e, (), 2)
    x_vf = x_face(1, ext_f, (slice(0, 1),), 1)
    x_u = x_face(2, ext_f, (slice(1, chans),), 1)
    y_e = copies("y", 3, (ys_e.at[0], yr_e.at[0]), (ys_e.at[1], yr_e.at[1]))
    y_f = copies("y", 4, (ys_f.at[0], yr_f.at[0]), (ys_f.at[1], yr_f.at[1]))
    c_e = copies("x", 5, (yr_e.at[:, cx - 2:cx], cr_e.at[0]), (yr_e.at[:, 0:2], cr_e.at[1]))
    c_f = copies("x", 6, (yr_f.at[:, :, cx - 1:cx], cr_f.at[0]), (yr_f.at[:, :, 0:1], cr_f.at[1]))
    last = 1 + 2 * chans
    spans = ((0, 1), (1, 1 + chans), (1 + chans, last), (last, last + fields))
    z_c = [copies("z", 7 + i, (zs.at[0, a:b], zr.at[0, a:b]), (zs.at[1, a:b], zr.at[1, a:b]))
           for i, (a, b) in enumerate(spans)]
    everything = [x_e, x_vf, x_u, y_e, y_f, c_e, c_f] + z_c

    loads[2].wait()
    loads[3].wait()
    start(x_vf)
    start(x_u)
    loads[0].wait()
    loads[1].wait()

    def encode(p, _):
        c = raw_c[p]
        cut = raw_m[p] == 1
        third = (c * 171) >> 9
        sz = c - 3 * third
        ninth = (third * 171) >> 9
        sy = third - 3 * ninth
        bit = lambda test, value: jnp.where(test, value, 0)
        e = (bit(ninth == 2, XP) + bit(ninth == 0, XM) + bit(sy == 2, YP) + bit(sy == 0, YM)
             + bit(sz == 2, ZP + (1 << UP)) + bit(sz == 0, ZM + (1 << DOWN)))
        ext_e[PX + p, PY:PY + cy, :] = jnp.where(cut, e, 0) + (1 << ONE)
        return 0

    lax.fori_loop(0, cx, encode, 0)
    start(x_e)
    ys_e[0] = ext_e[PX:PX + cx, PY + cy - 2:PY + cy, :]
    ys_e[1] = ext_e[PX:PX + cx, PY:PY + 2, :]
    start(y_e)
    for c in range(chans):
        ys_f[0, c] = ext_f[c, PX:PX + cx, PY + cy - 1:PY + cy, :]
        ys_f[1, c] = ext_f[c, PX:PX + cx, PY:PY + 1, :]
    start(y_f)

    end = PX + cx
    _, low, high = axes["x"]
    for has, (e0, e1), (f0, f1) in ((low, (0, 2), (1, 2)), (high, (end, end + 2), (end, end + 1))):
        @pl.when(jnp.logical_not(has))
        def _():
            ext_e[e0:e1, :, :] = jnp.full((e1 - e0,) + ext_e.shape[1:], 1 << ONE, jnp.int32)
            for c in range(chans):
                ext_f[c, f0:f1, :, :] = jnp.zeros((f1 - f0,) + ext_f.shape[2:], jnp.float32)
    _, low, high = axes["y"]
    for side, has in enumerate((low, high)):
        @pl.when(jnp.logical_not(has))
        def _():
            yr_e[side] = jnp.full(yr_e.shape[1:], 1 << ONE, jnp.int32)
            yr_f[side] = jnp.zeros(yr_f.shape[1:], jnp.float32)
    _, low, high = axes["z"]
    for side, has in enumerate((low, high)):
        @pl.when(jnp.logical_not(has))
        def _():
            zr[side] = jnp.zeros(zr.shape[1:], jnp.float32)

    recv(y_e)
    start(c_e)
    ext_e[PX:PX + cx, PY - 2:PY, :] = yr_e[0]
    ext_e[PX:PX + cx, PY + cy:PY + cy + 2, :] = yr_e[1]
    recv(x_e)
    recv(c_e)
    x_sides = [(side, has, at) for side, (has, at) in enumerate(zip(axes["x"][1:], (PX, end)))]
    for side, has, at in x_sides:
        @pl.when(has)
        def _():
            e0 = at - 2 if side == 0 else at
            for ys, er in ((0, PY - 2), (1, PY + cy)):
                ext_e[e0:e0 + 2, er:er + 2, :] = cr_e[side, ys]

    zero = me // n

    def blocks(planes, p0, count, row0, body):
        steps, plane_of = planes
        group = count

        def several(p, b0, size):
            packs = []
            for i in range(size):
                b = b0 + i
                k = (p - p0) * count + b
                packs.append((k, body(p, row0 + zero + 8 * b, k)))
            for j in range(len(packs[0][1])):
                slot = packs[0][1][j][0]
                upper, lower = zs[0, slot], zs[1, slot]
                for k, found in packs:
                    _, to_upper, to_lower = found[j]
                    here = lane == k
                    upper = jnp.where(here, pltpu.roll(to_upper, lax.rem(k + 1, cz), 1), upper)
                    lower = jnp.where(here, pltpu.roll(to_lower, k, 1), lower)
                zs[0, slot] = upper
                zs[1, slot] = lower

        def plane(i, _):
            several(plane_of(i), 0, count)
            return 0

        lax.fori_loop(0, steps, plane, 0)

    def span(p0, p1):
        return p1 - p0, lambda i: i + p0

    def both_ends(p0, p1, depth):
        return 2 * depth, lambda i: i + p0 + i // depth * (p1 - p0 - 2 * depth)

    def rows(ref, lead, p, r):
        return ref[lead + (p, pl.ds(r, 8), slice(None))]

    def from_lower(slot, k):
        return pltpu.roll(zr[0, slot], lax.rem(cz - k, cz), 1)

    def from_upper(slot, k):
        return pltpu.roll(zr[1, slot], cz - 1 - k, 1)

    pairs = [(ax, ay) for ax in (-1, 0, 1) for ay in (-1, 0, 1)]

    def count_body(p, r, k):
        acc = rows(ext_e, (), p, r)
        for ax, ay in pairs:
            if (ax, ay) != (0, 0):
                e = rows(ext_e, (), p - ax, r - ay)
                acc = acc + jnp.where(holds(e, flag(ax, ay, 0)), e, 0)
        up, down = (acc >> UP) & 15, (acc >> DOWN) & 15
        inner = ((acc >> ONE) & 15) + jnp.where(lane == 0, 0, pltpu.roll(up, 1, 1))
        inner = inner + jnp.where(lane == cz - 1, 0, pltpu.roll(down, cz - 1, 1))
        cnt[p, pl.ds(r, 8), :] = inner.astype(jnp.float32)
        return [(0, up.astype(jnp.float32), down.astype(jnp.float32))]

    blocks(span(PX - 1, end + 1), PX - 1, nyb, PY - 4, count_body)
    start(z_c[0])
    recv(y_f)
    start(c_f)
    for c in range(chans):
        ext_f[c, PX:PX + cx, PY - 1:PY, :] = yr_f[0, c]
        ext_f[c, PX:PX + cx, PY + cy:PY + cy + 1, :] = yr_f[1, c]
    recv(z_c[0])

    def weight_body(slot, p, r, k):
        c = rows(cnt, (), p, r)
        c = c + jnp.where(lane == 0, from_lower(0, k), 0.0)
        c = c + jnp.where(lane == cz - 1, from_upper(0, k), 0.0)
        cnt[p, pl.ds(r, 8), :] = c
        w = rows(ext_f, (0,), p, r) / c
        packs = []
        for ch in range(chans):
            v = w if ch == 0 else w * rows(ext_f, (ch,), p, r)
            w0[ch, p, pl.ds(r, 8), :] = v
            packs.append((slot + ch, v, v))
        return packs

    def shift_body(slot, p, r, k):
        for ch in range(chans):
            v = rows(w0, (ch,), p, r)
            wp[ch, p, pl.ds(r, 8), :] = jnp.where(
                lane == cz - 1, from_upper(slot + ch, k), pltpu.roll(v, cz - 1, 1))
            wm[ch, p, pl.ds(r, 8), :] = jnp.where(
                lane == 0, from_lower(slot + ch, k), pltpu.roll(v, 1, 1))
        return []

    def average_body(p, r, k):
        e = rows(ext_e, (), p, r)
        m = {b: holds(e, b) for b in (XP, XM, YP, YM, ZP, ZM)}

        def along_z(ch, q, s):
            side = jnp.where(m[ZP], rows(wp, (ch,), q, s), jnp.where(m[ZM], rows(wm, (ch,), q, s), 0.0))
            return rows(w0, (ch,), q, s) + side

        def along_y(ch, q):
            side = jnp.where(m[YP], along_z(ch, q, r + 1), jnp.where(m[YM], along_z(ch, q, r - 1), 0.0))
            return along_z(ch, q, r) + side

        def whole(ch):
            side = jnp.where(m[XP], along_y(ch, p + 1), jnp.where(m[XM], along_y(ch, p - 1), 0.0))
            return along_y(ch, p) + side

        inverse = 1.0 / whole(0)
        for ch in range(1, chans):
            avg[ch - 1, p, pl.ds(r, 8), :] = whole(ch) * inverse
        return []

    def deposit_body(p, r, k):
        acc = [[None] * 3 for _ in range(fields)]
        for ax, ay in pairs:
            e = rows(ext_e, (), p - ax, r - ay)
            ms = [holds(e, flag(ax, ay, az)) for az in (0, 1, -1)]
            for f in range(fields):
                v = rows(avg, (f,), p - ax, r - ay)
                for i in range(3):
                    term = v if (ax, ay, i) == (0, 0, 0) else jnp.where(ms[i], v, 0.0)
                    acc[f][i] = term if acc[f][i] is None else acc[f][i] + term
        packs = []
        for f in range(fields):
            here, up, down = acc[f]
            here = here + jnp.where(lane == 0, 0.0, pltpu.roll(up, 1, 1))
            here = here + jnp.where(lane == cz - 1, 0.0, pltpu.roll(down, cz - 1, 1))
            out_ref[0, f, p - PX, pl.ds(r - PY, 8), :] = here
            packs.append((1 + 2 * chans + f, up, down))
        return packs

    weight = lambda planes, slot: blocks(
        planes, PX - 1, nyb, PY - 4, functools.partial(weight_body, slot))
    shift = lambda planes, slot: blocks(
        planes, PX - 1, nyb, PY - 4, functools.partial(shift_body, slot))
    average = lambda planes: blocks(planes, PX - 1, nyb, PY - 4, average_body)
    deposit = lambda planes: blocks(planes, PX, cy // 8, PY, deposit_body)

    own, ghosts = span(PX, end), both_ends(PX - 1, end + 1, 1)
    weight(own, 1)
    start(z_c[1])
    recv(z_c[1])
    shift(own, 1)
    average(span(PX + 1, end - 1))
    for c in (x_vf, x_u, c_f):
        recv(c)
    for side, has, at in x_sides:
        @pl.when(has)
        def _():
            f0 = at - 1 if side == 0 else at
            for ys, fr in ((0, PY - 1), (1, PY + cy)):
                for c in range(chans):
                    ext_f[c, f0:f0 + 1, fr:fr + 1, :] = cr_f[side, ys, c]
    weight(ghosts, 1 + chans)
    start(z_c[2])
    deposit(span(PX + 2, end - 2))
    recv(z_c[2])
    shift(ghosts, 1 + chans)
    average(both_ends(PX - 1, end + 1, 2))
    deposit(both_ends(PX, end, 2))
    start(z_c[3])
    recv(z_c[3])

    def final_body(p, r, k):
        inverse = 1.0 / rows(cnt, (), p, r)
        for f in range(fields):
            v = out_ref[0, f, p - PX, pl.ds(r - PY, 8), :]
            v = v + jnp.where(lane == 0, from_lower(1 + 2 * chans + f, k), 0.0)
            v = v + jnp.where(lane == cz - 1, from_upper(1 + 2 * chans + f, k), 0.0)
            out_ref[0, f, p - PX, pl.ds(r - PY, 8), :] = v * inverse
        return []

    blocks(own, PX, cy // 8, PY, final_body)
    for c in everything:
        sent(c)


def per_device(n, conserved, volume_fraction, cut_mask, merge_code):
    fields, cx, cy, cz = conserved.shape[1:]
    chans = fields + 1
    ext = (cx + 5, cy + 24, cz)
    f32, i32 = jnp.float32, jnp.int32
    scratch = [
        pltpu.VMEM(ext, i32), pltpu.VMEM((chans,) + ext, f32), pltpu.VMEM(ext, f32),
        pltpu.VMEM((chans,) + ext, f32), pltpu.VMEM((chans,) + ext, f32), pltpu.VMEM((chans,) + ext, f32),
        pltpu.VMEM((fields,) + ext, f32),
        pltpu.VMEM((cx, cy, cz), i32), pltpu.VMEM((cx, cy, cz), i32),
        pltpu.VMEM((2, cx, 2, cz), i32), pltpu.VMEM((2, chans, cx, 1, cz), f32),
        pltpu.VMEM((2, cx, 2, cz), i32), pltpu.VMEM((2, chans, cx, 1, cz), f32),
        pltpu.VMEM((2, 2, 2, 2, cz), i32), pltpu.VMEM((2, 2, chans, 1, 1, cz), f32),
        pltpu.VMEM((2, 1 + 2 * chans + fields, 8, cz), f32), pltpu.VMEM((2, 1 + 2 * chans + fields, 8, cz), f32),
        pltpu.SemaphoreType.DMA((4,)), pltpu.SemaphoreType.DMA((22,)), pltpu.SemaphoreType.DMA((22,)),
    ]
    return pl.pallas_call(
        functools.partial(kernel, n, (fields, cx, cy, cz)),
        out_shape=pltpu.VMEM(conserved.shape, f32),
        in_specs=[pl.BlockSpec(memory_space=pl.ANY)] * 4,
        out_specs=pl.BlockSpec(memory_space=pltpu.VMEM),
        scratch_shapes=scratch,
        compiler_params=pltpu.CompilerParams(
            collective_id=0, has_side_effects=True, vmem_limit_bytes=60 * 1024 * 1024),
        name="redistribute",
    )(conserved, volume_fraction, cut_mask, merge_code)


def solution(mesh):
    return jax.shard_map(
        functools.partial(per_device, mesh.shape["boxes"]),
        mesh=mesh,
        in_specs=(
            P("boxes", None, None, None, None),
            P("boxes", None, None, None),
            P("boxes", None, None, None),
            P("boxes", None, None, None),
        ),
        out_specs=P("boxes", None, None, None, None),
        check_vma=False,
    )
```

```python
import functools

import jax
import jax.numpy as jnp
from jax import lax
from jax.experimental import pallas as pl
from jax.experimental.pallas import tpu as pltpu
from jax.sharding import PartitionSpec as P

NBY = 4
NBZ = 4
MESH = pl.DeviceIdType.MESH
XP, XM, YP, YM, ZP, ZM = 1, 2, 4, 8, 16, 32
ONE, UP, DOWN = 10, 14, 18
NONE = 1 << ONE
PAD = 8
PAIRS = [(ax, ay) for ax in (0, 1, -1) for ay in (0, 1, -1)]


def flag(ax, ay, az=0):
    return (
        {1: XP, -1: XM, 0: 0}[ax] | {1: YP, -1: YM, 0: 0}[ay] | {1: ZP, -1: ZM, 0: 0}[az]
    )


def holds(e, bits):
    return (e & bits) == bits


def kernel(n, dims, u_ref, vf_ref, mask_ref, code_ref, out_ref, ee, ff, inv, aa, avg,
           raw_m, raw_c, raw_f, ys_e, ys_f, yr_e, yr_f, xs_e, xr_e, xr_f, cr_e, cr_f,
           zs_e, zs_f, zr_e, zr_f, inj_c, inj_w, inj_d, load_sem, send_sem, recv_sem):
    fields, cx, cy, cz = dims
    chans = fields + 1
    nb = cy // 8 + 1
    pitch = 8 * nb
    me = lax.axis_index("boxes")
    bx, by, bz = me // (NBY * NBZ), me // NBZ % NBY, me % NBZ
    axes = {
        "x": (NBY * NBZ, bx > 0, bx < n // (NBY * NBZ) - 1),
        "y": (NBZ, by > 0, by < NBY - 1),
        "z": (1, bz > 0, bz < NBZ - 1),
    }
    lane = lax.broadcasted_iota(jnp.int32, (8, cz), 1)
    sub = lax.broadcasted_iota(jnp.int32, (8, cz), 0)
    first, final = lane == 0, lane == cz - 1

    loads = [
        pltpu.make_async_copy(u_ref.at[0], raw_f.at[1:chans], load_sem.at[0]),
        pltpu.make_async_copy(vf_ref.at[0], raw_f.at[0], load_sem.at[1]),
        pltpu.make_async_copy(mask_ref.at[0], raw_m, load_sem.at[2]),
        pltpu.make_async_copy(code_ref.at[0], raw_c, load_sem.at[3]),
    ]
    for copy in loads:
        copy.start()

    barrier = pltpu.get_barrier_semaphore()
    total = jnp.int32(0)
    for stride, low, high in axes.values():
        for has, there in ((low, me - stride), (high, me + stride)):
            @pl.when(has)
            def _():
                pl.semaphore_signal(barrier, inc=1, device_id=(there,), device_id_type=MESH)
            total = total + has.astype(jnp.int32)
    pl.semaphore_wait(barrier, total)

    def copies(axis, ident, up, down):
        stride = axes[axis][0]
        out = []
        for d, (pair, there) in enumerate(((up, me + stride), (down, me - stride))):
            out.append(pltpu.make_async_remote_copy(
                src_ref=pair[0], dst_ref=pair[1], send_sem=send_sem.at[2 * ident + d],
                recv_sem=recv_sem.at[2 * ident + d], device_id=(there,), device_id_type=MESH))
        return axis, out

    def start(c):
        axis, (up, down) = c
        _, low, high = axes[axis]
        pl.when(high)(lambda: up.start())
        pl.when(low)(lambda: down.start())

    def recv(c):
        axis, (up, down) = c
        _, low, high = axes[axis]
        pl.when(low)(lambda: up.wait_recv())
        pl.when(high)(lambda: down.wait_recv())

    def sent(c):
        axis, (up, down) = c
        _, low, high = axes[axis]
        pl.when(high)(lambda: up.wait_send())
        pl.when(low)(lambda: down.wait_send())

    x_f = copies("x", 0, (raw_f.at[:, cx - 1:cx], xr_f.at[0]), (raw_f.at[:, 0:1], xr_f.at[1]))
    x_e = copies("x", 1, (xs_e.at[1], xr_e.at[0]), (xs_e.at[0], xr_e.at[1]))
    y_e = copies("y", 2, (ys_e.at[0], yr_e.at[0]), (ys_e.at[1], yr_e.at[1]))
    y_f = copies("y", 3, (ys_f.at[0], yr_f.at[0]), (ys_f.at[1], yr_f.at[1]))
    c_e = copies("x", 4, (yr_e.at[:, cx - 2:cx], cr_e.at[0]), (yr_e.at[:, 0:2], cr_e.at[1]))
    c_f = copies("x", 5, (yr_f.at[:, :, cx - 1:cx], cr_f.at[0]), (yr_f.at[:, :, 0:1], cr_f.at[1]))
    z_e = [copies("z", 6 + t, (zs_e.at[1], zr_e.at[t, 0]), (zs_e.at[0], zr_e.at[t, 1])) for t in (0, 1)]
    z_f = [copies("z", 8 + t, (zs_f.at[1], zr_f.at[t, 0]), (zs_f.at[0], zr_f.at[t, 1])) for t in (0, 1)]

    loads[0].wait()
    loads[1].wait()
    start(x_f)
    loads[2].wait()
    loads[3].wait()

    def row_of(p, y):
        return PAD + pitch * (p + 2) + 8 + y

    _, x_low, x_high = axes["x"]
    _, y_low, y_high = axes["y"]
    _, z_low, z_high = axes["z"]
    clear = lambda has, bits: jnp.where(has, 0, bits)
    row2 = lax.broadcasted_iota(jnp.int32, (cy, cz), 0)
    lane2 = lax.broadcasted_iota(jnp.int32, (cy, cz), 1)
    drop = (jnp.where(row2 == 0, clear(y_low, YM), 0) + jnp.where(row2 == cy - 1, clear(y_high, YP), 0)
            + jnp.where(lane2 == 0, clear(z_low, ZM + (1 << DOWN)), 0)
            + jnp.where(lane2 == cz - 1, clear(z_high, ZP + (1 << UP)), 0))
    keep = ~drop

    def encode(p, _):
        c = raw_c[p]
        cut = raw_m[p] == 1
        third = (c * 171) >> 9
        sz = c - 3 * third
        ninth = (third * 171) >> 9
        sy = third - 3 * ninth
        bit = lambda test, value: jnp.where(test, value, 0)
        e = (bit(ninth == 2, XP) + bit(ninth == 0, XM) + bit(sy == 2, YP) + bit(sy == 0, YM)
             + bit(sz == 2, ZP + (1 << UP)) + bit(sz == 0, ZM + (1 << DOWN)))
        off = jnp.where(p == 0, clear(x_low, XM), 0) + jnp.where(p == cx - 1, clear(x_high, XP), 0)
        ee[pl.ds(row_of(p, 0), cy), :] = (jnp.where(cut, e, 0) & keep & ~off) + NONE
        ys_e[0, p] = ee[pl.ds(row_of(p, cy - 2), 2), :]
        ys_e[1, p] = ee[pl.ds(row_of(p, 0), 2), :]
        return 0

    lax.fori_loop(0, cx, encode, 0)
    start(y_e)
    for i in range(2):
        xs_e[0, i] = ee[row_of(i, 0):row_of(i, cy), :]
        xs_e[1, i] = ee[row_of(cx - 2 + i, 0):row_of(cx - 2 + i, cy), :]
    for c in range(chans):
        ys_f[0, c] = raw_f[c, :, cy - 1:cy, :]
        ys_f[1, c] = raw_f[c, :, 0:1, :]
    start(y_f)
    start(x_e)

    @pl.when(jnp.logical_not(x_low))
    def _():
        a, b = PAD, row_of(-1, cy + 2)
        ee[a:b, :] = jnp.full((b - a, cz), NONE, jnp.int32)

    @pl.when(jnp.logical_not(x_high))
    def _():
        a, b = row_of(cx, -2), row_of(cx + 1, cy + 8)
        ee[a:b, :] = jnp.full((b - a, cz), NONE, jnp.int32)

    for side, has in enumerate((y_low, y_high)):
        @pl.when(jnp.logical_not(has))
        def _():
            yr_e[side] = jnp.full(yr_e.shape[1:], NONE, jnp.int32)
            yr_f[side] = jnp.zeros(yr_f.shape[1:], jnp.float32)
    for side, has in enumerate((z_low, z_high)):
        @pl.when(jnp.logical_not(has))
        def _():
            for t in (0, 1):
                zr_e[t, side] = jnp.full(zr_e.shape[2:], NONE, jnp.int32)
                zr_f[t, side] = jnp.zeros(zr_f.shape[2:], jnp.float32)

    def turn(v, amount):
        if isinstance(amount, int):
            return pltpu.roll(v, amount % cz, 1) if amount % cz else v
        return pltpu.roll(v, lax.rem(amount + cz, cz), 1)

    def pack(ks, e_of, f_of):
        here = [lane == k for k in ks]
        es = [e_of(i) for i in range(len(ks))]
        for side, shifts in enumerate(((0, -1), (1, 2))):
            for j in (0, 1):
                acc = zs_e[side, j]
                for k, at, e in zip(ks, here, es):
                    acc = jnp.where(at, turn(e, k + shifts[j]), acc)
                zs_e[side, j] = acc
        for c in range(chans):
            fs = [f_of(i, c) for i in range(len(ks))]
            for side in (0, 1):
                acc = zs_f[side, c]
                for k, at, f in zip(ks, here, fs):
                    acc = jnp.where(at, turn(f, k + side), acc)
                zs_f[side, c] = acc

    def pack_flat(ks):
        pack(ks, lambda i: ee[PAD + 8 * ks[i]:PAD + 8 * ks[i] + 8, :],
             lambda i, c: ff[c, PAD + 8 * ks[i]:PAD + 8 * ks[i] + 8, :])

    zs_e[...] = jnp.full(zs_e.shape, NONE, jnp.int32)
    zs_f[...] = jnp.zeros(zs_f.shape, jnp.float32)
    group = 2 if cx % 2 == 0 else 1

    def pack_own(i, _):
        ks, where = [], []
        for j in range(group):
            p = i * group + j
            for c in range(chans):
                ff[c, pl.ds(row_of(p, 0), cy), :] = raw_f[c, p]
            for b in range(nb - 1):
                ks.append((p + 2) * nb + 1 + b)
                where.append((p, b))
        pack(ks, lambda i: ee[pl.ds(PAD + 8 * ks[i], 8), :],
             lambda i, c: raw_f[c, where[i][0], 8 * where[i][1]:8 * where[i][1] + 8, :])
        return 0

    lax.fori_loop(0, cx // group, pack_own, 0)

    recv(y_e)
    start(c_e)
    for p in range(cx):
        ee[row_of(p, -2):row_of(p, 0), :] = yr_e[0, p]
        ee[row_of(p, cy):row_of(p, cy + 2), :] = yr_e[1, p]
    recv(y_f)
    start(c_f)
    for p in range(cx):
        for c in range(chans):
            ff[c, row_of(p, -1):row_of(p, 0), :] = yr_f[0, c, p]
            ff[c, row_of(p, cy):row_of(p, cy + 1), :] = yr_f[1, c, p]
    between = [(p + 2) * nb for p in range(cx + 1)]
    pack_flat(between[:len(between) // 2])
    pack_flat(between[len(between) // 2:])
    start(z_e[0])
    start(z_f[0])

    zero = me // n

    def blocks(p0, p1, chunk, body):
        k0 = (p0 + 2) * nb
        steps = ((p1 - p0) * nb + chunk) // chunk

        def step(i, _):
            for j in range(chunk):
                k = k0 + i * chunk + j
                body(k, PAD + 8 * k)
            return 0

        lax.fori_loop(0, steps, step, 0)

    def rows(ref, lead, r):
        return ref[lead + (pl.ds(r, 8), slice(None))]

    def count_body(k, r):
        acc = rows(ee, (), r)
        for ax, ay in PAIRS[1:]:
            e = rows(ee, (), r - pitch * ax - ay)
            acc = acc + jnp.where(holds(e, flag(ax, ay)), e, 0)
        here = (acc >> ONE) & 15
        here = here + pltpu.roll((acc >> UP) & 15, 1, 1) + pltpu.roll((acc >> DOWN) & 15, cz - 1, 1)
        inv[pl.ds(r, 8), :] = 1.0 / here.astype(jnp.float32)

    def edge(ref, lead, k, side):
        return turn(ref[(side,) + lead], cz - side - k)

    def weight_body(k, r):
        i = rows(inv, (), r)
        i = jnp.where(first, edge(inj_c, (), k, 0), jnp.where(final, edge(inj_c, (), k, 1), i))
        inv[pl.ds(r, 8), :] = i
        w = rows(ff, (0,), r) * i
        for c in range(chans):
            v = w if c == 0 else w * rows(ff, (c,), r)
            aa[3 * c, pl.ds(r, 8), :] = v
            aa[3 * c + 1, pl.ds(r, 8), :] = v + jnp.where(final, edge(inj_w, (c,), k, 1), pltpu.roll(v, cz - 1, 1))
            aa[3 * c + 2, pl.ds(r, 8), :] = v + jnp.where(first, edge(inj_w, (c,), k, 0), pltpu.roll(v, 1, 1))

    def average_body(k, r):
        e = rows(ee, (), r)
        m = {b: holds(e, b) for b in (XP, XM, YP, YM, ZP, ZM)}

        def along_z(c, q):
            return jnp.where(m[ZP], rows(aa, (3 * c + 1,), q),
                             jnp.where(m[ZM], rows(aa, (3 * c + 2,), q), rows(aa, (3 * c,), q)))

        def along_y(c, q):
            side = jnp.where(m[YP], along_z(c, q + 1), jnp.where(m[YM], along_z(c, q - 1), 0.0))
            return along_z(c, q) + side

        def whole(c):
            side = jnp.where(m[XP], along_y(c, r + pitch), jnp.where(m[XM], along_y(c, r - pitch), 0.0))
            return along_y(c, r) + side

        inverse = 1.0 / whole(0)
        for c in range(1, chans):
            avg[c - 1, pl.ds(r, 8), :] = whole(c) * inverse

    def deposit_body(p, b):
        k = (p + 2) * nb + 1 + b
        r = PAD + 8 * k
        acc = [[None] * 3 for _ in range(fields)]
        for ax, ay in PAIRS:
            s = r - pitch * ax - ay
            e = rows(ee, (), s)
            ms = [holds(e, flag(ax, ay, az)) for az in (0, 1, -1)]
            for f in range(fields):
                v = rows(avg, (f,), s)
                for i in range(3):
                    term = v if (ax, ay, i) == (0, 0, 0) else jnp.where(ms[i], v, 0.0)
                    acc[f][i] = term if acc[f][i] is None else acc[f][i] + term
        i = rows(inv, (), r)
        for f in range(fields):
            here, up, down = acc[f]
            here = here + jnp.where(first, edge(inj_d, (f,), k, 0), pltpu.roll(up, 1, 1))
            here = here + jnp.where(final, edge(inj_d, (f,), k, 1), pltpu.roll(down, cz - 1, 1))
            out_ref[0, f, p, 8 * b:8 * b + 8, :] = here * i

    def deposit(p0, p1):
        def plane(i, _):
            for b in range(nb - 1):
                deposit_body(p0 + i, b)
            return 0

        lax.fori_loop(0, p1 - p0, plane, 0)

    def shift_y(v, dy):
        if dy == 0:
            return v
        w = pltpu.roll(v, 7 if dy == 1 else 1, 0)
        return jnp.where(sub == (7 if dy == 1 else 0), turn(w, -dy), w)

    def shift_x(v, dx):
        return turn(v, -nb * dx) if dx else v

    def spread(t):
        lines = {ax: t[ax, 0] + shift_y(t[ax, 1], -1) + shift_y(t[ax, -1], 1) for ax in (0, 1, -1)}
        return lines[0] + shift_x(lines[1], -1) + shift_x(lines[-1], 1)

    def ghost(t, side):
        toward, away = (ZP, ZM) if side == 0 else (ZM, ZP)
        e0, e1, g0, g1 = zs_e[side, 0], zs_e[side, 1], zr_e[t, side, 0], zr_e[t, side, 1]
        from_g0 = jnp.where(holds(g0, toward), 257, 1)
        from_e0 = jnp.where(holds(e0, away), 257, 256)
        found = {}
        for ax, ay in PAIRS:
            b = flag(ax, ay)
            found[ax, ay] = (jnp.where(holds(g1, b | toward), 1, 0) + jnp.where(holds(g0, b), from_g0, 0)
                             + jnp.where(holds(e0, b), from_e0, 0) + jnp.where(holds(e1, b | away), 256, 0))
        found = spread(found)
        i_ghost = 1.0 / (found & 255).astype(jnp.float32)
        i_own = 1.0 / (found >> 8).astype(jnp.float32)
        inj_c[side] = i_own
        w_ghost, w_own = zr_f[t, side, 0] * i_ghost, zs_f[side, 0] * i_own
        m = {b: holds(g0, b) for b in (XP, XM, YP, YM)}
        mine = holds(g0, toward)
        inverse = None
        for c in range(chans):
            v = w_ghost if c == 0 else w_ghost * zr_f[t, side, c]
            inj_w[side, c] = v
            v = v + (w_own if c == 0 else w_own * zs_f[side, c])
            above, below = shift_y(v, 1), shift_y(v, -1)
            line = {dx: shift_x(v, dx) + jnp.where(m[YP], shift_x(above, dx), jnp.where(m[YM], shift_x(below, dx), 0.0))
                    for dx in (0, 1, -1)}
            whole = line[0] + jnp.where(m[XP], line[1], jnp.where(m[XM], line[-1], 0.0))
            if c == 0:
                inverse = 1.0 / whole
                continue
            a = jnp.where(mine, whole * inverse, 0.0)
            inj_d[side, c - 1] = spread({
                (ax, ay): jnp.where(holds(g0, flag(ax, ay)), a, 0.0) if (ax, ay) != (0, 0) else a
                for ax, ay in PAIRS})

    low, high = x_low.astype(jnp.int32), x_high.astype(jnp.int32)
    blocks(low, cx - high, 6, count_body)
    recv(z_e[0])
    recv(z_f[0])
    for side in (0, 1):
        ghost(0, side)
    blocks(low, cx - high, 6, weight_body)
    blocks(2 * low, cx - 2 * high, 5, average_body)

    for c in (x_f, x_e, c_e, c_f):
        recv(c)
    for c in (z_e[0], z_f[0]):
        sent(c)
    for side, has in enumerate((x_low, x_high)):
        @pl.when(has)
        def _():
            for i in range(2):
                p = (i - 2, cx + i)[side]
                ee[row_of(p, 0):row_of(p, cy), :] = xr_e[side, i]
                ee[row_of(p, -2):row_of(p, 0), :] = cr_e[side, 0, i]
                ee[row_of(p, cy):row_of(p, cy + 2), :] = cr_e[side, 1, i]
            p = (-1, cx)[side]
            for c in range(chans):
                ff[c, row_of(p, 0):row_of(p, cy), :] = xr_f[side, c, 0]
                ff[c, row_of(p, -1):row_of(p, 0), :] = cr_f[side, 0, c, 0]
                ff[c, row_of(p, cy):row_of(p, cy + 1), :] = cr_f[side, 1, c, 0]
            k = (0, (cx + 2) * nb)[side]
            pack_flat(list(range(k, k + 2 * nb + 1)))
    start(z_e[1])
    start(z_f[1])
    deposit(3 * low, cx - 3 * high)

    recv(z_e[1])
    recv(z_f[1])
    for side in (0, 1):
        ghost(1, side)
    edges = []
    for has, (a, b) in ((low, (-1, 1)), (high, (cx - 1, cx + 1))):
        edges.append((has, a, b))
    for has, a, b in edges:
        @pl.when(has == 1)
        def _():
            blocks(zero + a, b, 6, count_body)
            blocks(zero + a, b, 6, weight_body)
            a2, b2 = (a, b + 1) if a < 0 else (a - 1, b)
            blocks(zero + a2, b2, 4, average_body)
            a3, b3 = (0, 3) if a < 0 else (cx - 3, cx)
            deposit(zero + a3, b3)
    for c in [x_f, x_e, y_e, y_f, c_e, c_f, z_e[1], z_f[1]]:
        sent(c)


def per_device(n, conserved, volume_fraction, cut_mask, merge_code):
    fields, cx, cy, cz = conserved.shape[1:]
    chans = fields + 1
    flat = PAD + (cx + 4) * (cy + 8) + 2 * (cy + 8) + 64
    f32, i32 = jnp.float32, jnp.int32
    V = pltpu.VMEM
    scratch = [
        V((flat, cz), i32), V((chans, flat, cz), f32), V((flat, cz), f32),
        V((3 * chans, flat, cz), f32), V((fields, flat, cz), f32),
        V((cx, cy, cz), i32), V((cx, cy, cz), i32), V((chans, cx, cy, cz), f32),
        V((2, cx, 2, cz), i32), V((2, chans, cx, 1, cz), f32),
        V((2, cx, 2, cz), i32), V((2, chans, cx, 1, cz), f32),
        V((2, 2, cy, cz), i32), V((2, 2, cy, cz), i32), V((2, chans, 1, cy, cz), f32),
        V((2, 2, 2, 2, cz), i32), V((2, 2, chans, 1, 1, cz), f32),
        V((2, 2, 8, cz), i32), V((2, chans, 8, cz), f32),
        V((2, 2, 2, 8, cz), i32), V((2, 2, chans, 8, cz), f32),
        V((2, 8, cz), f32), V((2, chans, 8, cz), f32), V((2, fields, 8, cz), f32),
        pltpu.SemaphoreType.DMA((4,)), pltpu.SemaphoreType.DMA((20,)), pltpu.SemaphoreType.DMA((20,)),
    ]
    return pl.pallas_call(
        functools.partial(kernel, n, (fields, cx, cy, cz)),
        out_shape=pltpu.VMEM(conserved.shape, f32),
        in_specs=[pl.BlockSpec(memory_space=pl.ANY)] * 4,
        out_specs=pl.BlockSpec(memory_space=pltpu.VMEM),
        scratch_shapes=scratch,
        compiler_params=pltpu.CompilerParams(
            collective_id=0, has_side_effects=True, vmem_limit_bytes=60 * 1024 * 1024),
        name="redistribute",
    )(conserved, volume_fraction, cut_mask, merge_code)


def solution(mesh):
    return jax.shard_map(
        functools.partial(per_device, mesh.shape["boxes"]),
        mesh=mesh,
        in_specs=(
            P("boxes", None, None, None, None),
            P("boxes", None, None, None),
            P("boxes", None, None, None),
            P("boxes", None, None, None),
        ),
        out_specs=P("boxes", None, None, None, None),
        check_vma=False,
    )
```

```python
import functools

import jax
import jax.numpy as jnp
from jax import lax
from jax.experimental import pallas as pl
from jax.experimental.pallas import tpu as pltpu
from jax.sharding import PartitionSpec as P

NBY = 4
NBZ = 4
MESH = pl.DeviceIdType.MESH
XP, XM, YP, YM, ZP, ZM = 1, 2, 4, 8, 16, 32
ONE, UP, DOWN = 10, 14, 18
NONE = 1 << ONE
PAD = 8
PAIRS = [(ax, ay) for ax in (0, 1, -1) for ay in (0, 1, -1)]


def flag(ax, ay, az=0):
    return (
        {1: XP, -1: XM, 0: 0}[ax] | {1: YP, -1: YM, 0: 0}[ay] | {1: ZP, -1: ZM, 0: 0}[az]
    )


def holds(e, bits):
    return (e & bits) == bits


def kernel(n, dims, u_ref, vf_ref, mask_ref, code_ref, out_ref, ee, ff, inv, w0, wp, wm, avg,
           raw_m, raw_c, raw_f, ys_e, ys_f, yr_e, yr_f, xs_e, xr_e, xr_f, cr_e, cr_f,
           zs_e, zs_f, zr_e, zr_f, inj_c, inj_w, inj_d, load_sem, send_sem, recv_sem):
    fields, cx, cy, cz = dims
    chans = fields + 1
    nb = cy // 8 + 1
    pitch = 8 * nb
    me = lax.axis_index("boxes")
    bx, by, bz = me // (NBY * NBZ), me // NBZ % NBY, me % NBZ
    axes = {
        "x": (NBY * NBZ, bx > 0, bx < n // (NBY * NBZ) - 1),
        "y": (NBZ, by > 0, by < NBY - 1),
        "z": (1, bz > 0, bz < NBZ - 1),
    }
    lane = lax.broadcasted_iota(jnp.int32, (8, cz), 1)
    sub = lax.broadcasted_iota(jnp.int32, (8, cz), 0)
    first, final = lane == 0, lane == cz - 1

    loads = [
        pltpu.make_async_copy(u_ref.at[0], raw_f.at[1:chans], load_sem.at[0]),
        pltpu.make_async_copy(vf_ref.at[0], raw_f.at[0], load_sem.at[1]),
        pltpu.make_async_copy(mask_ref.at[0], raw_m, load_sem.at[2]),
        pltpu.make_async_copy(code_ref.at[0], raw_c, load_sem.at[3]),
    ]
    for copy in loads:
        copy.start()

    barrier = pltpu.get_barrier_semaphore()
    total = jnp.int32(0)
    for stride, low, high in axes.values():
        for has, there in ((low, me - stride), (high, me + stride)):
            @pl.when(has)
            def _():
                pl.semaphore_signal(barrier, inc=1, device_id=(there,), device_id_type=MESH)
            total = total + has.astype(jnp.int32)
    def copies(axis, ident, up, down):
        stride = axes[axis][0]
        out = []
        for d, (pair, there) in enumerate(((up, me + stride), (down, me - stride))):
            out.append(pltpu.make_async_remote_copy(
                src_ref=pair[0], dst_ref=pair[1], send_sem=send_sem.at[2 * ident + d],
                recv_sem=recv_sem.at[2 * ident + d], device_id=(there,), device_id_type=MESH))
        return axis, out

    def start(c):
        axis, (up, down) = c
        _, low, high = axes[axis]
        pl.when(high)(lambda: up.start())
        pl.when(low)(lambda: down.start())

    def recv(c):
        axis, (up, down) = c
        _, low, high = axes[axis]
        pl.when(low)(lambda: up.wait_recv())
        pl.when(high)(lambda: down.wait_recv())

    def sent(c):
        axis, (up, down) = c
        _, low, high = axes[axis]
        pl.when(high)(lambda: up.wait_send())
        pl.when(low)(lambda: down.wait_send())

    x_f = copies("x", 0, (raw_f.at[:, cx - 1:cx], xr_f.at[0]), (raw_f.at[:, 0:1], xr_f.at[1]))
    x_e = copies("x", 1, (xs_e.at[1], xr_e.at[0]), (xs_e.at[0], xr_e.at[1]))
    y_e = copies("y", 2, (ys_e.at[0], yr_e.at[0]), (ys_e.at[1], yr_e.at[1]))
    y_f = copies("y", 3, (ys_f.at[0], yr_f.at[0]), (ys_f.at[1], yr_f.at[1]))
    c_e = copies("x", 4, (yr_e.at[:, cx - 2:cx], cr_e.at[0]), (yr_e.at[:, 0:2], cr_e.at[1]))
    c_f = copies("x", 5, (yr_f.at[:, :, cx - 1:cx], cr_f.at[0]), (yr_f.at[:, :, 0:1], cr_f.at[1]))
    z_e = [copies("z", 6 + t, (zs_e.at[1], zr_e.at[t, 0]), (zs_e.at[0], zr_e.at[t, 1])) for t in (0, 1)]
    z_f = [copies("z", 8 + t, (zs_f.at[1], zr_f.at[t, 0]), (zs_f.at[0], zr_f.at[t, 1])) for t in (0, 1)]

    for copy in loads:
        copy.wait()

    def row_of(p, y):
        return PAD + pitch * (p + 2) + 8 + y

    _, x_low, x_high = axes["x"]
    _, y_low, y_high = axes["y"]
    _, z_low, z_high = axes["z"]
    clear = lambda has, bits: jnp.where(has, 0, bits)
    row2 = lax.broadcasted_iota(jnp.int32, (cy, cz), 0)
    lane2 = lax.broadcasted_iota(jnp.int32, (cy, cz), 1)
    drop = (jnp.where(row2 == 0, clear(y_low, YM), 0) + jnp.where(row2 == cy - 1, clear(y_high, YP), 0)
            + jnp.where(lane2 == 0, clear(z_low, ZM + (1 << DOWN)), 0)
            + jnp.where(lane2 == cz - 1, clear(z_high, ZP + (1 << UP)), 0))
    keep = ~drop

    def encode(p, _):
        c = raw_c[p]
        cut = raw_m[p] == 1
        third = (c * 171) >> 9
        sz = c - 3 * third
        ninth = (third * 171) >> 9
        sy = third - 3 * ninth
        bit = lambda test, value: jnp.where(test, value, 0)
        e = (bit(ninth == 2, XP) + bit(ninth == 0, XM) + bit(sy == 2, YP) + bit(sy == 0, YM)
             + bit(sz == 2, ZP + (1 << UP)) + bit(sz == 0, ZM + (1 << DOWN)))
        off = jnp.where(p == 0, clear(x_low, XM), 0) + jnp.where(p == cx - 1, clear(x_high, XP), 0)
        ee[pl.ds(row_of(p, 0), cy), :] = (jnp.where(cut, e, 0) & keep & ~off) + NONE
        ys_e[0, p] = ee[pl.ds(row_of(p, cy - 2), 2), :]
        ys_e[1, p] = ee[pl.ds(row_of(p, 0), 2), :]
        return 0

    lax.fori_loop(0, cx, encode, 0)
    for i in range(2):
        xs_e[0, i] = ee[row_of(i, 0):row_of(i, cy), :]
        xs_e[1, i] = ee[row_of(cx - 2 + i, 0):row_of(cx - 2 + i, cy), :]
    for c in range(chans):
        ys_f[0, c] = raw_f[c, :, cy - 1:cy, :]
        ys_f[1, c] = raw_f[c, :, 0:1, :]

    @pl.when(jnp.logical_not(x_low))
    def _():
        a, b = PAD, row_of(-1, cy + 2)
        ee[a:b, :] = jnp.full((b - a, cz), NONE, jnp.int32)

    @pl.when(jnp.logical_not(x_high))
    def _():
        a, b = row_of(cx, -2), row_of(cx + 1, cy + 8)
        ee[a:b, :] = jnp.full((b - a, cz), NONE, jnp.int32)

    for side, has in enumerate((y_low, y_high)):
        @pl.when(jnp.logical_not(has))
        def _():
            yr_e[side] = jnp.full(yr_e.shape[1:], NONE, jnp.int32)
            yr_f[side] = jnp.zeros(yr_f.shape[1:], jnp.float32)
    for side, has in enumerate((z_low, z_high)):
        @pl.when(jnp.logical_not(has))
        def _():
            for t in (0, 1):
                zr_e[t, side] = jnp.full(zr_e.shape[2:], NONE, jnp.int32)
                zr_f[t, side] = jnp.zeros(zr_f.shape[2:], jnp.float32)

    def turn(v, amount):
        if isinstance(amount, int):
            return pltpu.roll(v, amount % cz, 1) if amount % cz else v
        return pltpu.roll(v, lax.rem(amount + cz, cz), 1)

    def pack(ks, e_of, f_of):
        here = [lane == k for k in ks]
        es = [e_of(i) for i in range(len(ks))]
        for side, shifts in enumerate(((0, -1), (1, 2))):
            for j in (0, 1):
                acc = zs_e[side, j]
                for k, at, e in zip(ks, here, es):
                    acc = jnp.where(at, turn(e, k + shifts[j]), acc)
                zs_e[side, j] = acc
        for c in range(chans):
            fs = [f_of(i, c) for i in range(len(ks))]
            for side in (0, 1):
                acc = zs_f[side, c]
                for k, at, f in zip(ks, here, fs):
                    acc = jnp.where(at, turn(f, k + side), acc)
                zs_f[side, c] = acc

    def pack_flat(ks):
        pack(ks, lambda i: ee[PAD + 8 * ks[i]:PAD + 8 * ks[i] + 8, :],
             lambda i, c: ff[c, PAD + 8 * ks[i]:PAD + 8 * ks[i] + 8, :])

    zs_e[...] = jnp.full(zs_e.shape, NONE, jnp.int32)
    zs_f[...] = jnp.zeros(zs_f.shape, jnp.float32)
    group = 4 if cx % 4 == 0 else 1

    def pack_own(i, _):
        ks, where = [], []
        for j in range(group):
            p = i * group + j
            for c in range(chans):
                ff[c, pl.ds(row_of(p, 0), cy), :] = raw_f[c, p]
            for b in range(nb - 1):
                ks.append((p + 2) * nb + 1 + b)
                where.append((p, b))
        pack(ks, lambda i: ee[pl.ds(PAD + 8 * ks[i], 8), :],
             lambda i, c: raw_f[c, where[i][0], 8 * where[i][1]:8 * where[i][1] + 8, :])
        return 0

    lax.fori_loop(0, cx // group, pack_own, 0)

    pl.semaphore_wait(barrier, total)
    start(y_e)
    start(x_f)
    start(y_f)
    start(x_e)

    recv(y_e)
    start(c_e)
    for p in range(cx):
        ee[row_of(p, -2):row_of(p, 0), :] = yr_e[0, p]
        ee[row_of(p, cy):row_of(p, cy + 2), :] = yr_e[1, p]
    recv(y_f)
    start(c_f)
    for p in range(cx):
        for c in range(chans):
            ff[c, row_of(p, -1):row_of(p, 0), :] = yr_f[0, c, p]
            ff[c, row_of(p, cy):row_of(p, cy + 1), :] = yr_f[1, c, p]
    between = [(p + 2) * nb for p in range(cx + 1)]
    pack_flat(between[:len(between) // 2])
    pack_flat(between[len(between) // 2:])
    start(z_e[0])
    start(z_f[0])

    zero = me // n

    def blocks(p0, p1, chunk, body):
        k0 = (p0 + 2) * nb
        steps = ((p1 - p0) * nb + chunk) // chunk

        def step(i, _):
            for j in range(chunk):
                k = k0 + i * chunk + j
                body(k, PAD + 8 * k)
            return 0

        lax.fori_loop(0, steps, step, 0)

    def rows(ref, lead, r):
        return ref[lead + (pl.ds(r, 8), slice(None))]

    def count_body(k, r):
        acc = rows(ee, (), r)
        for ax, ay in PAIRS[1:]:
            e = rows(ee, (), r - pitch * ax - ay)
            acc = acc + jnp.where(holds(e, flag(ax, ay)), e, 0)
        here = (acc >> ONE) & 15
        here = here + pltpu.roll((acc >> UP) & 15, 1, 1) + pltpu.roll((acc >> DOWN) & 15, cz - 1, 1)
        inv[pl.ds(r, 8), :] = 1.0 / here.astype(jnp.float32)

    def edge(ref, lead, k, side):
        return turn(ref[(side,) + lead], cz - side - k)

    def weight_body(k, r):
        i = rows(inv, (), r)
        i = jnp.where(first, edge(inj_c, (), k, 0), jnp.where(final, edge(inj_c, (), k, 1), i))
        inv[pl.ds(r, 8), :] = i
        w = rows(ff, (0,), r) * i
        for c in range(chans):
            w0[c, pl.ds(r, 8), :] = w if c == 0 else w * rows(ff, (c,), r)

    def shift_body(k, r):
        for c in range(chans):
            v = rows(w0, (c,), r)
            wp[c, pl.ds(r, 8), :] = v + jnp.where(final, edge(inj_w, (c,), k, 1), pltpu.roll(v, cz - 1, 1))
            wm[c, pl.ds(r, 8), :] = v + jnp.where(first, edge(inj_w, (c,), k, 0), pltpu.roll(v, 1, 1))

    def weights(p0, p1, chunk):
        k0 = (p0 + 2) * nb
        steps = ((p1 - p0) * nb + chunk) // chunk

        def step(i, _):
            before = k0 + jnp.maximum(i - 1, 0) * chunk
            for j in range(chunk):
                shift_body(before + j, PAD + 8 * (before + j))
            for j in range(chunk):
                k = k0 + i * chunk + j
                weight_body(k, PAD + 8 * k)
            return 0

        lax.fori_loop(0, steps + 1, step, 0)

    def average_body(k, r):
        e = rows(ee, (), r)
        m = {b: holds(e, b) for b in (XP, XM, YP, YM, ZP, ZM)}

        def along_z(c, q):
            return jnp.where(m[ZP], rows(wp, (c,), q), jnp.where(m[ZM], rows(wm, (c,), q), rows(w0, (c,), q)))

        def along_y(c, q):
            side = jnp.where(m[YP], along_z(c, q + 1), jnp.where(m[YM], along_z(c, q - 1), 0.0))
            return along_z(c, q) + side

        def whole(c):
            side = jnp.where(m[XP], along_y(c, r + pitch), jnp.where(m[XM], along_y(c, r - pitch), 0.0))
            return along_y(c, r) + side

        inverse = 1.0 / whole(0)
        for c in range(1, chans):
            avg[c - 1, pl.ds(r, 8), :] = whole(c) * inverse

    def deposit_body(p, b):
        k = (p + 2) * nb + 1 + b
        r = PAD + 8 * k
        acc = [[None] * 3 for _ in range(fields)]
        for ax, ay in PAIRS:
            s = r - pitch * ax - ay
            e = rows(ee, (), s)
            ms = [holds(e, flag(ax, ay, az)) for az in (0, 1, -1)]
            for f in range(fields):
                v = rows(avg, (f,), s)
                for i in range(3):
                    term = v if (ax, ay, i) == (0, 0, 0) else jnp.where(ms[i], v, 0.0)
                    acc[f][i] = term if acc[f][i] is None else acc[f][i] + term
        i = rows(inv, (), r)
        for f in range(fields):
            here, up, down = acc[f]
            here = here + jnp.where(first, edge(inj_d, (f,), k, 0), pltpu.roll(up, 1, 1))
            here = here + jnp.where(final, edge(inj_d, (f,), k, 1), pltpu.roll(down, cz - 1, 1))
            out_ref[0, f, p, 8 * b:8 * b + 8, :] = here * i

    def deposit(p0, p1):
        def plane(i, _):
            for b in range(nb - 1):
                deposit_body(p0 + i, b)
            return 0

        lax.fori_loop(0, p1 - p0, plane, 0)

    def shift_y(v, dy):
        if dy == 0:
            return v
        w = pltpu.roll(v, 7 if dy == 1 else 1, 0)
        return jnp.where(sub == (7 if dy == 1 else 0), turn(w, -dy), w)

    def shift_x(v, dx):
        return turn(v, -nb * dx) if dx else v

    def spread(t):
        lines = {ax: t[ax, 0] + shift_y(t[ax, 1], -1) + shift_y(t[ax, -1], 1) for ax in (0, 1, -1)}
        return lines[0] + shift_x(lines[1], -1) + shift_x(lines[-1], 1)

    def ghost(t, side):
        toward, away = (ZP, ZM) if side == 0 else (ZM, ZP)
        e0, e1, g0, g1 = zs_e[side, 0], zs_e[side, 1], zr_e[t, side, 0], zr_e[t, side, 1]
        from_g0 = jnp.where(holds(g0, toward), 257, 1)
        from_e0 = jnp.where(holds(e0, away), 257, 256)
        found = {}
        for ax, ay in PAIRS:
            b = flag(ax, ay)
            found[ax, ay] = (jnp.where(holds(g1, b | toward), 1, 0) + jnp.where(holds(g0, b), from_g0, 0)
                             + jnp.where(holds(e0, b), from_e0, 0) + jnp.where(holds(e1, b | away), 256, 0))
        found = spread(found)
        i_ghost = 1.0 / (found & 255).astype(jnp.float32)
        i_own = 1.0 / (found >> 8).astype(jnp.float32)
        inj_c[side] = i_own
        w_ghost, w_own = zr_f[t, side, 0] * i_ghost, zs_f[side, 0] * i_own
        m = {b: holds(g0, b) for b in (XP, XM, YP, YM)}
        mine = holds(g0, toward)
        inverse = None
        for c in range(chans):
            v = w_ghost if c == 0 else w_ghost * zr_f[t, side, c]
            inj_w[side, c] = v
            v = v + (w_own if c == 0 else w_own * zs_f[side, c])
            above, below = shift_y(v, 1), shift_y(v, -1)
            line = {dx: shift_x(v, dx) + jnp.where(m[YP], shift_x(above, dx), jnp.where(m[YM], shift_x(below, dx), 0.0))
                    for dx in (0, 1, -1)}
            whole = line[0] + jnp.where(m[XP], line[1], jnp.where(m[XM], line[-1], 0.0))
            if c == 0:
                inverse = 1.0 / whole
                continue
            a = jnp.where(mine, whole * inverse, 0.0)
            inj_d[side, c - 1] = spread({
                (ax, ay): jnp.where(holds(g0, flag(ax, ay)), a, 0.0) if (ax, ay) != (0, 0) else a
                for ax, ay in PAIRS})

    low, high = x_low.astype(jnp.int32), x_high.astype(jnp.int32)
    blocks(low, cx - high, 6, count_body)
    recv(z_e[0])
    recv(z_f[0])
    for side in (0, 1):
        ghost(0, side)
    weights(low, cx - high, 10)
    blocks(2 * low, cx - 2 * high, 5, average_body)

    for c in (x_f, x_e, c_e, c_f):
        recv(c)
    for c in (z_e[0], z_f[0]):
        sent(c)
    for side, has in enumerate((x_low, x_high)):
        @pl.when(has)
        def _():
            for i in range(2):
                p = (i - 2, cx + i)[side]
                ee[row_of(p, 0):row_of(p, cy), :] = xr_e[side, i]
                ee[row_of(p, -2):row_of(p, 0), :] = cr_e[side, 0, i]
                ee[row_of(p, cy):row_of(p, cy + 2), :] = cr_e[side, 1, i]
            p = (-1, cx)[side]
            for c in range(chans):
                ff[c, row_of(p, 0):row_of(p, cy), :] = xr_f[side, c, 0]
                ff[c, row_of(p, -1):row_of(p, 0), :] = cr_f[side, 0, c, 0]
                ff[c, row_of(p, cy):row_of(p, cy + 1), :] = cr_f[side, 1, c, 0]
            k = (0, (cx + 2) * nb)[side]
            pack_flat(list(range(k, k + 2 * nb + 1)))
    start(z_e[1])
    start(z_f[1])
    deposit(3 * low, cx - 3 * high)

    recv(z_e[1])
    recv(z_f[1])
    for side in (0, 1):
        ghost(1, side)
    edges = []
    for has, (a, b) in ((low, (-1, 1)), (high, (cx - 1, cx + 1))):
        edges.append((has, a, b))
    for has, a, b in edges:
        @pl.when(has == 1)
        def _():
            blocks(zero + a, b, 6, count_body)
            weights(zero + a, b, 6)
            a2, b2 = (a, b + 1) if a < 0 else (a - 1, b)
            blocks(zero + a2, b2, 4, average_body)
            a3, b3 = (0, 3) if a < 0 else (cx - 3, cx)
            deposit(zero + a3, b3)
    for c in [x_f, x_e, y_e, y_f, c_e, c_f, z_e[1], z_f[1]]:
        sent(c)


def per_device(n, conserved, volume_fraction, cut_mask, merge_code):
    fields, cx, cy, cz = conserved.shape[1:]
    chans = fields + 1
    flat = PAD + (cx + 4) * (cy + 8) + 2 * (cy + 8) + 64
    f32, i32 = jnp.float32, jnp.int32
    V = pltpu.VMEM
    scratch = [
        V((flat, cz), i32), V((chans, flat, cz), f32), V((flat, cz), f32),
        V((chans, flat, cz), f32), V((chans, flat, cz), f32), V((chans, flat, cz), f32),
        V((fields, flat, cz), f32),
        V((cx, cy, cz), i32), V((cx, cy, cz), i32), V((chans, cx, cy, cz), f32),
        V((2, cx, 2, cz), i32), V((2, chans, cx, 1, cz), f32),
        V((2, cx, 2, cz), i32), V((2, chans, cx, 1, cz), f32),
        V((2, 2, cy, cz), i32), V((2, 2, cy, cz), i32), V((2, chans, 1, cy, cz), f32),
        V((2, 2, 2, 2, cz), i32), V((2, 2, chans, 1, 1, cz), f32),
        V((2, 2, 8, cz), i32), V((2, chans, 8, cz), f32),
        V((2, 2, 2, 8, cz), i32), V((2, 2, chans, 8, cz), f32),
        V((2, 8, cz), f32), V((2, chans, 8, cz), f32), V((2, fields, 8, cz), f32),
        pltpu.SemaphoreType.DMA((4,)), pltpu.SemaphoreType.DMA((20,)), pltpu.SemaphoreType.DMA((20,)),
    ]
    return pl.pallas_call(
        functools.partial(kernel, n, (fields, cx, cy, cz)),
        out_shape=pltpu.VMEM(conserved.shape, f32),
        in_specs=[pl.BlockSpec(memory_space=pl.ANY)] * 4,
        out_specs=pl.BlockSpec(memory_space=pltpu.VMEM),
        scratch_shapes=scratch,
        compiler_params=pltpu.CompilerParams(
            collective_id=0, has_side_effects=True, vmem_limit_bytes=60 * 1024 * 1024),
        name="redistribute",
    )(conserved, volume_fraction, cut_mask, merge_code)


def solution(mesh):
    return jax.shard_map(
        functools.partial(per_device, mesh.shape["boxes"]),
        mesh=mesh,
        in_specs=(
            P("boxes", None, None, None, None),
            P("boxes", None, None, None),
            P("boxes", None, None, None),
            P("boxes", None, None, None),
        ),
        out_specs=P("boxes", None, None, None, None),
        check_vma=False,
    )
```

```python
import functools

import jax
import jax.numpy as jnp
from jax import lax
from jax.experimental import pallas as pl
from jax.experimental.pallas import tpu as pltpu
from jax.sharding import PartitionSpec as P

NBY = 4
NBZ = 4
MESH = pl.DeviceIdType.MESH
XP, XM, YP, YM, ZP, ZM = 1, 2, 4, 8, 16, 32
ONE, UP, DOWN = 10, 14, 18
NONE = 1 << ONE
PAD = 8
PAIRS = [(ax, ay) for ax in (0, 1, -1) for ay in (0, 1, -1)]


def flag(ax, ay, az=0):
    return (
        {1: XP, -1: XM, 0: 0}[ax] | {1: YP, -1: YM, 0: 0}[ay] | {1: ZP, -1: ZM, 0: 0}[az]
    )


def holds(e, bits):
    return (e & bits) == bits


def kernel(n, dims, u_ref, vf_ref, mask_ref, code_ref, out_ref, ee, ff, inv, w0, wp, wm, avg,
           raw_m, raw_c, raw_f, ys_e, ys_f, yr_e, yr_f, xs_e, xr_e, xr_f, cr_e, cr_f,
           zs_e, zs_f, zr_e, zr_f, ts_e, ts_f, tr_e, tr_f, two_c, two_w, two_d, inj_c, inj_w, inj_d, load_sem, send_sem, recv_sem):
    fields, cx, cy, cz = dims
    chans = fields + 1
    nb = cy // 8 + 1
    pitch = 8 * nb
    me = lax.axis_index("boxes")
    bx, by, bz = me // (NBY * NBZ), me // NBZ % NBY, me % NBZ
    axes = {
        "x": (NBY * NBZ, bx > 0, bx < n // (NBY * NBZ) - 1),
        "y": (NBZ, by > 0, by < NBY - 1),
        "z": (1, bz > 0, bz < NBZ - 1),
    }
    lane = lax.broadcasted_iota(jnp.int32, (8, cz), 1)
    sub = lax.broadcasted_iota(jnp.int32, (8, cz), 0)
    first, final = lane == 0, lane == cz - 1
    ends = jnp.logical_or(first, final)
    odd = (lane & 1) == 1
    slot = lane - nb * ((lane * (4096 // nb + 1)) >> 12)

    loads = [
        pltpu.make_async_copy(u_ref.at[0], raw_f.at[1:chans], load_sem.at[0]),
        pltpu.make_async_copy(vf_ref.at[0], raw_f.at[0], load_sem.at[1]),
        pltpu.make_async_copy(mask_ref.at[0], raw_m, load_sem.at[2]),
        pltpu.make_async_copy(code_ref.at[0], raw_c, load_sem.at[3]),
    ]
    for copy in loads:
        copy.start()

    barrier = pltpu.get_barrier_semaphore()
    total = jnp.int32(0)
    for stride, low, high in axes.values():
        for has, there in ((low, me - stride), (high, me + stride)):
            @pl.when(has)
            def _():
                pl.semaphore_signal(barrier, inc=1, device_id=(there,), device_id_type=MESH)
            total = total + has.astype(jnp.int32)
    def copies(axis, ident, up, down):
        stride = axes[axis][0]
        out = []
        for d, (pair, there) in enumerate(((up, me + stride), (down, me - stride))):
            out.append(pltpu.make_async_remote_copy(
                src_ref=pair[0], dst_ref=pair[1], send_sem=send_sem.at[2 * ident + d],
                recv_sem=recv_sem.at[2 * ident + d], device_id=(there,), device_id_type=MESH))
        return axis, out

    def start(c):
        axis, (up, down) = c
        _, low, high = axes[axis]
        pl.when(high)(lambda: up.start())
        pl.when(low)(lambda: down.start())

    def recv(c):
        axis, (up, down) = c
        _, low, high = axes[axis]
        pl.when(low)(lambda: up.wait_recv())
        pl.when(high)(lambda: down.wait_recv())

    def sent(c):
        axis, (up, down) = c
        _, low, high = axes[axis]
        pl.when(high)(lambda: up.wait_send())
        pl.when(low)(lambda: down.wait_send())

    x_f = copies("x", 0, (raw_f.at[:, cx - 1:cx], xr_f.at[0]), (raw_f.at[:, 0:1], xr_f.at[1]))
    x_e = copies("x", 1, (xs_e.at[1], xr_e.at[0]), (xs_e.at[0], xr_e.at[1]))
    y_e = copies("y", 2, (ys_e.at[0], yr_e.at[0]), (ys_e.at[1], yr_e.at[1]))
    y_f = copies("y", 3, (ys_f.at[0], yr_f.at[0]), (ys_f.at[1], yr_f.at[1]))
    c_e = copies("x", 4, (yr_e.at[:, cx - 2:cx], cr_e.at[0]), (yr_e.at[:, 0:2], cr_e.at[1]))
    c_f = copies("x", 5, (yr_f.at[:, :, cx - 1:cx], cr_f.at[0]), (yr_f.at[:, :, 0:1], cr_f.at[1]))
    z_e = [copies("z", 6 + t, (zs_e.at[1], zr_e.at[t, 0]), (zs_e.at[0], zr_e.at[t, 1])) for t in (0, 1)]
    t_e = copies("y", 10, (ts_e.at[0], tr_e.at[0]), (ts_e.at[1], tr_e.at[1]))
    t_f = copies("y", 11, (ts_f.at[0], tr_f.at[0]), (ts_f.at[1], tr_f.at[1]))
    z_f = [copies("z", 8 + t, (zs_f.at[1], zr_f.at[t, 0]), (zs_f.at[0], zr_f.at[t, 1])) for t in (0, 1)]

    loads[0].wait()
    loads[1].wait()
    for c in range(chans):
        ys_f[0, c] = raw_f[c, :, cy - 1:cy, :]
        ys_f[1, c] = raw_f[c, :, 0:1, :]
    pl.semaphore_wait(barrier, total)
    start(y_f)
    start(x_f)
    loads[2].wait()
    loads[3].wait()

    def row_of(p, y):
        return PAD + pitch * (p + 2) + 8 + y

    _, x_low, x_high = axes["x"]
    _, y_low, y_high = axes["y"]
    _, z_low, z_high = axes["z"]
    clear = lambda has, bits: jnp.where(has, 0, bits)
    row2 = lax.broadcasted_iota(jnp.int32, (cy, cz), 0)
    lane2 = lax.broadcasted_iota(jnp.int32, (cy, cz), 1)
    drop = (jnp.where(row2 == 0, clear(y_low, YM), 0) + jnp.where(row2 == cy - 1, clear(y_high, YP), 0)
            + jnp.where(lane2 == 0, clear(z_low, ZM + (1 << DOWN)), 0)
            + jnp.where(lane2 == cz - 1, clear(z_high, ZP + (1 << UP)), 0))
    keep = ~drop

    def encode(p, _):
        c = raw_c[p]
        cut = raw_m[p] == 1
        third = (c * 171) >> 9
        sz = c - 3 * third
        ninth = (third * 171) >> 9
        sy = third - 3 * ninth
        bit = lambda test, value: jnp.where(test, value, 0)
        e = (bit(ninth == 2, XP) + bit(ninth == 0, XM) + bit(sy == 2, YP) + bit(sy == 0, YM)
             + bit(sz == 2, ZP + (1 << UP)) + bit(sz == 0, ZM + (1 << DOWN)))
        off = jnp.where(p == 0, clear(x_low, XM), 0) + jnp.where(p == cx - 1, clear(x_high, XP), 0)
        ee[pl.ds(row_of(p, 0), cy), :] = (jnp.where(cut, e, 0) & keep & ~off) + NONE
        ys_e[0, p] = ee[pl.ds(row_of(p, cy - 2), 2), :]
        ys_e[1, p] = ee[pl.ds(row_of(p, 0), 2), :]
        return 0

    lax.fori_loop(0, cx, encode, 0)
    start(y_e)
    for i in range(2):
        xs_e[0, i] = ee[row_of(i, 0):row_of(i, cy), :]
        xs_e[1, i] = ee[row_of(cx - 2 + i, 0):row_of(cx - 2 + i, cy), :]
    start(x_e)

    @pl.when(jnp.logical_not(x_low))
    def _():
        a, b = PAD, row_of(-1, cy + 2)
        ee[a:b, :] = jnp.full((b - a, cz), NONE, jnp.int32)

    @pl.when(jnp.logical_not(x_high))
    def _():
        a, b = row_of(cx, -2), row_of(cx + 1, cy + 8)
        ee[a:b, :] = jnp.full((b - a, cz), NONE, jnp.int32)

    for side, has in enumerate((y_low, y_high)):
        @pl.when(jnp.logical_not(has))
        def _():
            yr_e[side] = jnp.full(yr_e.shape[1:], NONE, jnp.int32)
            yr_f[side] = jnp.zeros(yr_f.shape[1:], jnp.float32)
    for side, has in enumerate((z_low, z_high)):
        @pl.when(jnp.logical_not(has))
        def _():
            for t in (0, 1):
                zr_e[t, side] = jnp.full(zr_e.shape[2:], NONE, jnp.int32)
                zr_f[t, side] = jnp.zeros(zr_f.shape[2:], jnp.float32)

    def turn(v, amount):
        if isinstance(amount, int):
            return pltpu.roll(v, amount % cz, 1) if amount % cz else v
        return pltpu.roll(v, lax.rem(amount + cz, cz), 1)

    shifts = ((0, 1), (-1, -2))

    def pack(ks, e_of, f_of):
        at = [{d: lane == (k + d) % cz if isinstance(k, int) else lane == k + d for d in (-2, -1, 0, 1)} for k in ks]
        acc = {(side, j): zs_e[side, j] for side in (0, 1) for j in (0, 1)}
        for i, k in enumerate(ks):
            e = turn(e_of(i), k)
            for side, j in acc:
                acc[side, j] = jnp.where(at[i][shifts[side][j]], e, acc[side, j])
        for side, j in acc:
            zs_e[side, j] = acc[side, j]
        for c in range(chans):
            acc = [zs_f[side, c] for side in (0, 1)]
            for i, k in enumerate(ks):
                f = turn(f_of(i, c), k)
                acc = [jnp.where(at[i][shifts[side][0]], f, acc[side]) for side in (0, 1)]
            for side in (0, 1):
                zs_f[side, c] = acc[side]

    def settle(t):
        for side in (0, 1):
            for j in (0, 1):
                zr_e[t, side, j] = turn(zr_e[t, side, j], -shifts[1 - side][j])
            for c in range(chans):
                zr_f[t, side, c] = turn(zr_f[t, side, c], -shifts[1 - side][0])

    def pack_flat(ks):
        pack(ks, lambda i: ee[PAD + 8 * ks[i]:PAD + 8 * ks[i] + 8, :],
             lambda i, c: ff[c, PAD + 8 * ks[i]:PAD + 8 * ks[i] + 8, :])

    zs_e[...] = jnp.full(zs_e.shape, NONE, jnp.int32)
    zs_f[...] = jnp.zeros(zs_f.shape, jnp.float32)
    group = 4 if cx % 4 == 0 else 1

    def pack_own(i, _):
        ks, where = [], []
        for j in range(group):
            p = i * group + j
            for c in range(chans):
                ff[c, pl.ds(row_of(p, 0), cy), :] = raw_f[c, p]
            for b in range(nb - 1):
                ks.append((p + 2) * nb + 1 + b)
                where.append((p, b))
        pack(ks, lambda i: ee[pl.ds(PAD + 8 * ks[i], 8), :],
             lambda i, c: raw_f[c, where[i][0], 8 * where[i][1]:8 * where[i][1] + 8, :])
        return 0

    lax.fori_loop(0, cx // group, pack_own, 0)
    start(z_e[0])
    start(z_f[0])


    recv(z_e[0])
    recv(z_f[0])
    settle(0)
    for d, source, direct in ((0, nb - 1, sub >= 4), (1, 1, sub < 4)):
        for side in (0, 1):
            ts_e[d, side] = jnp.where(slot == 0, turn(zr_e[0, side, 0], -source), turn(zr_e[0, side, 1], 1 - source))
            line = [None, None]
            for c in range(chans):
                v = turn(zr_f[0, side, c], c % 4 - source)
                line[c // 4] = v if c % 4 == 0 else jnp.where(slot == c % 4, v, line[c // 4])
            ts_f[d, side] = jnp.where(direct, line[0], pltpu.roll(line[1], 4, 0))
    start(t_e)
    start(t_f)

    recv(y_e)
    start(c_e)
    for p in range(cx):
        ee[row_of(p, -2):row_of(p, 0), :] = yr_e[0, p]
        ee[row_of(p, cy):row_of(p, cy + 2), :] = yr_e[1, p]
    recv(y_f)
    start(c_f)
    for p in range(cx):
        for c in range(chans):
            ff[c, row_of(p, -1):row_of(p, 0), :] = yr_f[0, c, p]
            ff[c, row_of(p, cy):row_of(p, cy + 1), :] = yr_f[1, c, p]
    for c in (z_e[0], z_f[0]):
        sent(c)
    pack_flat([(p + 2) * nb for p in range(cx + 1)])

    zero = me // n

    def blocks(p0, p1, chunk, body):
        k0 = (p0 + 2) * nb
        steps = ((p1 - p0) * nb + chunk) // chunk

        def step(i, _):
            for j in range(chunk):
                k = k0 + i * chunk + j
                body(k, PAD + 8 * k)
            return 0

        lax.fori_loop(0, steps, step, 0)

    def rows(ref, lead, r):
        return ref[lead + (pl.ds(r, 8), slice(None))]

    def count_body(k, r):
        acc = rows(ee, (), r)
        for ax, ay in PAIRS[1:]:
            e = rows(ee, (), r - pitch * ax - ay)
            acc = acc + jnp.where(holds(e, flag(ax, ay)), e, 0)
        here = (acc >> ONE) & 15
        here = here + pltpu.roll((acc >> UP) & 15, 1, 1) + pltpu.roll((acc >> DOWN) & 15, cz - 1, 1)
        inv[pl.ds(r, 8), :] = 1.0 / here.astype(jnp.float32)

    def edge(ref, lead, k):
        return turn(ref[(lax.rem(k, 2),) + lead], cz - k)

    def weight_body(k, r):
        i = rows(inv, (), r)
        i = jnp.where(ends, edge(inj_c, (), k), i)
        inv[pl.ds(r, 8), :] = i
        w = rows(ff, (0,), r) * i
        for c in range(chans):
            w0[c, pl.ds(r, 8), :] = w if c == 0 else w * rows(ff, (c,), r)

    def shift_body(k, r):
        for c in range(chans):
            v, g = rows(w0, (c,), r), edge(inj_w, (c,), k)
            wp[c, pl.ds(r, 8), :] = v + jnp.where(final, g, pltpu.roll(v, cz - 1, 1))
            wm[c, pl.ds(r, 8), :] = v + jnp.where(first, g, pltpu.roll(v, 1, 1))

    def weights(p0, p1, chunk):
        k0 = (p0 + 2) * nb
        steps = ((p1 - p0) * nb + chunk) // chunk

        def step(i, _):
            before = k0 + jnp.maximum(i - 1, 0) * chunk
            for j in range(chunk):
                shift_body(before + j, PAD + 8 * (before + j))
            for j in range(chunk):
                k = k0 + i * chunk + j
                weight_body(k, PAD + 8 * k)
            return 0

        lax.fori_loop(0, steps + 1, step, 0)

    def average_body(k, r):
        e = rows(ee, (), r)
        m = {b: holds(e, b) for b in (XP, XM, YP, YM, ZP, ZM)}

        def along_z(c, q):
            return jnp.where(m[ZP], rows(wp, (c,), q), jnp.where(m[ZM], rows(wm, (c,), q), rows(w0, (c,), q)))

        def along_y(c, q):
            side = jnp.where(m[YP], along_z(c, q + 1), jnp.where(m[YM], along_z(c, q - 1), 0.0))
            return along_z(c, q) + side

        def whole(c):
            side = jnp.where(m[XP], along_y(c, r + pitch), jnp.where(m[XM], along_y(c, r - pitch), 0.0))
            return along_y(c, r) + side

        inverse = 1.0 / whole(0)
        for c in range(1, chans):
            avg[c - 1, pl.ds(r, 8), :] = whole(c) * inverse

    def deposit_body(p, b):
        k = (p + 2) * nb + 1 + b
        r = PAD + 8 * k
        acc = [[None] * 3 for _ in range(fields)]
        for ax, ay in PAIRS:
            s = r - pitch * ax - ay
            e = rows(ee, (), s)
            ms = [holds(e, flag(ax, ay, az)) for az in (0, 1, -1)]
            for f in range(fields):
                v = rows(avg, (f,), s)
                for i in range(3):
                    term = v if (ax, ay, i) == (0, 0, 0) else jnp.where(ms[i], v, 0.0)
                    acc[f][i] = term if acc[f][i] is None else acc[f][i] + term
        i = rows(inv, (), r)
        for f in range(fields):
            here, up, down = acc[f]
            g = edge(inj_d, (f,), k)
            here = here + jnp.where(first, g, pltpu.roll(up, 1, 1))
            here = here + jnp.where(final, g, pltpu.roll(down, cz - 1, 1))
            out_ref[0, f, p, 8 * b:8 * b + 8, :] = here * i

    def deposit(p0, p1):
        def plane(i, _):
            for b in range(nb - 1):
                deposit_body(p0 + i, b)
            return 0

        lax.fori_loop(0, p1 - p0, plane, 0)

    def shift_y(v, dy):
        if dy == 0:
            return v
        w = pltpu.roll(v, 7 if dy == 1 else 1, 0)
        return jnp.where(sub == (7 if dy == 1 else 0), turn(w, -dy), w)

    def shift_x(v, dx):
        return turn(v, -nb * dx) if dx else v

    def spread(t):
        lines = {ax: t[ax, 0] + shift_y(t[ax, 1], -1) + shift_y(t[ax, -1], 1) for ax in (0, 1, -1)}
        return lines[0] + shift_x(lines[1], -1) + shift_x(lines[-1], 1)

    def ghost(t, side):
        toward, away = (ZP, ZM) if side == 0 else (ZM, ZP)
        e0, e1 = (turn(zs_e[side, j], -shifts[side][j]) for j in (0, 1))
        g0, g1 = zr_e[t, side, 0], zr_e[t, side, 1]
        own = [turn(zs_f[side, c], -shifts[side][0]) for c in range(chans)]
        from_g0 = jnp.where(holds(g0, toward), 257, 1)
        from_e0 = jnp.where(holds(e0, away), 257, 256)
        found = {}
        for ax, ay in PAIRS:
            b = flag(ax, ay)
            found[ax, ay] = (jnp.where(holds(g1, b | toward), 1, 0) + jnp.where(holds(g0, b), from_g0, 0)
                             + jnp.where(holds(e0, b), from_e0, 0) + jnp.where(holds(e1, b | away), 256, 0))
        found = spread(found)
        i_ghost = 1.0 / (found & 255).astype(jnp.float32)
        i_own = 1.0 / (found >> 8).astype(jnp.float32)
        two_c[side] = i_own
        w_ghost, w_own = zr_f[t, side, 0] * i_ghost, own[0] * i_own
        m = {b: holds(g0, b) for b in (XP, XM, YP, YM)}
        mine = holds(g0, toward)
        inverse = None
        for c in range(chans):
            v = w_ghost if c == 0 else w_ghost * zr_f[t, side, c]
            two_w[side, c] = v
            v = v + (w_own if c == 0 else w_own * own[c])
            above, below = shift_y(v, 1), shift_y(v, -1)
            line = {dx: shift_x(v, dx) + jnp.where(m[YP], shift_x(above, dx), jnp.where(m[YM], shift_x(below, dx), 0.0))
                    for dx in (0, 1, -1)}
            whole = line[0] + jnp.where(m[XP], line[1], jnp.where(m[XM], line[-1], 0.0))
            if c == 0:
                inverse = 1.0 / whole
                continue
            a = jnp.where(mine, whole * inverse, 0.0)
            two_d[side, c - 1] = spread({
                (ax, ay): jnp.where(holds(g0, flag(ax, ay)), a, 0.0) if (ax, ay) != (0, 0) else a
                for ax, ay in PAIRS})

    def ghosts(t):
        for side in (0, 1):
            ghost(t, side)
        pairs = [(two_c, inj_c, ())] + [(two_w, inj_w, (c,)) for c in range(chans)]
        for two, inj, lead in pairs + [(two_d, inj_d, (f,)) for f in range(fields)]:
            below, above = two[(0,) + lead], turn(two[(1,) + lead], -1)
            inj[(0,) + lead] = jnp.where(odd, above, below)
            inj[(1,) + lead] = jnp.where(odd, below, above)

    low, high = x_low.astype(jnp.int32), x_high.astype(jnp.int32)
    blocks(low, cx - high, 6, count_body)
    recv(t_e)
    recv(t_f)
    for i, (has, rows_of) in enumerate(((y_low, sub >= 4), (y_high, sub < 4))):
        @pl.when(has)
        def _():
            at = jnp.logical_and(slot == 0, rows_of)
            for side in (0, 1):
                for j in (0, 1):
                    zr_e[0, side, j] = jnp.where(at, turn(tr_e[i, side], nb * i - j), zr_e[0, side, j])
                for c in range(chans):
                    v = turn(tr_f[i, side], nb * i - c % 4)
                    v = v if c < 4 else pltpu.roll(v, 4, 0)
                    zr_f[0, side, c] = jnp.where(at, v, zr_f[0, side, c])
    ghosts(0)
    weights(low, cx - high, 10)
    blocks(2 * low, cx - 2 * high, 5, average_body)

    for c in (x_f, x_e, c_e, c_f):
        recv(c)
    for side, has in enumerate((x_low, x_high)):
        @pl.when(has)
        def _():
            for i in range(2):
                p = (i - 2, cx + i)[side]
                ee[row_of(p, 0):row_of(p, cy), :] = xr_e[side, i]
                ee[row_of(p, -2):row_of(p, 0), :] = cr_e[side, 0, i]
                ee[row_of(p, cy):row_of(p, cy + 2), :] = cr_e[side, 1, i]
            p = (-1, cx)[side]
            for c in range(chans):
                ff[c, row_of(p, 0):row_of(p, cy), :] = xr_f[side, c, 0]
                ff[c, row_of(p, -1):row_of(p, 0), :] = cr_f[side, 0, c, 0]
                ff[c, row_of(p, cy):row_of(p, cy + 1), :] = cr_f[side, 1, c, 0]
            k = (0, (cx + 2) * nb)[side]
            pack_flat(list(range(k, k + 2 * nb + 1)))
    start(z_e[1])
    start(z_f[1])
    deposit(3 * low, cx - 3 * high)

    recv(z_e[1])
    recv(z_f[1])
    settle(1)
    ghosts(1)
    edges = []
    for has, (a, b) in ((low, (-1, 1)), (high, (cx - 1, cx + 1))):
        edges.append((has, a, b))
    for has, a, b in edges:
        @pl.when(has == 1)
        def _():
            blocks(zero + a, b, 6, count_body)
            weights(zero + a, b, 6)
            a2, b2 = (a, b + 1) if a < 0 else (a - 1, b)
            blocks(zero + a2, b2, 4, average_body)
            a3, b3 = (0, 3) if a < 0 else (cx - 3, cx)
            deposit(zero + a3, b3)
    for c in [x_f, x_e, y_e, y_f, c_e, c_f, t_e, t_f, z_e[1], z_f[1]]:
        sent(c)


def per_device(n, conserved, volume_fraction, cut_mask, merge_code):
    fields, cx, cy, cz = conserved.shape[1:]
    chans = fields + 1
    flat = PAD + (cx + 4) * (cy + 8) + 2 * (cy + 8) + 64
    f32, i32 = jnp.float32, jnp.int32
    V = pltpu.VMEM
    scratch = [
        V((flat, cz), i32), V((chans, flat, cz), f32), V((flat, cz), f32),
        V((chans, flat, cz), f32), V((chans, flat, cz), f32), V((chans, flat, cz), f32),
        V((fields, flat, cz), f32),
        V((cx, cy, cz), i32), V((cx, cy, cz), i32), V((chans, cx, cy, cz), f32),
        V((2, cx, 2, cz), i32), V((2, chans, cx, 1, cz), f32),
        V((2, cx, 2, cz), i32), V((2, chans, cx, 1, cz), f32),
        V((2, 2, cy, cz), i32), V((2, 2, cy, cz), i32), V((2, chans, 1, cy, cz), f32),
        V((2, 2, 2, 2, cz), i32), V((2, 2, chans, 1, 1, cz), f32),
        V((2, 2, 8, cz), i32), V((2, chans, 8, cz), f32),
        V((2, 2, 2, 8, cz), i32), V((2, 2, chans, 8, cz), f32),
        V((2, 2, 8, cz), i32), V((2, 2, 8, cz), f32), V((2, 2, 8, cz), i32), V((2, 2, 8, cz), f32),
        V((2, 8, cz), f32), V((2, chans, 8, cz), f32), V((2, fields, 8, cz), f32),
        V((2, 8, cz), f32), V((2, chans, 8, cz), f32), V((2, fields, 8, cz), f32),
        pltpu.SemaphoreType.DMA((4,)), pltpu.SemaphoreType.DMA((24,)), pltpu.SemaphoreType.DMA((24,)),
    ]
    return pl.pallas_call(
        functools.partial(kernel, n, (fields, cx, cy, cz)),
        out_shape=pltpu.VMEM(conserved.shape, f32),
        in_specs=[pl.BlockSpec(memory_space=pl.ANY)] * 4,
        out_specs=pl.BlockSpec(memory_space=pltpu.VMEM),
        scratch_shapes=scratch,
        compiler_params=pltpu.CompilerParams(
            collective_id=0, has_side_effects=True, vmem_limit_bytes=60 * 1024 * 1024),
        name="redistribute",
    )(conserved, volume_fraction, cut_mask, merge_code)


def solution(mesh):
    return jax.shard_map(
        functools.partial(per_device, mesh.shape["boxes"]),
        mesh=mesh,
        in_specs=(
            P("boxes", None, None, None, None),
            P("boxes", None, None, None),
            P("boxes", None, None, None),
            P("boxes", None, None, None),
        ),
        out_specs=P("boxes", None, None, None, None),
        check_vma=False,
    )
```

```python
import functools

import jax
import jax.numpy as jnp
from jax import lax
from jax.experimental import pallas as pl
from jax.experimental.pallas import tpu as pltpu
from jax.sharding import PartitionSpec as P

NBY = 4
NBZ = 4
MESH = pl.DeviceIdType.MESH
XP, XM, YP, YM, ZP, ZM = 1, 2, 4, 8, 16, 32
ONE, UP, DOWN = 10, 14, 18
NONE = 1 << ONE
PAD = 8
PAIRS = [(ax, ay) for ax in (0, 1, -1) for ay in (0, 1, -1)]


def flag(ax, ay, az=0):
    return (
        {1: XP, -1: XM, 0: 0}[ax] | {1: YP, -1: YM, 0: 0}[ay] | {1: ZP, -1: ZM, 0: 0}[az]
    )


def holds(e, bits):
    return (e & bits) == bits


def kernel(n, dims, u_ref, vf_ref, mask_ref, code_ref, out_ref, ee, ff, inv, w0, wp, wm, avg,
           raw_m, raw_c, raw_f, ys_e, ys_f, yr_e, yr_f, xs_e, xr_e, xr_f, cr_e, cr_f,
           zs_e, zs_f, zr_e, zr_f, ts_e, ts_f, tr_e, tr_f, two_c, two_w, two_d, inj_c, inj_w, inj_d, load_sem, send_sem, recv_sem):
    fields, cx, cy, cz = dims
    chans = fields + 1
    nb = cy // 8 + 1
    pitch = 8 * nb
    me = lax.axis_index("boxes")
    bx, by, bz = me // (NBY * NBZ), me // NBZ % NBY, me % NBZ
    axes = {
        "x": (NBY * NBZ, bx > 0, bx < n // (NBY * NBZ) - 1),
        "y": (NBZ, by > 0, by < NBY - 1),
        "z": (1, bz > 0, bz < NBZ - 1),
    }
    lane = lax.broadcasted_iota(jnp.int32, (8, cz), 1)
    sub = lax.broadcasted_iota(jnp.int32, (8, cz), 0)
    first, final = lane == 0, lane == cz - 1
    ends = jnp.logical_or(first, final)
    odd = (lane & 1) == 1
    slot = lane - nb * ((lane * (4096 // nb + 1)) >> 12)

    loads = [
        pltpu.make_async_copy(u_ref.at[0], raw_f.at[1:chans], load_sem.at[0]),
        pltpu.make_async_copy(vf_ref.at[0], raw_f.at[0], load_sem.at[1]),
        pltpu.make_async_copy(mask_ref.at[0], raw_m, load_sem.at[2]),
        pltpu.make_async_copy(code_ref.at[0], raw_c, load_sem.at[3]),
    ]
    for copy in loads:
        copy.start()

    barrier = pltpu.get_barrier_semaphore()
    total = jnp.int32(0)
    for stride, low, high in axes.values():
        for has, there in ((low, me - stride), (high, me + stride)):
            @pl.when(has)
            def _():
                pl.semaphore_signal(barrier, inc=1, device_id=(there,), device_id_type=MESH)
            total = total + has.astype(jnp.int32)
    for dy in (1, -1):
        for dz in (-1, 1):
            has = jnp.logical_and(axes["y"][1 + (dy == 1)], axes["z"][1 + (dz == 1)])
            @pl.when(has)
            def _():
                pl.semaphore_signal(barrier, inc=1, device_id=(me + NBZ * dy + dz,), device_id_type=MESH)
            total = total + has.astype(jnp.int32)
    def copies(axis, ident, up, down):
        stride = axes[axis][0]
        out = []
        for d, (pair, there) in enumerate(((up, me + stride), (down, me - stride))):
            out.append(pltpu.make_async_remote_copy(
                src_ref=pair[0], dst_ref=pair[1], send_sem=send_sem.at[2 * ident + d],
                recv_sem=recv_sem.at[2 * ident + d], device_id=(there,), device_id_type=MESH))
        return axis, out

    def start(c):
        axis, (up, down) = c
        _, low, high = axes[axis]
        pl.when(high)(lambda: up.start())
        pl.when(low)(lambda: down.start())

    def recv(c):
        axis, (up, down) = c
        _, low, high = axes[axis]
        pl.when(low)(lambda: up.wait_recv())
        pl.when(high)(lambda: down.wait_recv())

    def sent(c):
        axis, (up, down) = c
        _, low, high = axes[axis]
        pl.when(high)(lambda: up.wait_send())
        pl.when(low)(lambda: down.wait_send())

    x_f = copies("x", 0, (raw_f.at[:, cx - 1:cx], xr_f.at[0]), (raw_f.at[:, 0:1], xr_f.at[1]))
    x_e = copies("x", 1, (xs_e.at[1], xr_e.at[0]), (xs_e.at[0], xr_e.at[1]))
    y_e = copies("y", 2, (ys_e.at[0], yr_e.at[0]), (ys_e.at[1], yr_e.at[1]))
    y_f = copies("y", 3, (ys_f.at[0], yr_f.at[0]), (ys_f.at[1], yr_f.at[1]))
    c_e = copies("x", 4, (yr_e.at[:, cx - 2:cx], cr_e.at[0]), (yr_e.at[:, 0:2], cr_e.at[1]))
    c_f = copies("x", 5, (yr_f.at[:, :, cx - 1:cx], cr_f.at[0]), (yr_f.at[:, :, 0:1], cr_f.at[1]))
    z_e = [copies("z", 6 + t, (zs_e.at[1], zr_e.at[t, 0]), (zs_e.at[0], zr_e.at[t, 1])) for t in (0, 1)]
    z_f = [copies("z", 8 + t, (zs_f.at[1], zr_f.at[t, 0]), (zs_f.at[0], zr_f.at[t, 1])) for t in (0, 1)]

    loads[0].wait()
    loads[1].wait()
    for c in range(chans):
        ys_f[0, c] = raw_f[c, :, cy - 1:cy, :]
        ys_f[1, c] = raw_f[c, :, 0:1, :]
    pl.semaphore_wait(barrier, total)
    start(y_f)
    start(x_f)
    loads[2].wait()
    loads[3].wait()

    diagonal = []
    for d, dy in enumerate((1, -1)):
        for side, dz in enumerate((-1, 1)):
            to = jnp.logical_and(axes["y"][1 + (dy == 1)], axes["z"][1 + (dz == 1)])
            frm = jnp.logical_and(axes["y"][1 + (dy == -1)], axes["z"][1 + (dz == -1)])
            for ts, tr in ((ts_e, tr_e), (ts_f, tr_f)):
                at = 20 + len(diagonal)
                diagonal.append((to, frm, pltpu.make_async_remote_copy(
                    src_ref=ts.at[d, side], dst_ref=tr.at[d, 1 - side], send_sem=send_sem.at[at],
                    recv_sem=recv_sem.at[at], device_id=(me + NBZ * dy + dz,), device_id_type=MESH)))

    def row_of(p, y):
        return PAD + pitch * (p + 2) + 8 + y

    _, x_low, x_high = axes["x"]
    _, y_low, y_high = axes["y"]
    _, z_low, z_high = axes["z"]
    clear = lambda has, bits: jnp.where(has, 0, bits)
    row2 = lax.broadcasted_iota(jnp.int32, (cy, cz), 0)
    lane2 = lax.broadcasted_iota(jnp.int32, (cy, cz), 1)
    drop = (jnp.where(row2 == 0, clear(y_low, YM), 0) + jnp.where(row2 == cy - 1, clear(y_high, YP), 0)
            + jnp.where(lane2 == 0, clear(z_low, ZM + (1 << DOWN)), 0)
            + jnp.where(lane2 == cz - 1, clear(z_high, ZP + (1 << UP)), 0))
    keep = ~drop

    def encode(p, _):
        c = raw_c[p]
        cut = raw_m[p] == 1
        third = (c * 171) >> 9
        sz = c - 3 * third
        ninth = (third * 171) >> 9
        sy = third - 3 * ninth
        bit = lambda test, value: jnp.where(test, value, 0)
        e = (bit(ninth == 2, XP) + bit(ninth == 0, XM) + bit(sy == 2, YP) + bit(sy == 0, YM)
             + bit(sz == 2, ZP + (1 << UP)) + bit(sz == 0, ZM + (1 << DOWN)))
        off = jnp.where(p == 0, clear(x_low, XM), 0) + jnp.where(p == cx - 1, clear(x_high, XP), 0)
        ee[pl.ds(row_of(p, 0), cy), :] = (jnp.where(cut, e, 0) & keep & ~off) + NONE
        ys_e[0, p] = ee[pl.ds(row_of(p, cy - 2), 2), :]
        ys_e[1, p] = ee[pl.ds(row_of(p, 0), 2), :]
        return 0

    lax.fori_loop(0, cx, encode, 0)
    start(y_e)
    for i in range(2):
        xs_e[0, i] = ee[row_of(i, 0):row_of(i, cy), :]
        xs_e[1, i] = ee[row_of(cx - 2 + i, 0):row_of(cx - 2 + i, cy), :]
    start(x_e)

    @pl.when(jnp.logical_not(x_low))
    def _():
        a, b = PAD, row_of(-1, cy + 2)
        ee[a:b, :] = jnp.full((b - a, cz), NONE, jnp.int32)

    @pl.when(jnp.logical_not(x_high))
    def _():
        a, b = row_of(cx, -2), row_of(cx + 1, cy + 8)
        ee[a:b, :] = jnp.full((b - a, cz), NONE, jnp.int32)

    for side, has in enumerate((y_low, y_high)):
        @pl.when(jnp.logical_not(has))
        def _():
            yr_e[side] = jnp.full(yr_e.shape[1:], NONE, jnp.int32)
            yr_f[side] = jnp.zeros(yr_f.shape[1:], jnp.float32)
    for side, has in enumerate((z_low, z_high)):
        @pl.when(jnp.logical_not(has))
        def _():
            for t in (0, 1):
                zr_e[t, side] = jnp.full(zr_e.shape[2:], NONE, jnp.int32)
                zr_f[t, side] = jnp.zeros(zr_f.shape[2:], jnp.float32)

    def turn(v, amount):
        if isinstance(amount, int):
            return pltpu.roll(v, amount % cz, 1) if amount % cz else v
        return pltpu.roll(v, lax.rem(amount + cz, cz), 1)

    shifts = ((0, 1), (-1, -2))

    def pack(ks, e_of, f_of):
        at = [{d: lane == (k + d) % cz if isinstance(k, int) else lane == k + d for d in (-2, -1, 0, 1)} for k in ks]
        acc = {(side, j): zs_e[side, j] for side in (0, 1) for j in (0, 1)}
        for i, k in enumerate(ks):
            e = turn(e_of(i), k)
            for side, j in acc:
                acc[side, j] = jnp.where(at[i][shifts[side][j]], e, acc[side, j])
        for side, j in acc:
            zs_e[side, j] = acc[side, j]
        for c in range(chans):
            acc = [zs_f[side, c] for side in (0, 1)]
            for i, k in enumerate(ks):
                f = turn(f_of(i, c), k)
                acc = [jnp.where(at[i][shifts[side][0]], f, acc[side]) for side in (0, 1)]
            for side in (0, 1):
                zs_f[side, c] = acc[side]

    def settle(t):
        for side in (0, 1):
            for j in (0, 1):
                zr_e[t, side, j] = turn(zr_e[t, side, j], -shifts[1 - side][j])
            for c in range(chans):
                zr_f[t, side, c] = turn(zr_f[t, side, c], -shifts[1 - side][0])

    def pack_flat(ks):
        pack(ks, lambda i: ee[PAD + 8 * ks[i]:PAD + 8 * ks[i] + 8, :],
             lambda i, c: ff[c, PAD + 8 * ks[i]:PAD + 8 * ks[i] + 8, :])

    zs_e[...] = jnp.full(zs_e.shape, NONE, jnp.int32)
    zs_f[...] = jnp.zeros(zs_f.shape, jnp.float32)
    group = 4 if cx % 4 == 0 else 1

    def pack_own(i, _):
        ks, where = [], []
        for j in range(group):
            p = i * group + j
            for c in range(chans):
                ff[c, pl.ds(row_of(p, 0), cy), :] = raw_f[c, p]
            for b in range(nb - 1):
                ks.append((p + 2) * nb + 1 + b)
                where.append((p, b))
        pack(ks, lambda i: ee[pl.ds(PAD + 8 * ks[i], 8), :],
             lambda i, c: raw_f[c, where[i][0], 8 * where[i][1]:8 * where[i][1] + 8, :])
        return 0

    lax.fori_loop(0, cx // group, pack_own, 0)
    start(z_e[0])
    start(z_f[0])


    for d, source, direct in ((0, nb - 1, sub >= 4), (1, 1, sub < 4)):
        for side in (0, 1):
            back = [shift + source for shift in shifts[side]]
            ts_e[d, side] = jnp.where(slot == 0, turn(zs_e[side, 0], -back[0]), turn(zs_e[side, 1], 1 - back[1]))
            line = [None, None]
            for c in range(chans):
                v = turn(zs_f[side, c], c % 4 - back[0])
                line[c // 4] = v if c % 4 == 0 else jnp.where(slot == c % 4, v, line[c // 4])
            ts_f[d, side] = jnp.where(direct, line[0], pltpu.roll(line[1], 4, 0))
    for to, _, copy in diagonal:
        pl.when(to)(lambda: copy.start())

    recv(y_e)
    start(c_e)
    for p in range(cx):
        ee[row_of(p, -2):row_of(p, 0), :] = yr_e[0, p]
        ee[row_of(p, cy):row_of(p, cy + 2), :] = yr_e[1, p]
    recv(y_f)
    start(c_f)
    for p in range(cx):
        for c in range(chans):
            ff[c, row_of(p, -1):row_of(p, 0), :] = yr_f[0, c, p]
            ff[c, row_of(p, cy):row_of(p, cy + 1), :] = yr_f[1, c, p]
    for c in (z_e[0], z_f[0]):
        sent(c)
    pack_flat([(p + 2) * nb for p in range(cx + 1)])

    zero = me // n

    def blocks(p0, p1, chunk, body):
        k0 = (p0 + 2) * nb
        steps = ((p1 - p0) * nb + chunk) // chunk

        def step(i, _):
            for j in range(chunk):
                k = k0 + i * chunk + j
                body(k, PAD + 8 * k)
            return 0

        lax.fori_loop(0, steps, step, 0)

    def rows(ref, lead, r):
        return ref[lead + (pl.ds(r, 8), slice(None))]

    def count_body(k, r):
        acc = rows(ee, (), r)
        for ax, ay in PAIRS[1:]:
            e = rows(ee, (), r - pitch * ax - ay)
            acc = acc + jnp.where(holds(e, flag(ax, ay)), e, 0)
        here = (acc >> ONE) & 15
        here = here + pltpu.roll((acc >> UP) & 15, 1, 1) + pltpu.roll((acc >> DOWN) & 15, cz - 1, 1)
        inv[pl.ds(r, 8), :] = 1.0 / here.astype(jnp.float32)

    def edge(ref, lead, k):
        return turn(ref[(lax.rem(k, 2),) + lead], cz - k)

    def weight_body(k, r):
        i = rows(inv, (), r)
        i = jnp.where(ends, edge(inj_c, (), k), i)
        inv[pl.ds(r, 8), :] = i
        w = rows(ff, (0,), r) * i
        for c in range(chans):
            w0[c, pl.ds(r, 8), :] = w if c == 0 else w * rows(ff, (c,), r)

    def shift_body(k, r):
        for c in range(chans):
            v, g = rows(w0, (c,), r), edge(inj_w, (c,), k)
            wp[c, pl.ds(r, 8), :] = v + jnp.where(final, g, pltpu.roll(v, cz - 1, 1))
            wm[c, pl.ds(r, 8), :] = v + jnp.where(first, g, pltpu.roll(v, 1, 1))

    def weights(p0, p1, chunk):
        k0 = (p0 + 2) * nb
        steps = ((p1 - p0) * nb + chunk) // chunk

        def step(i, _):
            before = k0 + jnp.maximum(i - 1, 0) * chunk
            for j in range(chunk):
                shift_body(before + j, PAD + 8 * (before + j))
            for j in range(chunk):
                k = k0 + i * chunk + j
                weight_body(k, PAD + 8 * k)
            return 0

        lax.fori_loop(0, steps + 1, step, 0)

    def average_body(k, r):
        e = rows(ee, (), r)
        m = {b: holds(e, b) for b in (XP, XM, YP, YM, ZP, ZM)}

        def along_z(c, q):
            return jnp.where(m[ZP], rows(wp, (c,), q), jnp.where(m[ZM], rows(wm, (c,), q), rows(w0, (c,), q)))

        def along_y(c, q):
            side = jnp.where(m[YP], along_z(c, q + 1), jnp.where(m[YM], along_z(c, q - 1), 0.0))
            return along_z(c, q) + side

        def whole(c):
            side = jnp.where(m[XP], along_y(c, r + pitch), jnp.where(m[XM], along_y(c, r - pitch), 0.0))
            return along_y(c, r) + side

        inverse = 1.0 / whole(0)
        for c in range(1, chans):
            avg[c - 1, pl.ds(r, 8), :] = whole(c) * inverse

    def deposit_body(p, b):
        k = (p + 2) * nb + 1 + b
        r = PAD + 8 * k
        acc = [[None] * 3 for _ in range(fields)]
        for ax, ay in PAIRS:
            s = r - pitch * ax - ay
            e = rows(ee, (), s)
            ms = [holds(e, flag(ax, ay, az)) for az in (0, 1, -1)]
            for f in range(fields):
                v = rows(avg, (f,), s)
                for i in range(3):
                    term = v if (ax, ay, i) == (0, 0, 0) else jnp.where(ms[i], v, 0.0)
                    acc[f][i] = term if acc[f][i] is None else acc[f][i] + term
        i = rows(inv, (), r)
        for f in range(fields):
            here, up, down = acc[f]
            g = edge(inj_d, (f,), k)
            here = here + jnp.where(first, g, pltpu.roll(up, 1, 1))
            here = here + jnp.where(final, g, pltpu.roll(down, cz - 1, 1))
            out_ref[0, f, p, 8 * b:8 * b + 8, :] = here * i

    def deposit(p0, p1):
        def plane(i, _):
            for b in range(nb - 1):
                deposit_body(p0 + i, b)
            return 0

        lax.fori_loop(0, p1 - p0, plane, 0)

    def shift_y(v, dy):
        if dy == 0:
            return v
        w = pltpu.roll(v, 7 if dy == 1 else 1, 0)
        return jnp.where(sub == (7 if dy == 1 else 0), turn(w, -dy), w)

    def shift_x(v, dx):
        return turn(v, -nb * dx) if dx else v

    def spread(t):
        lines = {ax: t[ax, 0] + shift_y(t[ax, 1], -1) + shift_y(t[ax, -1], 1) for ax in (0, 1, -1)}
        return lines[0] + shift_x(lines[1], -1) + shift_x(lines[-1], 1)

    def ghost(t, side):
        toward, away = (ZP, ZM) if side == 0 else (ZM, ZP)
        e0, e1 = (turn(zs_e[side, j], -shifts[side][j]) for j in (0, 1))
        g0, g1 = zr_e[t, side, 0], zr_e[t, side, 1]
        own = [turn(zs_f[side, c], -shifts[side][0]) for c in range(chans)]
        from_g0 = jnp.where(holds(g0, toward), 257, 1)
        from_e0 = jnp.where(holds(e0, away), 257, 256)
        found = {}
        for ax, ay in PAIRS:
            b = flag(ax, ay)
            found[ax, ay] = (jnp.where(holds(g1, b | toward), 1, 0) + jnp.where(holds(g0, b), from_g0, 0)
                             + jnp.where(holds(e0, b), from_e0, 0) + jnp.where(holds(e1, b | away), 256, 0))
        found = spread(found)
        i_ghost = 1.0 / (found & 255).astype(jnp.float32)
        i_own = 1.0 / (found >> 8).astype(jnp.float32)
        two_c[side] = i_own
        w_ghost, w_own = zr_f[t, side, 0] * i_ghost, own[0] * i_own
        m = {b: holds(g0, b) for b in (XP, XM, YP, YM)}
        mine = holds(g0, toward)
        inverse = None
        for c in range(chans):
            v = w_ghost if c == 0 else w_ghost * zr_f[t, side, c]
            two_w[side, c] = v
            v = v + (w_own if c == 0 else w_own * own[c])
            above, below = shift_y(v, 1), shift_y(v, -1)
            line = {dx: shift_x(v, dx) + jnp.where(m[YP], shift_x(above, dx), jnp.where(m[YM], shift_x(below, dx), 0.0))
                    for dx in (0, 1, -1)}
            whole = line[0] + jnp.where(m[XP], line[1], jnp.where(m[XM], line[-1], 0.0))
            if c == 0:
                inverse = 1.0 / whole
                continue
            a = jnp.where(mine, whole * inverse, 0.0)
            two_d[side, c - 1] = spread({
                (ax, ay): jnp.where(holds(g0, flag(ax, ay)), a, 0.0) if (ax, ay) != (0, 0) else a
                for ax, ay in PAIRS})

    def ghosts(t):
        for side in (0, 1):
            ghost(t, side)
        pairs = [(two_c, inj_c, ())] + [(two_w, inj_w, (c,)) for c in range(chans)]
        for two, inj, lead in pairs + [(two_d, inj_d, (f,)) for f in range(fields)]:
            below, above = two[(0,) + lead], turn(two[(1,) + lead], -1)
            inj[(0,) + lead] = jnp.where(odd, above, below)
            inj[(1,) + lead] = jnp.where(odd, below, above)

    low, high = x_low.astype(jnp.int32), x_high.astype(jnp.int32)
    blocks(low, cx - high, 6, count_body)
    recv(z_e[0])
    recv(z_f[0])
    settle(0)
    for _, frm, copy in diagonal:
        pl.when(frm)(lambda: copy.wait_recv())
    for i, (has, rows_of) in enumerate(((y_low, sub >= 4), (y_high, sub < 4))):
        for side, beside in enumerate((z_low, z_high)):
            @pl.when(jnp.logical_and(has, beside))
            def _():
                at = jnp.logical_and(slot == 0, rows_of)
                for j in (0, 1):
                    zr_e[0, side, j] = jnp.where(at, turn(tr_e[i, side], nb * i - j), zr_e[0, side, j])
                for c in range(chans):
                    v = turn(tr_f[i, side], nb * i - c % 4)
                    v = v if c < 4 else pltpu.roll(v, 4, 0)
                    zr_f[0, side, c] = jnp.where(at, v, zr_f[0, side, c])
    ghosts(0)
    weights(low, cx - high, 10)
    blocks(2 * low, cx - 2 * high, 5, average_body)

    for c in (x_f, x_e, c_e, c_f):
        recv(c)
    for side, has in enumerate((x_low, x_high)):
        @pl.when(has)
        def _():
            for i in range(2):
                p = (i - 2, cx + i)[side]
                ee[row_of(p, 0):row_of(p, cy), :] = xr_e[side, i]
                ee[row_of(p, -2):row_of(p, 0), :] = cr_e[side, 0, i]
                ee[row_of(p, cy):row_of(p, cy + 2), :] = cr_e[side, 1, i]
            p = (-1, cx)[side]
            for c in range(chans):
                ff[c, row_of(p, 0):row_of(p, cy), :] = xr_f[side, c, 0]
                ff[c, row_of(p, -1):row_of(p, 0), :] = cr_f[side, 0, c, 0]
                ff[c, row_of(p, cy):row_of(p, cy + 1), :] = cr_f[side, 1, c, 0]
            k = (0, (cx + 2) * nb)[side]
            pack_flat(list(range(k, k + 2 * nb + 1)))
    start(z_e[1])
    start(z_f[1])
    deposit(3 * low, cx - 3 * high)

    recv(z_e[1])
    recv(z_f[1])
    settle(1)
    ghosts(1)
    edges = []
    for has, (a, b) in ((low, (-1, 1)), (high, (cx - 1, cx + 1))):
        edges.append((has, a, b))
    for has, a, b in edges:
        @pl.when(has == 1)
        def _():
            blocks(zero + a, b, 6, count_body)
            weights(zero + a, b, 6)
            a2, b2 = (a, b + 1) if a < 0 else (a - 1, b)
            blocks(zero + a2, b2, 4, average_body)
            a3, b3 = (0, 3) if a < 0 else (cx - 3, cx)
            deposit(zero + a3, b3)
    for c in [x_f, x_e, y_e, y_f, c_e, c_f, z_e[1], z_f[1]]:
        sent(c)
    for to, _, copy in diagonal:
        pl.when(to)(lambda: copy.wait_send())


def per_device(n, conserved, volume_fraction, cut_mask, merge_code):
    fields, cx, cy, cz = conserved.shape[1:]
    chans = fields + 1
    flat = PAD + (cx + 4) * (cy + 8) + 2 * (cy + 8) + 64
    f32, i32 = jnp.float32, jnp.int32
    V = pltpu.VMEM
    scratch = [
        V((flat, cz), i32), V((chans, flat, cz), f32), V((flat, cz), f32),
        V((chans, flat, cz), f32), V((chans, flat, cz), f32), V((chans, flat, cz), f32),
        V((fields, flat, cz), f32),
        V((cx, cy, cz), i32), V((cx, cy, cz), i32), V((chans, cx, cy, cz), f32),
        V((2, cx, 2, cz), i32), V((2, chans, cx, 1, cz), f32),
        V((2, cx, 2, cz), i32), V((2, chans, cx, 1, cz), f32),
        V((2, 2, cy, cz), i32), V((2, 2, cy, cz), i32), V((2, chans, 1, cy, cz), f32),
        V((2, 2, 2, 2, cz), i32), V((2, 2, chans, 1, 1, cz), f32),
        V((2, 2, 8, cz), i32), V((2, chans, 8, cz), f32),
        V((2, 2, 2, 8, cz), i32), V((2, 2, chans, 8, cz), f32),
        V((2, 2, 8, cz), i32), V((2, 2, 8, cz), f32), V((2, 2, 8, cz), i32), V((2, 2, 8, cz), f32),
        V((2, 8, cz), f32), V((2, chans, 8, cz), f32), V((2, fields, 8, cz), f32),
        V((2, 8, cz), f32), V((2, chans, 8, cz), f32), V((2, fields, 8, cz), f32),
        pltpu.SemaphoreType.DMA((4,)), pltpu.SemaphoreType.DMA((28,)), pltpu.SemaphoreType.DMA((28,)),
    ]
    return pl.pallas_call(
        functools.partial(kernel, n, (fields, cx, cy, cz)),
        out_shape=pltpu.VMEM(conserved.shape, f32),
        in_specs=[pl.BlockSpec(memory_space=pl.ANY)] * 4,
        out_specs=pl.BlockSpec(memory_space=pltpu.VMEM),
        scratch_shapes=scratch,
        compiler_params=pltpu.CompilerParams(
            collective_id=0, has_side_effects=True, vmem_limit_bytes=60 * 1024 * 1024),
        name="redistribute",
    )(conserved, volume_fraction, cut_mask, merge_code)


def solution(mesh):
    return jax.shard_map(
        functools.partial(per_device, mesh.shape["boxes"]),
        mesh=mesh,
        in_specs=(
            P("boxes", None, None, None, None),
            P("boxes", None, None, None),
            P("boxes", None, None, None),
            P("boxes", None, None, None),
        ),
        out_specs=P("boxes", None, None, None, None),
        check_vma=False,
    )
```

```python
import functools

import jax
import jax.numpy as jnp
from jax import lax
from jax.experimental import pallas as pl
from jax.experimental.pallas import tpu as pltpu
from jax.sharding import PartitionSpec as P

NBY = 4
NBZ = 4
MESH = pl.DeviceIdType.MESH
XP, XM, YP, YM, ZP, ZM = 1, 2, 4, 8, 16, 32
ONE, UP, DOWN = 10, 14, 18
NONE = 1 << ONE
PAD = 8
PAIRS = [(ax, ay) for ax in (0, 1, -1) for ay in (0, 1, -1)]


def flag(ax, ay, az=0):
    return (
        {1: XP, -1: XM, 0: 0}[ax] | {1: YP, -1: YM, 0: 0}[ay] | {1: ZP, -1: ZM, 0: 0}[az]
    )


def holds(e, bits):
    return (e & bits) == bits


def kernel(n, dims, u_ref, vf_ref, mask_ref, code_ref, out_ref, ee, ff, inv, w0, wp, wm, avg,
           raw_m, raw_c, raw_f, ys_e, ys_f, yr_e, yr_f, xs_e, xr_e, xr_f, cr_e, cr_f,
           zs_e, zs_f, zr_e, zr_f, ts_e, ts_f, tr_e, tr_f, two_c, two_w, two_d, inj_c, inj_w, inj_d, load_sem, send_sem, recv_sem):
    fields, cx, cy, cz = dims
    chans = fields + 1
    nb = cy // 8 + 1
    pitch = 8 * nb
    me = lax.axis_index("boxes")
    bx, by, bz = me // (NBY * NBZ), me // NBZ % NBY, me % NBZ
    axes = {
        "x": (NBY * NBZ, bx > 0, bx < n // (NBY * NBZ) - 1),
        "y": (NBZ, by > 0, by < NBY - 1),
        "z": (1, bz > 0, bz < NBZ - 1),
    }
    lane = lax.broadcasted_iota(jnp.int32, (8, cz), 1)
    sub = lax.broadcasted_iota(jnp.int32, (8, cz), 0)
    first, final = lane == 0, lane == cz - 1
    ends = jnp.logical_or(first, final)
    odd = (lane & 1) == 1
    slot = lane - nb * ((lane * (4096 // nb + 1)) >> 12)

    loads = [
        pltpu.make_async_copy(mask_ref.at[0], raw_m, load_sem.at[0]),
        pltpu.make_async_copy(code_ref.at[0], raw_c, load_sem.at[1]),
        pltpu.make_async_copy(u_ref.at[0], raw_f.at[1:chans], load_sem.at[2]),
        pltpu.make_async_copy(vf_ref.at[0], raw_f.at[0], load_sem.at[3]),
    ]
    for copy in loads:
        copy.start()

    barrier = pltpu.get_barrier_semaphore()
    total = jnp.int32(0)
    for stride, low, high in axes.values():
        for has, there in ((low, me - stride), (high, me + stride)):
            @pl.when(has)
            def _():
                pl.semaphore_signal(barrier, inc=1, device_id=(there,), device_id_type=MESH)
            total = total + has.astype(jnp.int32)
    for dy in (1, -1):
        for dz in (-1, 1):
            has = jnp.logical_and(axes["y"][1 + (dy == 1)], axes["z"][1 + (dz == 1)])
            @pl.when(has)
            def _():
                pl.semaphore_signal(barrier, inc=1, device_id=(me + NBZ * dy + dz,), device_id_type=MESH)
            total = total + has.astype(jnp.int32)
    def copies(axis, ident, up, down):
        stride = axes[axis][0]
        out = []
        for d, (pair, there) in enumerate(((up, me + stride), (down, me - stride))):
            out.append(pltpu.make_async_remote_copy(
                src_ref=pair[0], dst_ref=pair[1], send_sem=send_sem.at[2 * ident + d],
                recv_sem=recv_sem.at[2 * ident + d], device_id=(there,), device_id_type=MESH))
        return axis, out

    def start(c):
        axis, (up, down) = c
        _, low, high = axes[axis]
        pl.when(high)(lambda: up.start())
        pl.when(low)(lambda: down.start())

    def recv(c):
        axis, (up, down) = c
        _, low, high = axes[axis]
        pl.when(low)(lambda: up.wait_recv())
        pl.when(high)(lambda: down.wait_recv())

    def sent(c):
        axis, (up, down) = c
        _, low, high = axes[axis]
        pl.when(high)(lambda: up.wait_send())
        pl.when(low)(lambda: down.wait_send())

    x_f = copies("x", 0, (raw_f.at[:, cx - 1:cx], xr_f.at[0]), (raw_f.at[:, 0:1], xr_f.at[1]))
    x_e = copies("x", 1, (xs_e.at[1], xr_e.at[0]), (xs_e.at[0], xr_e.at[1]))
    y_e = copies("y", 2, (ys_e.at[0], yr_e.at[0]), (ys_e.at[1], yr_e.at[1]))
    y_f = copies("y", 3, (ys_f.at[0], yr_f.at[0]), (ys_f.at[1], yr_f.at[1]))
    c_e = copies("x", 4, (yr_e.at[:, cx - 2:cx], cr_e.at[0]), (yr_e.at[:, 0:2], cr_e.at[1]))
    c_f = copies("x", 5, (yr_f.at[:, :, cx - 1:cx], cr_f.at[0]), (yr_f.at[:, :, 0:1], cr_f.at[1]))
    z_e = [copies("z", 6 + t, (zs_e.at[1], zr_e.at[t, 0]), (zs_e.at[0], zr_e.at[t, 1])) for t in (0, 1)]
    z_f = [copies("z", 8 + t, (zs_f.at[1], zr_f.at[t, 0]), (zs_f.at[0], zr_f.at[t, 1])) for t in (0, 1)]

    loads[0].wait()
    loads[1].wait()

    diagonal = []
    for d, dy in enumerate((1, -1)):
        for side, dz in enumerate((-1, 1)):
            to = jnp.logical_and(axes["y"][1 + (dy == 1)], axes["z"][1 + (dz == 1)])
            frm = jnp.logical_and(axes["y"][1 + (dy == -1)], axes["z"][1 + (dz == -1)])
            for ts, tr in ((ts_e, tr_e), (ts_f, tr_f)):
                at = 20 + len(diagonal)
                diagonal.append((to, frm, pltpu.make_async_remote_copy(
                    src_ref=ts.at[d, side], dst_ref=tr.at[d, 1 - side], send_sem=send_sem.at[at],
                    recv_sem=recv_sem.at[at], device_id=(me + NBZ * dy + dz,), device_id_type=MESH)))

    def row_of(p, y):
        return PAD + pitch * (p + 2) + 8 + y

    _, x_low, x_high = axes["x"]
    _, y_low, y_high = axes["y"]
    _, z_low, z_high = axes["z"]
    clear = lambda has, bits: jnp.where(has, 0, bits)
    row2 = lax.broadcasted_iota(jnp.int32, (cy, cz), 0)
    lane2 = lax.broadcasted_iota(jnp.int32, (cy, cz), 1)
    drop = (jnp.where(row2 == 0, clear(y_low, YM), 0) + jnp.where(row2 == cy - 1, clear(y_high, YP), 0)
            + jnp.where(lane2 == 0, clear(z_low, ZM + (1 << DOWN)), 0)
            + jnp.where(lane2 == cz - 1, clear(z_high, ZP + (1 << UP)), 0))
    keep = ~drop

    def encode(p, _):
        c = raw_c[p]
        cut = raw_m[p] == 1
        third = (c * 171) >> 9
        sz = c - 3 * third
        ninth = (third * 171) >> 9
        sy = third - 3 * ninth
        bit = lambda test, value: jnp.where(test, value, 0)
        e = (bit(ninth == 2, XP) + bit(ninth == 0, XM) + bit(sy == 2, YP) + bit(sy == 0, YM)
             + bit(sz == 2, ZP + (1 << UP)) + bit(sz == 0, ZM + (1 << DOWN)))
        off = jnp.where(p == 0, clear(x_low, XM), 0) + jnp.where(p == cx - 1, clear(x_high, XP), 0)
        ee[pl.ds(row_of(p, 0), cy), :] = (jnp.where(cut, e, 0) & keep & ~off) + NONE
        ys_e[0, p] = ee[pl.ds(row_of(p, cy - 2), 2), :]
        ys_e[1, p] = ee[pl.ds(row_of(p, 0), 2), :]
        return 0

    lax.fori_loop(0, cx, encode, 0)
    loads[2].wait()
    loads[3].wait()
    for c in range(chans):
        ys_f[0, c] = raw_f[c, :, cy - 1:cy, :]
        ys_f[1, c] = raw_f[c, :, 0:1, :]
    pl.semaphore_wait(barrier, total)
    start(y_e)
    start(y_f)
    for i in range(2):
        xs_e[0, i] = ee[row_of(i, 0):row_of(i, cy), :]
        xs_e[1, i] = ee[row_of(cx - 2 + i, 0):row_of(cx - 2 + i, cy), :]

    @pl.when(jnp.logical_not(x_low))
    def _():
        a, b = PAD, row_of(-1, cy + 2)
        ee[a:b, :] = jnp.full((b - a, cz), NONE, jnp.int32)

    @pl.when(jnp.logical_not(x_high))
    def _():
        a, b = row_of(cx, -2), row_of(cx + 1, cy + 8)
        ee[a:b, :] = jnp.full((b - a, cz), NONE, jnp.int32)

    for side, has in enumerate((y_low, y_high)):
        @pl.when(jnp.logical_not(has))
        def _():
            yr_e[side] = jnp.full(yr_e.shape[1:], NONE, jnp.int32)
            yr_f[side] = jnp.zeros(yr_f.shape[1:], jnp.float32)
    for side, has in enumerate((z_low, z_high)):
        @pl.when(jnp.logical_not(has))
        def _():
            for t in (0, 1):
                zr_e[t, side] = jnp.full(zr_e.shape[2:], NONE, jnp.int32)
                zr_f[t, side] = jnp.zeros(zr_f.shape[2:], jnp.float32)

    def turn(v, amount):
        if isinstance(amount, int):
            return pltpu.roll(v, amount % cz, 1) if amount % cz else v
        return pltpu.roll(v, lax.rem(amount + cz, cz), 1)

    shifts = ((0, 1), (-1, -2))

    def pack(ks, e_of, f_of):
        at = [{d: lane == (k + d) % cz if isinstance(k, int) else lane == k + d for d in (-2, -1, 0, 1)} for k in ks]
        acc = {(side, j): zs_e[side, j] for side in (0, 1) for j in (0, 1)}
        for i, k in enumerate(ks):
            e = turn(e_of(i), k)
            for side, j in acc:
                acc[side, j] = jnp.where(at[i][shifts[side][j]], e, acc[side, j])
        for side, j in acc:
            zs_e[side, j] = acc[side, j]
        for c in range(chans):
            acc = [zs_f[side, c] for side in (0, 1)]
            for i, k in enumerate(ks):
                f = turn(f_of(i, c), k)
                acc = [jnp.where(at[i][shifts[side][0]], f, acc[side]) for side in (0, 1)]
            for side in (0, 1):
                zs_f[side, c] = acc[side]

    def settle(t):
        for side in (0, 1):
            for j in (0, 1):
                zr_e[t, side, j] = turn(zr_e[t, side, j], -shifts[1 - side][j])
            for c in range(chans):
                zr_f[t, side, c] = turn(zr_f[t, side, c], -shifts[1 - side][0])

    def pack_flat(ks):
        pack(ks, lambda i: ee[PAD + 8 * ks[i]:PAD + 8 * ks[i] + 8, :],
             lambda i, c: ff[c, PAD + 8 * ks[i]:PAD + 8 * ks[i] + 8, :])

    zs_e[...] = jnp.full(zs_e.shape, NONE, jnp.int32)
    zs_f[...] = jnp.zeros(zs_f.shape, jnp.float32)
    group = 4 if cx % 4 == 0 else 1

    def pack_own(i, _):
        ks, where = [], []
        for j in range(group):
            p = i * group + j
            for c in range(chans):
                ff[c, pl.ds(row_of(p, 0), cy), :] = raw_f[c, p]
            for b in range(nb - 1):
                ks.append((p + 2) * nb + 1 + b)
                where.append((p, b))
        pack(ks, lambda i: ee[pl.ds(PAD + 8 * ks[i], 8), :],
             lambda i, c: raw_f[c, where[i][0], 8 * where[i][1]:8 * where[i][1] + 8, :])
        return 0

    lax.fori_loop(0, cx // group, pack_own, 0)
    start(z_e[0])
    start(z_f[0])


    for d, source, direct in ((0, nb - 1, sub >= 4), (1, 1, sub < 4)):
        for side in (0, 1):
            back = [shift + source for shift in shifts[side]]
            ts_e[d, side] = jnp.where(slot == 0, turn(zs_e[side, 0], -back[0]), turn(zs_e[side, 1], 1 - back[1]))
            line = [None, None]
            for c in range(chans):
                v = turn(zs_f[side, c], c % 4 - back[0])
                line[c // 4] = v if c % 4 == 0 else jnp.where(slot == c % 4, v, line[c // 4])
            ts_f[d, side] = jnp.where(direct, line[0], pltpu.roll(line[1], 4, 0))
    for to, _, copy in diagonal:
        pl.when(to)(lambda: copy.start())
    start(x_f)
    start(x_e)

    recv(y_e)
    start(c_e)
    for p in range(cx):
        ee[row_of(p, -2):row_of(p, 0), :] = yr_e[0, p]
        ee[row_of(p, cy):row_of(p, cy + 2), :] = yr_e[1, p]

    zero = me // n

    def blocks(p0, p1, chunk, body):
        k0 = (p0 + 2) * nb
        steps = ((p1 - p0) * nb + chunk) // chunk

        def step(i, _):
            for j in range(chunk):
                k = k0 + i * chunk + j
                body(k, PAD + 8 * k)
            return 0

        lax.fori_loop(0, steps, step, 0)

    def rows(ref, lead, r):
        return ref[lead + (pl.ds(r, 8), slice(None))]

    def count_body(k, r):
        acc = rows(ee, (), r)
        for ax, ay in PAIRS[1:]:
            e = rows(ee, (), r - pitch * ax - ay)
            acc = acc + jnp.where(holds(e, flag(ax, ay)), e, 0)
        here = (acc >> ONE) & 15
        here = here + pltpu.roll((acc >> UP) & 15, 1, 1) + pltpu.roll((acc >> DOWN) & 15, cz - 1, 1)
        inv[pl.ds(r, 8), :] = 1.0 / here.astype(jnp.float32)

    def edge(ref, lead, k):
        return turn(ref[(lax.rem(k, 2),) + lead], cz - k)

    def weight_body(k, r):
        i = rows(inv, (), r)
        i = jnp.where(ends, edge(inj_c, (), k), i)
        inv[pl.ds(r, 8), :] = i
        w = rows(ff, (0,), r) * i
        for c in range(chans):
            w0[c, pl.ds(r, 8), :] = w if c == 0 else w * rows(ff, (c,), r)

    def shift_body(k, r):
        for c in range(chans):
            v, g = rows(w0, (c,), r), edge(inj_w, (c,), k)
            wp[c, pl.ds(r, 8), :] = v + jnp.where(final, g, pltpu.roll(v, cz - 1, 1))
            wm[c, pl.ds(r, 8), :] = v + jnp.where(first, g, pltpu.roll(v, 1, 1))

    def weights(p0, p1, chunk):
        k0 = (p0 + 2) * nb
        steps = ((p1 - p0) * nb + chunk) // chunk

        def step(i, _):
            before = k0 + jnp.maximum(i - 1, 0) * chunk
            for j in range(chunk):
                shift_body(before + j, PAD + 8 * (before + j))
            for j in range(chunk):
                k = k0 + i * chunk + j
                weight_body(k, PAD + 8 * k)
            return 0

        lax.fori_loop(0, steps + 1, step, 0)

    def average_body(k, r):
        e = rows(ee, (), r)
        m = {b: holds(e, b) for b in (XP, XM, YP, YM, ZP, ZM)}

        def along_z(c, q):
            return jnp.where(m[ZP], rows(wp, (c,), q), jnp.where(m[ZM], rows(wm, (c,), q), rows(w0, (c,), q)))

        def along_y(c, q):
            side = jnp.where(m[YP], along_z(c, q + 1), jnp.where(m[YM], along_z(c, q - 1), 0.0))
            return along_z(c, q) + side

        def whole(c):
            side = jnp.where(m[XP], along_y(c, r + pitch), jnp.where(m[XM], along_y(c, r - pitch), 0.0))
            return along_y(c, r) + side

        inverse = 1.0 / whole(0)
        for c in range(1, chans):
            avg[c - 1, pl.ds(r, 8), :] = whole(c) * inverse

    def deposit_body(p, b):
        k = (p + 2) * nb + 1 + b
        r = PAD + 8 * k
        acc = [[None] * 3 for _ in range(fields)]
        for ax, ay in PAIRS:
            s = r - pitch * ax - ay
            e = rows(ee, (), s)
            ms = [holds(e, flag(ax, ay, az)) for az in (0, 1, -1)]
            for f in range(fields):
                v = rows(avg, (f,), s)
                for i in range(3):
                    term = v if (ax, ay, i) == (0, 0, 0) else jnp.where(ms[i], v, 0.0)
                    acc[f][i] = term if acc[f][i] is None else acc[f][i] + term
        i = rows(inv, (), r)
        for f in range(fields):
            here, up, down = acc[f]
            g = edge(inj_d, (f,), k)
            here = here + jnp.where(first, g, pltpu.roll(up, 1, 1))
            here = here + jnp.where(final, g, pltpu.roll(down, cz - 1, 1))
            out_ref[0, f, p, 8 * b:8 * b + 8, :] = here * i

    def deposit(p0, p1):
        def plane(i, _):
            for b in range(nb - 1):
                deposit_body(p0 + i, b)
            return 0

        lax.fori_loop(0, p1 - p0, plane, 0)

    def shift_y(v, dy):
        if dy == 0:
            return v
        w = pltpu.roll(v, 7 if dy == 1 else 1, 0)
        return jnp.where(sub == (7 if dy == 1 else 0), turn(w, -dy), w)

    def shift_x(v, dx):
        return turn(v, -nb * dx) if dx else v

    def spread(t):
        lines = {ax: t[ax, 0] + shift_y(t[ax, 1], -1) + shift_y(t[ax, -1], 1) for ax in (0, 1, -1)}
        return lines[0] + shift_x(lines[1], -1) + shift_x(lines[-1], 1)

    def ghost(t, side):
        toward, away = (ZP, ZM) if side == 0 else (ZM, ZP)
        e0, e1 = (turn(zs_e[side, j], -shifts[side][j]) for j in (0, 1))
        g0, g1 = zr_e[t, side, 0], zr_e[t, side, 1]
        own = [turn(zs_f[side, c], -shifts[side][0]) for c in range(chans)]
        from_g0 = jnp.where(holds(g0, toward), 257, 1)
        from_e0 = jnp.where(holds(e0, away), 257, 256)
        found = {}
        for ax, ay in PAIRS:
            b = flag(ax, ay)
            found[ax, ay] = (jnp.where(holds(g1, b | toward), 1, 0) + jnp.where(holds(g0, b), from_g0, 0)
                             + jnp.where(holds(e0, b), from_e0, 0) + jnp.where(holds(e1, b | away), 256, 0))
        found = spread(found)
        i_ghost = 1.0 / (found & 255).astype(jnp.float32)
        i_own = 1.0 / (found >> 8).astype(jnp.float32)
        two_c[side] = i_own
        w_ghost, w_own = zr_f[t, side, 0] * i_ghost, own[0] * i_own
        m = {b: holds(g0, b) for b in (XP, XM, YP, YM)}
        mine = holds(g0, toward)
        inverse = None
        for c in range(chans):
            v = w_ghost if c == 0 else w_ghost * zr_f[t, side, c]
            two_w[side, c] = v
            v = v + (w_own if c == 0 else w_own * own[c])
            above, below = shift_y(v, 1), shift_y(v, -1)
            line = {dx: shift_x(v, dx) + jnp.where(m[YP], shift_x(above, dx), jnp.where(m[YM], shift_x(below, dx), 0.0))
                    for dx in (0, 1, -1)}
            whole = line[0] + jnp.where(m[XP], line[1], jnp.where(m[XM], line[-1], 0.0))
            if c == 0:
                inverse = 1.0 / whole
                continue
            a = jnp.where(mine, whole * inverse, 0.0)
            two_d[side, c - 1] = spread({
                (ax, ay): jnp.where(holds(g0, flag(ax, ay)), a, 0.0) if (ax, ay) != (0, 0) else a
                for ax, ay in PAIRS})

    def ghosts(t):
        for side in (0, 1):
            ghost(t, side)
        pairs = [(two_c, inj_c, ())] + [(two_w, inj_w, (c,)) for c in range(chans)]
        for two, inj, lead in pairs + [(two_d, inj_d, (f,)) for f in range(fields)]:
            below, above = two[(0,) + lead], turn(two[(1,) + lead], -1)
            inj[(0,) + lead] = jnp.where(odd, above, below)
            inj[(1,) + lead] = jnp.where(odd, below, above)

    low, high = x_low.astype(jnp.int32), x_high.astype(jnp.int32)
    blocks(low, cx - high, 6, count_body)
    recv(y_f)
    start(c_f)
    for p in range(cx):
        for c in range(chans):
            ff[c, row_of(p, -1):row_of(p, 0), :] = yr_f[0, c, p]
            ff[c, row_of(p, cy):row_of(p, cy + 1), :] = yr_f[1, c, p]
    for c in (z_e[0], z_f[0]):
        sent(c)
    pack_flat([(p + 2) * nb for p in range(cx + 1)])
    recv(z_e[0])
    recv(z_f[0])
    settle(0)
    for _, frm, copy in diagonal:
        pl.when(frm)(lambda: copy.wait_recv())
    for i, (has, rows_of) in enumerate(((y_low, sub >= 4), (y_high, sub < 4))):
        for side, beside in enumerate((z_low, z_high)):
            @pl.when(jnp.logical_and(has, beside))
            def _():
                at = jnp.logical_and(slot == 0, rows_of)
                for j in (0, 1):
                    zr_e[0, side, j] = jnp.where(at, turn(tr_e[i, side], nb * i - j), zr_e[0, side, j])
                for c in range(chans):
                    v = turn(tr_f[i, side], nb * i - c % 4)
                    v = v if c < 4 else pltpu.roll(v, 4, 0)
                    zr_f[0, side, c] = jnp.where(at, v, zr_f[0, side, c])
    ghosts(0)
    weights(low, cx - high, 10)
    blocks(2 * low, cx - 2 * high, 5, average_body)

    for c in (x_f, x_e, c_e, c_f):
        recv(c)
    for side, has in enumerate((x_low, x_high)):
        @pl.when(has)
        def _():
            for i in range(2):
                p = (i - 2, cx + i)[side]
                ee[row_of(p, 0):row_of(p, cy), :] = xr_e[side, i]
                ee[row_of(p, -2):row_of(p, 0), :] = cr_e[side, 0, i]
                ee[row_of(p, cy):row_of(p, cy + 2), :] = cr_e[side, 1, i]
            p = (-1, cx)[side]
            for c in range(chans):
                ff[c, row_of(p, 0):row_of(p, cy), :] = xr_f[side, c, 0]
                ff[c, row_of(p, -1):row_of(p, 0), :] = cr_f[side, 0, c, 0]
                ff[c, row_of(p, cy):row_of(p, cy + 1), :] = cr_f[side, 1, c, 0]
            k = (0, (cx + 2) * nb)[side]
            pack_flat(list(range(k, k + 2 * nb + 1)))
    start(z_e[1])
    start(z_f[1])
    deposit(3 * low, cx - 3 * high)

    recv(z_e[1])
    recv(z_f[1])
    settle(1)
    ghosts(1)
    edges = []
    for has, (a, b) in ((low, (-1, 1)), (high, (cx - 1, cx + 1))):
        edges.append((has, a, b))
    for has, a, b in edges:
        @pl.when(has == 1)
        def _():
            blocks(zero + a, b, 6, count_body)
            weights(zero + a, b, 6)
            a2, b2 = (a, b + 1) if a < 0 else (a - 1, b)
            blocks(zero + a2, b2, 4, average_body)
            a3, b3 = (0, 3) if a < 0 else (cx - 3, cx)
            deposit(zero + a3, b3)
    for c in [x_f, x_e, y_e, y_f, c_e, c_f, z_e[1], z_f[1]]:
        sent(c)
    for to, _, copy in diagonal:
        pl.when(to)(lambda: copy.wait_send())


def per_device(n, conserved, volume_fraction, cut_mask, merge_code):
    fields, cx, cy, cz = conserved.shape[1:]
    chans = fields + 1
    flat = PAD + (cx + 4) * (cy + 8) + 2 * (cy + 8) + 64
    f32, i32 = jnp.float32, jnp.int32
    V = pltpu.VMEM
    scratch = [
        V((flat, cz), i32), V((chans, flat, cz), f32), V((flat, cz), f32),
        V((chans, flat, cz), f32), V((chans, flat, cz), f32), V((chans, flat, cz), f32),
        V((fields, flat, cz), f32),
        V((cx, cy, cz), i32), V((cx, cy, cz), i32), V((chans, cx, cy, cz), f32),
        V((2, cx, 2, cz), i32), V((2, chans, cx, 1, cz), f32),
        V((2, cx, 2, cz), i32), V((2, chans, cx, 1, cz), f32),
        V((2, 2, cy, cz), i32), V((2, 2, cy, cz), i32), V((2, chans, 1, cy, cz), f32),
        V((2, 2, 2, 2, cz), i32), V((2, 2, chans, 1, 1, cz), f32),
        V((2, 2, 8, cz), i32), V((2, chans, 8, cz), f32),
        V((2, 2, 2, 8, cz), i32), V((2, 2, chans, 8, cz), f32),
        V((2, 2, 8, cz), i32), V((2, 2, 8, cz), f32), V((2, 2, 8, cz), i32), V((2, 2, 8, cz), f32),
        V((2, 8, cz), f32), V((2, chans, 8, cz), f32), V((2, fields, 8, cz), f32),
        V((2, 8, cz), f32), V((2, chans, 8, cz), f32), V((2, fields, 8, cz), f32),
        pltpu.SemaphoreType.DMA((4,)), pltpu.SemaphoreType.DMA((28,)), pltpu.SemaphoreType.DMA((28,)),
    ]
    return pl.pallas_call(
        functools.partial(kernel, n, (fields, cx, cy, cz)),
        out_shape=pltpu.VMEM(conserved.shape, f32),
        in_specs=[pl.BlockSpec(memory_space=pl.ANY)] * 4,
        out_specs=pl.BlockSpec(memory_space=pltpu.VMEM),
        scratch_shapes=scratch,
        compiler_params=pltpu.CompilerParams(
            collective_id=0, has_side_effects=True, vmem_limit_bytes=60 * 1024 * 1024),
        name="redistribute",
    )(conserved, volume_fraction, cut_mask, merge_code)


def solution(mesh):
    return jax.shard_map(
        functools.partial(per_device, mesh.shape["boxes"]),
        mesh=mesh,
        in_specs=(
            P("boxes", None, None, None, None),
            P("boxes", None, None, None),
            P("boxes", None, None, None),
            P("boxes", None, None, None),
        ),
        out_specs=P("boxes", None, None, None, None),
        check_vma=False,
    )
```

```python
import functools

import jax
import jax.numpy as jnp
from jax import lax
from jax.experimental import pallas as pl
from jax.experimental.pallas import tpu as pltpu
from jax.sharding import PartitionSpec as P

NBY = 4
NBZ = 4
MESH = pl.DeviceIdType.MESH
XP, XM, YP, YM, ZP, ZM = 1, 2, 4, 8, 16, 32
ONE, UP, DOWN = 10, 14, 18
NONE = 1 << ONE
PAD = 8
PAIRS = [(ax, ay) for ax in (0, 1, -1) for ay in (0, 1, -1)]


def flag(ax, ay, az=0):
    return (
        {1: XP, -1: XM, 0: 0}[ax] | {1: YP, -1: YM, 0: 0}[ay] | {1: ZP, -1: ZM, 0: 0}[az]
    )


def holds(e, bits):
    return (e & bits) == bits


def kernel(n, dims, u_ref, vf_ref, mask_ref, code_ref, out_ref, ee, ff, fp, fm, inv, w0, wp, wm, avg,
           raw_m, raw_c, raw_f, ys_e, ys_f, yr_e, yr_f, xs_e, xr_e, xr_f, cr_e, cr_f,
           zs_e, zs_f, zr_e, zr_f, ts_e, ts_f, tr_e, tr_f, two_c, two_w, two_d, inj_c, inj_w, inj_d, load_sem, send_sem, recv_sem):
    fields, cx, cy, cz = dims
    chans = fields + 1
    nb = cy // 8 + 1
    pitch = 8 * nb
    me = lax.axis_index("boxes")
    bx, by, bz = me // (NBY * NBZ), me // NBZ % NBY, me % NBZ
    axes = {
        "x": (NBY * NBZ, bx > 0, bx < n // (NBY * NBZ) - 1),
        "y": (NBZ, by > 0, by < NBY - 1),
        "z": (1, bz > 0, bz < NBZ - 1),
    }
    lane = lax.broadcasted_iota(jnp.int32, (8, cz), 1)
    sub = lax.broadcasted_iota(jnp.int32, (8, cz), 0)
    first, final = lane == 0, lane == cz - 1
    ends = jnp.logical_or(first, final)
    odd = (lane & 1) == 1
    slot = lane - nb * ((lane * (4096 // nb + 1)) >> 12)

    loads = [
        pltpu.make_async_copy(mask_ref.at[0], raw_m, load_sem.at[0]),
        pltpu.make_async_copy(code_ref.at[0], raw_c, load_sem.at[1]),
        pltpu.make_async_copy(u_ref.at[0], raw_f.at[1:chans], load_sem.at[2]),
        pltpu.make_async_copy(vf_ref.at[0], raw_f.at[0], load_sem.at[3]),
    ]
    for copy in loads:
        copy.start()

    barrier = pltpu.get_barrier_semaphore()
    total = jnp.int32(0)
    for stride, low, high in axes.values():
        for has, there in ((low, me - stride), (high, me + stride)):
            @pl.when(has)
            def _():
                pl.semaphore_signal(barrier, inc=1, device_id=(there,), device_id_type=MESH)
            total = total + has.astype(jnp.int32)
    for dy in (1, -1):
        for dz in (-1, 1):
            has = jnp.logical_and(axes["y"][1 + (dy == 1)], axes["z"][1 + (dz == 1)])
            @pl.when(has)
            def _():
                pl.semaphore_signal(barrier, inc=1, device_id=(me + NBZ * dy + dz,), device_id_type=MESH)
            total = total + has.astype(jnp.int32)
    def copies(axis, ident, up, down):
        stride = axes[axis][0]
        out = []
        for d, (pair, there) in enumerate(((up, me + stride), (down, me - stride))):
            out.append(pltpu.make_async_remote_copy(
                src_ref=pair[0], dst_ref=pair[1], send_sem=send_sem.at[2 * ident + d],
                recv_sem=recv_sem.at[2 * ident + d], device_id=(there,), device_id_type=MESH))
        return axis, out

    def start(c):
        axis, (up, down) = c
        _, low, high = axes[axis]
        pl.when(high)(lambda: up.start())
        pl.when(low)(lambda: down.start())

    def recv(c):
        axis, (up, down) = c
        _, low, high = axes[axis]
        pl.when(low)(lambda: up.wait_recv())
        pl.when(high)(lambda: down.wait_recv())

    def sent(c):
        axis, (up, down) = c
        _, low, high = axes[axis]
        pl.when(high)(lambda: up.wait_send())
        pl.when(low)(lambda: down.wait_send())

    x_f = copies("x", 0, (raw_f.at[:, cx - 1:cx], xr_f.at[0]), (raw_f.at[:, 0:1], xr_f.at[1]))
    x_e = copies("x", 1, (xs_e.at[1], xr_e.at[0]), (xs_e.at[0], xr_e.at[1]))
    y_e = copies("y", 2, (ys_e.at[0], yr_e.at[0]), (ys_e.at[1], yr_e.at[1]))
    y_f = copies("y", 3, (ys_f.at[0], yr_f.at[0]), (ys_f.at[1], yr_f.at[1]))
    c_e = copies("x", 4, (yr_e.at[:, cx - 2:cx], cr_e.at[0]), (yr_e.at[:, 0:2], cr_e.at[1]))
    c_f = copies("x", 5, (yr_f.at[:, :, cx - 1:cx], cr_f.at[0]), (yr_f.at[:, :, 0:1], cr_f.at[1]))
    z_e = [copies("z", 6 + t, (zs_e.at[1], zr_e.at[t, 0]), (zs_e.at[0], zr_e.at[t, 1])) for t in (0, 1)]
    z_f = [copies("z", 8 + t, (zs_f.at[1], zr_f.at[t, 0]), (zs_f.at[0], zr_f.at[t, 1])) for t in (0, 1)]

    loads[0].wait()
    loads[1].wait()

    diagonal = []
    for d, dy in enumerate((1, -1)):
        for side, dz in enumerate((-1, 1)):
            to = jnp.logical_and(axes["y"][1 + (dy == 1)], axes["z"][1 + (dz == 1)])
            frm = jnp.logical_and(axes["y"][1 + (dy == -1)], axes["z"][1 + (dz == -1)])
            for ts, tr in ((ts_e, tr_e), (ts_f, tr_f)):
                at = 20 + len(diagonal)
                diagonal.append((to, frm, pltpu.make_async_remote_copy(
                    src_ref=ts.at[d, side], dst_ref=tr.at[d, 1 - side], send_sem=send_sem.at[at],
                    recv_sem=recv_sem.at[at], device_id=(me + NBZ * dy + dz,), device_id_type=MESH)))

    def row_of(p, y):
        return PAD + pitch * (p + 2) + 8 + y

    _, x_low, x_high = axes["x"]
    _, y_low, y_high = axes["y"]
    _, z_low, z_high = axes["z"]
    clear = lambda has, bits: jnp.where(has, 0, bits)
    row2 = lax.broadcasted_iota(jnp.int32, (cy, cz), 0)
    lane2 = lax.broadcasted_iota(jnp.int32, (cy, cz), 1)
    drop = (jnp.where(row2 == 0, clear(y_low, YM), 0) + jnp.where(row2 == cy - 1, clear(y_high, YP), 0)
            + jnp.where(lane2 == 0, clear(z_low, ZM + (1 << DOWN)), 0)
            + jnp.where(lane2 == cz - 1, clear(z_high, ZP + (1 << UP)), 0))
    keep = ~drop

    def encode(p, _):
        c = raw_c[p]
        cut = raw_m[p] == 1
        third = (c * 171) >> 9
        sz = c - 3 * third
        ninth = (third * 171) >> 9
        sy = third - 3 * ninth
        bit = lambda test, value: jnp.where(test, value, 0)
        e = (bit(ninth == 2, XP) + bit(ninth == 0, XM) + bit(sy == 2, YP) + bit(sy == 0, YM)
             + bit(sz == 2, ZP + (1 << UP)) + bit(sz == 0, ZM + (1 << DOWN)))
        off = jnp.where(p == 0, clear(x_low, XM), 0) + jnp.where(p == cx - 1, clear(x_high, XP), 0)
        ee[pl.ds(row_of(p, 0), cy), :] = (jnp.where(cut, e, 0) & keep & ~off) + NONE
        ys_e[0, p] = ee[pl.ds(row_of(p, cy - 2), 2), :]
        ys_e[1, p] = ee[pl.ds(row_of(p, 0), 2), :]
        return 0

    lax.fori_loop(0, cx, encode, 0)
    loads[2].wait()
    loads[3].wait()
    for c in range(chans):
        ys_f[0, c] = raw_f[c, :, cy - 1:cy, :]
        ys_f[1, c] = raw_f[c, :, 0:1, :]
    pl.semaphore_wait(barrier, total)
    start(y_e)
    start(y_f)

    def turn(v, amount):
        if isinstance(amount, int):
            return pltpu.roll(v, amount % cz, 1) if amount % cz else v
        return pltpu.roll(v, lax.rem(amount + cz, cz), 1)

    shifts = ((0, 1), (-1, -2))

    def pack(ks, e_of, f_of):
        at = [{d: lane == (k + d) % cz if isinstance(k, int) else lane == k + d for d in (-2, -1, 0, 1)} for k in ks]
        acc = {(side, j): zs_e[side, j] for side in (0, 1) for j in (0, 1)}
        for i, k in enumerate(ks):
            e = turn(e_of(i), k)
            for side, j in acc:
                acc[side, j] = jnp.where(at[i][shifts[side][j]], e, acc[side, j])
        for side, j in acc:
            zs_e[side, j] = acc[side, j]
        for c in range(chans):
            acc = [zs_f[side, c] for side in (0, 1)]
            for i, k in enumerate(ks):
                f = turn(f_of(i, c), k)
                acc = [jnp.where(at[i][shifts[side][0]], f, acc[side]) for side in (0, 1)]
            for side in (0, 1):
                zs_f[side, c] = acc[side]

    def settle(t, merge):
        for side, beside in enumerate((z_low, z_high)):
            at = []
            for has, rows_of in ((y_low, sub >= 4), (y_high, sub < 4)):
                both = jnp.full((8, cz), jnp.logical_and(has, beside).astype(jnp.int32), jnp.int32) == 1
                at.append(jnp.logical_and(jnp.logical_and(slot == 0, rows_of), both))
            for j in (0, 1):
                e = turn(zr_e[t, side, j], -shifts[1 - side][j])
                for i in (0, 1) if merge else ():
                    e = jnp.where(at[i], turn(tr_e[i, side], nb * i - j), e)
                zr_e[t, side, j] = e
            for c in range(chans):
                f = turn(zr_f[t, side, c], -shifts[1 - side][0])
                for i in (0, 1) if merge else ():
                    v = turn(tr_f[i, side], nb * i - c % 4)
                    f = jnp.where(at[i], v if c < 4 else pltpu.roll(v, 4, 0), f)
                zr_f[t, side, c] = f

    def pack_flat(ks):
        pack(ks, lambda i: ee[PAD + 8 * ks[i]:PAD + 8 * ks[i] + 8, :],
             lambda i, c: ff[c, PAD + 8 * ks[i]:PAD + 8 * ks[i] + 8, :])

    zs_e[...] = jnp.full(zs_e.shape, NONE, jnp.int32)
    zs_f[...] = jnp.zeros(zs_f.shape, jnp.float32)
    group = 4 if cx % 4 == 0 else 1

    def pack_own(group, places):
        def step(i, _):
            ks, where = [], []
            for j in range(group):
                p = i * group + j
                for c in range(chans):
                    for b in places:
                        ff[c, pl.ds(row_of(p, 8 * b), 8), :] = raw_f[c, p, 8 * b:8 * b + 8, :]
                for b in places:
                    ks.append((p + 2) * nb + 1 + b)
                    where.append((p, b))
            pack(ks, lambda i: ee[pl.ds(PAD + 8 * ks[i], 8), :],
                 lambda i, c: raw_f[c, where[i][0], 8 * where[i][1]:8 * where[i][1] + 8, :])
            return 0

        lax.fori_loop(0, cx // group, step, 0)

    pack_own(8 if cx % 8 == 0 else 1, (0, nb - 2))
    for d, source, direct in ((0, nb - 1, sub >= 4), (1, 1, sub < 4)):
        for side in (0, 1):
            back = [shift + source for shift in shifts[side]]
            ts_e[d, side] = jnp.where(slot == 0, turn(zs_e[side, 0], -back[0]), turn(zs_e[side, 1], 1 - back[1]))
            line = [None, None]
            for c in range(chans):
                v = turn(zs_f[side, c], c % 4 - back[0])
                line[c // 4] = v if c % 4 == 0 else jnp.where(slot == c % 4, v, line[c // 4])
            ts_f[d, side] = jnp.where(direct, line[0], pltpu.roll(line[1], 4, 0))
    for to, _, copy in diagonal:
        pl.when(to)(lambda: copy.start())
    pack_own(8 if cx % 8 == 0 else 1, range(1, nb - 2))
    start(z_e[0])
    start(z_f[0])
    for i in range(2):
        xs_e[0, i] = ee[row_of(i, 0):row_of(i, cy), :]
        xs_e[1, i] = ee[row_of(cx - 2 + i, 0):row_of(cx - 2 + i, cy), :]
    start(x_f)
    start(x_e)

    @pl.when(jnp.logical_not(x_low))
    def _():
        a, b = PAD, row_of(-1, cy + 2)
        ee[a:b, :] = jnp.full((b - a, cz), NONE, jnp.int32)

    @pl.when(jnp.logical_not(x_high))
    def _():
        a, b = row_of(cx, -2), row_of(cx + 1, cy + 8)
        ee[a:b, :] = jnp.full((b - a, cz), NONE, jnp.int32)

    for side, has in enumerate((y_low, y_high)):
        @pl.when(jnp.logical_not(has))
        def _():
            yr_e[side] = jnp.full(yr_e.shape[1:], NONE, jnp.int32)
            yr_f[side] = jnp.zeros(yr_f.shape[1:], jnp.float32)
    for side, has in enumerate((z_low, z_high)):
        @pl.when(jnp.logical_not(has))
        def _():
            for t in (0, 1):
                zr_e[t, side] = jnp.full(zr_e.shape[2:], NONE, jnp.int32)
                zr_f[t, side] = jnp.zeros(zr_f.shape[2:], jnp.float32)

    def rotate(ks):
        for k in ks:
            r = PAD + 8 * k
            for c in range(chans):
                v = ff[c, pl.ds(r, 8), :]
                fp[c, pl.ds(r, 8), :] = pltpu.roll(v, cz - 1, 1)
                fm[c, pl.ds(r, 8), :] = pltpu.roll(v, 1, 1)

    def rotate_own(i, _):
        rotate([(i * group + j + 2) * nb + 1 + b for j in range(group) for b in range(nb - 1)])
        return 0

    lax.fori_loop(0, cx // group, rotate_own, 0)

    zero = me // n
    low, high = x_low.astype(jnp.int32), x_high.astype(jnp.int32)

    def blocks(p0, p1, chunk, body):
        k0 = (p0 + 2) * nb
        steps = ((p1 - p0) * nb + chunk) // chunk

        def step(i, _):
            for j in range(chunk):
                k = k0 + i * chunk + j
                body(k, PAD + 8 * k)
            return 0

        lax.fori_loop(0, steps, step, 0)

    def rows(ref, lead, r):
        return ref[lead + (pl.ds(r, 8), slice(None))]

    def count_body(k, r):
        acc = rows(ee, (), r)
        for ax, ay in PAIRS[1:]:
            e = rows(ee, (), r - pitch * ax - ay)
            acc = acc + jnp.where(holds(e, flag(ax, ay)), e, 0)
        here = (acc >> ONE) & 15
        here = here + pltpu.roll((acc >> UP) & 15, 1, 1) + pltpu.roll((acc >> DOWN) & 15, cz - 1, 1)
        inv[pl.ds(r, 8), :] = 1.0 / here.astype(jnp.float32)

    def plane_blocks(p0, p1, places, body):
        def step(i, _):
            for j in (0, 1):
                for b in places:
                    k = (p0 + 2 * i + j + 2) * nb + b
                    body(k, PAD + 8 * k)
            return 0

        lax.fori_loop(0, (p1 - p0 + 1) // 2, step, 0)

    plane_blocks(low, cx - high, range(2, nb - 1), count_body)
    recv(y_e)
    start(c_e)
    for p in range(cx):
        ee[row_of(p, -2):row_of(p, 0), :] = yr_e[0, p]
        ee[row_of(p, cy):row_of(p, cy + 2), :] = yr_e[1, p]

    def edge(ref, lead, k):
        return turn(ref[(lax.rem(k, 2),) + lead], cz - k)

    def inverse_body(k, r):
        inv[pl.ds(r, 8), :] = jnp.where(ends, edge(inj_c, (), k), rows(inv, (), r))

    def weight_body(k, r):
        i = rows(inv, (), r)
        up, down = pltpu.roll(i, cz - 1, 1), pltpu.roll(i, 1, 1)
        w, up, down = i * rows(ff, (0,), r), up * rows(fp, (0,), r), down * rows(fm, (0,), r)
        for c in range(chans):
            g = edge(inj_w, (c,), k)
            v, a, b = (w, up, down) if c == 0 else (
                w * rows(ff, (c,), r), up * rows(fp, (c,), r), down * rows(fm, (c,), r))
            w0[c, pl.ds(r, 8), :] = v
            wp[c, pl.ds(r, 8), :] = v + jnp.where(final, g, a)
            wm[c, pl.ds(r, 8), :] = v + jnp.where(first, g, b)

    def weights(p0, p1, chunk):
        k0 = (p0 + 2) * nb
        steps = ((p1 - p0) * nb + chunk) // chunk

        def step(i, _):
            before = k0 + jnp.maximum(i - 1, 0) * chunk
            for j in range(chunk):
                weight_body(before + j, PAD + 8 * (before + j))
            for j in range(chunk):
                k = k0 + i * chunk + j
                inverse_body(k, PAD + 8 * k)
            return 0

        lax.fori_loop(0, steps + 1, step, 0)

    def average_body(k, r):
        e = rows(ee, (), r)
        m = {b: holds(e, b) for b in (XP, XM, YP, YM, ZP, ZM)}

        def along_z(c, q):
            return jnp.where(m[ZP], rows(wp, (c,), q), jnp.where(m[ZM], rows(wm, (c,), q), rows(w0, (c,), q)))

        def along_y(c, q):
            side = jnp.where(m[YP], along_z(c, q + 1), jnp.where(m[YM], along_z(c, q - 1), 0.0))
            return along_z(c, q) + side

        def whole(c):
            side = jnp.where(m[XP], along_y(c, r + pitch), jnp.where(m[XM], along_y(c, r - pitch), 0.0))
            return along_y(c, r) + side

        inverse = 1.0 / whole(0)
        for c in range(1, chans):
            avg[c - 1, pl.ds(r, 8), :] = whole(c) * inverse

    def deposit_body(p, b):
        k = (p + 2) * nb + 1 + b
        r = PAD + 8 * k
        acc = [[None] * 3 for _ in range(fields)]
        for ax, ay in PAIRS:
            s = r - pitch * ax - ay
            e = rows(ee, (), s)
            ms = [holds(e, flag(ax, ay, az)) for az in (0, 1, -1)]
            for f in range(fields):
                v = rows(avg, (f,), s)
                for i in range(3):
                    term = v if (ax, ay, i) == (0, 0, 0) else jnp.where(ms[i], v, 0.0)
                    acc[f][i] = term if acc[f][i] is None else acc[f][i] + term
        i = rows(inv, (), r)
        for f in range(fields):
            here, up, down = acc[f]
            g = edge(inj_d, (f,), k)
            here = here + jnp.where(first, g, pltpu.roll(up, 1, 1))
            here = here + jnp.where(final, g, pltpu.roll(down, cz - 1, 1))
            out_ref[0, f, p, 8 * b:8 * b + 8, :] = here * i

    def deposit(p0, p1):
        def plane(i, _):
            for b in range(nb - 1):
                deposit_body(p0 + i, b)
            return 0

        lax.fori_loop(0, p1 - p0, plane, 0)

    def shift_y(v, dy):
        if dy == 0:
            return v
        w = pltpu.roll(v, 7 if dy == 1 else 1, 0)
        return jnp.where(sub == (7 if dy == 1 else 0), turn(w, -dy), w)

    def shift_x(v, dx):
        return turn(v, -nb * dx) if dx else v

    def spread(t):
        lines = {ax: t[ax, 0] + shift_y(t[ax, 1], -1) + shift_y(t[ax, -1], 1) for ax in (0, 1, -1)}
        return lines[0] + shift_x(lines[1], -1) + shift_x(lines[-1], 1)

    def ghost(t, side):
        toward, away = (ZP, ZM) if side == 0 else (ZM, ZP)
        e0, e1 = (turn(zs_e[side, j], -shifts[side][j]) for j in (0, 1))
        g0, g1 = zr_e[t, side, 0], zr_e[t, side, 1]
        own = [turn(zs_f[side, c], -shifts[side][0]) for c in range(chans)]
        from_g0 = jnp.where(holds(g0, toward), 257, 1)
        from_e0 = jnp.where(holds(e0, away), 257, 256)
        found = {}
        for ax, ay in PAIRS:
            b = flag(ax, ay)
            found[ax, ay] = (jnp.where(holds(g1, b | toward), 1, 0) + jnp.where(holds(g0, b), from_g0, 0)
                             + jnp.where(holds(e0, b), from_e0, 0) + jnp.where(holds(e1, b | away), 256, 0))
        found = spread(found)
        i_ghost = 1.0 / (found & 255).astype(jnp.float32)
        i_own = 1.0 / (found >> 8).astype(jnp.float32)
        two_c[side] = i_own
        w_ghost, w_own = zr_f[t, side, 0] * i_ghost, own[0] * i_own
        m = {b: holds(g0, b) for b in (XP, XM, YP, YM)}
        mine = holds(g0, toward)
        inverse = None
        for c in range(chans):
            v = w_ghost if c == 0 else w_ghost * zr_f[t, side, c]
            two_w[side, c] = v
            v = v + (w_own if c == 0 else w_own * own[c])
            above, below = shift_y(v, 1), shift_y(v, -1)
            line = {dx: shift_x(v, dx) + jnp.where(m[YP], shift_x(above, dx), jnp.where(m[YM], shift_x(below, dx), 0.0))
                    for dx in (0, 1, -1)}
            whole = line[0] + jnp.where(m[XP], line[1], jnp.where(m[XM], line[-1], 0.0))
            if c == 0:
                inverse = 1.0 / whole
                continue
            a = jnp.where(mine, whole * inverse, 0.0)
            two_d[side, c - 1] = spread({
                (ax, ay): jnp.where(holds(g0, flag(ax, ay)), a, 0.0) if (ax, ay) != (0, 0) else a
                for ax, ay in PAIRS})

    def ghosts(t):
        for side in (0, 1):
            ghost(t, side)
        pairs = [(two_c, inj_c, ())] + [(two_w, inj_w, (c,)) for c in range(chans)]
        for two, inj, lead in pairs + [(two_d, inj_d, (f,)) for f in range(fields)]:
            below, above = two[(0,) + lead], turn(two[(1,) + lead], -1)
            inj[(0,) + lead] = jnp.where(odd, above, below)
            inj[(1,) + lead] = jnp.where(odd, below, above)

    plane_blocks(low, cx - high + 1, (0, 1, nb - 1), count_body)
    recv(y_f)
    start(c_f)
    for c in (z_e[0], z_f[0]):
        recv(c)
        sent(c)
    for _, frm, copy in diagonal:
        pl.when(frm)(lambda: copy.wait_recv())
    for p in range(cx):
        for c in range(chans):
            ff[c, row_of(p, -1):row_of(p, 0), :] = yr_f[0, c, p]
            ff[c, row_of(p, cy):row_of(p, cy + 1), :] = yr_f[1, c, p]
    pack_flat([(p + 2) * nb for p in range(cx + 1)])
    rotate([(p + 2) * nb for p in range(cx + 1)])
    settle(0, True)
    ghosts(0)
    weights(low, cx - high, 10)
    blocks(2 * low, cx - 2 * high, 5, average_body)

    for c in (x_f, x_e, c_e, c_f):
        recv(c)
    for side, has in enumerate((x_low, x_high)):
        @pl.when(has)
        def _():
            for i in range(2):
                p = (i - 2, cx + i)[side]
                ee[row_of(p, 0):row_of(p, cy), :] = xr_e[side, i]
                ee[row_of(p, -2):row_of(p, 0), :] = cr_e[side, 0, i]
                ee[row_of(p, cy):row_of(p, cy + 2), :] = cr_e[side, 1, i]
            p = (-1, cx)[side]
            for c in range(chans):
                ff[c, row_of(p, 0):row_of(p, cy), :] = xr_f[side, c, 0]
                ff[c, row_of(p, -1):row_of(p, 0), :] = cr_f[side, 0, c, 0]
                ff[c, row_of(p, cy):row_of(p, cy + 1), :] = cr_f[side, 1, c, 0]
            k = (0, (cx + 2) * nb)[side]
            pack_flat(list(range(k, k + 2 * nb + 1)))
            k = (nb, (cx + 2) * nb)[side]
            rotate(range(k, k + nb + 1))
    start(z_e[1])
    start(z_f[1])
    edges = ((low, -1, 1), (high, cx - 1, cx + 1))
    for has, a, b in edges:
        @pl.when(has == 1)
        def _():
            blocks(zero + a, b, 6, count_body)
    deposit(3 * low, cx - 3 * high)

    recv(z_e[1])
    recv(z_f[1])
    settle(1, False)
    ghosts(1)
    for has, a, b in edges:
        @pl.when(has == 1)
        def _():
            weights(zero + a, b, 6)
            a2, b2 = (a, b + 1) if a < 0 else (a - 1, b)
            blocks(zero + a2, b2, 4, average_body)
            a3, b3 = (0, 3) if a < 0 else (cx - 3, cx)
            deposit(zero + a3, b3)
    for c in [x_f, x_e, y_e, y_f, c_e, c_f, z_e[1], z_f[1]]:
        sent(c)
    for to, _, copy in diagonal:
        pl.when(to)(lambda: copy.wait_send())


def per_device(n, conserved, volume_fraction, cut_mask, merge_code):
    fields, cx, cy, cz = conserved.shape[1:]
    chans = fields + 1
    flat = PAD + (cx + 4) * (cy + 8) + 2 * (cy + 8) + 64
    f32, i32 = jnp.float32, jnp.int32
    V = pltpu.VMEM
    scratch = [
        V((flat, cz), i32), V((chans, flat, cz), f32), V((chans, flat, cz), f32), V((chans, flat, cz), f32),
        V((flat, cz), f32),
        V((chans, flat, cz), f32), V((chans, flat, cz), f32), V((chans, flat, cz), f32),
        V((fields, flat, cz), f32),
        V((cx, cy, cz), i32), V((cx, cy, cz), i32), V((chans, cx, cy, cz), f32),
        V((2, cx, 2, cz), i32), V((2, chans, cx, 1, cz), f32),
        V((2, cx, 2, cz), i32), V((2, chans, cx, 1, cz), f32),
        V((2, 2, cy, cz), i32), V((2, 2, cy, cz), i32), V((2, chans, 1, cy, cz), f32),
        V((2, 2, 2, 2, cz), i32), V((2, 2, chans, 1, 1, cz), f32),
        V((2, 2, 8, cz), i32), V((2, chans, 8, cz), f32),
        V((2, 2, 2, 8, cz), i32), V((2, 2, chans, 8, cz), f32),
        V((2, 2, 8, cz), i32), V((2, 2, 8, cz), f32), V((2, 2, 8, cz), i32), V((2, 2, 8, cz), f32),
        V((2, 8, cz), f32), V((2, chans, 8, cz), f32), V((2, fields, 8, cz), f32),
        V((2, 8, cz), f32), V((2, chans, 8, cz), f32), V((2, fields, 8, cz), f32),
        pltpu.SemaphoreType.DMA((4,)), pltpu.SemaphoreType.DMA((28,)), pltpu.SemaphoreType.DMA((28,)),
    ]
    return pl.pallas_call(
        functools.partial(kernel, n, (fields, cx, cy, cz)),
        out_shape=pltpu.VMEM(conserved.shape, f32),
        in_specs=[pl.BlockSpec(memory_space=pl.ANY)] * 4,
        out_specs=pl.BlockSpec(memory_space=pltpu.VMEM),
        scratch_shapes=scratch,
        compiler_params=pltpu.CompilerParams(
            collective_id=0, has_side_effects=True, vmem_limit_bytes=60 * 1024 * 1024),
        name="redistribute",
    )(conserved, volume_fraction, cut_mask, merge_code)


def solution(mesh):
    return jax.shard_map(
        functools.partial(per_device, mesh.shape["boxes"]),
        mesh=mesh,
        in_specs=(
            P("boxes", None, None, None, None),
            P("boxes", None, None, None),
            P("boxes", None, None, None),
            P("boxes", None, None, None),
        ),
        out_specs=P("boxes", None, None, None, None),
        check_vma=False,
    )
```

```python
import functools

import jax
import jax.numpy as jnp
from jax import lax
from jax.experimental import pallas as pl
from jax.experimental.pallas import tpu as pltpu
from jax.sharding import PartitionSpec as P

NBY = 4
NBZ = 4
MESH = pl.DeviceIdType.MESH
XP, XM, YP, YM, ZP, ZM = 1, 2, 4, 8, 16, 32
ONE, UP, DOWN = 10, 14, 18
NONE = 1 << ONE
PAD = 8
PAIRS = [(ax, ay) for ax in (0, 1, -1) for ay in (0, 1, -1)]


def flag(ax, ay, az=0):
    return (
        {1: XP, -1: XM, 0: 0}[ax] | {1: YP, -1: YM, 0: 0}[ay] | {1: ZP, -1: ZM, 0: 0}[az]
    )


def holds(e, bits):
    return (e & bits) == bits


def kernel(n, dims, u_ref, vf_ref, mask_ref, code_ref, out_ref, ee, ff, fp, fm, inv, w0, wp, wm, avg,
           raw_m, raw_c, raw_f, ys_e, ys_f, yr_e, yr_f, xs_e, xr_e, xr_f, cr_e, cr_f,
           zs_e, zs_f, zr_e, zr_f, ts_e, ts_f, tr_e, tr_f, two_c, two_w, two_d, inj_c, inj_w, inj_d, load_sem, send_sem, recv_sem):
    fields, cx, cy, cz = dims
    chans = fields + 1
    nb = cy // 8 + 1
    pitch = 8 * nb
    me = lax.axis_index("boxes")
    bx, by, bz = me // (NBY * NBZ), me // NBZ % NBY, me % NBZ
    axes = {
        "x": (NBY * NBZ, bx > 0, bx < n // (NBY * NBZ) - 1),
        "y": (NBZ, by > 0, by < NBY - 1),
        "z": (1, bz > 0, bz < NBZ - 1),
    }
    lane = lax.broadcasted_iota(jnp.int32, (8, cz), 1)
    sub = lax.broadcasted_iota(jnp.int32, (8, cz), 0)
    first, final = lane == 0, lane == cz - 1
    ends = jnp.logical_or(first, final)
    odd = (lane & 1) == 1
    slot = lane - nb * ((lane * (4096 // nb + 1)) >> 12)

    loads = [
        pltpu.make_async_copy(mask_ref.at[0], raw_m, load_sem.at[0]),
        pltpu.make_async_copy(code_ref.at[0], raw_c, load_sem.at[1]),
        pltpu.make_async_copy(u_ref.at[0], raw_f.at[1:chans], load_sem.at[2]),
        pltpu.make_async_copy(vf_ref.at[0], raw_f.at[0], load_sem.at[3]),
    ]
    for copy in loads:
        copy.start()

    barrier = pltpu.get_barrier_semaphore()
    total = jnp.int32(0)
    for stride, low, high in axes.values():
        for has, there in ((low, me - stride), (high, me + stride)):
            @pl.when(has)
            def _():
                pl.semaphore_signal(barrier, inc=1, device_id=(there,), device_id_type=MESH)
            total = total + has.astype(jnp.int32)
    for dy in (1, -1):
        for dz in (-1, 1):
            has = jnp.logical_and(axes["y"][1 + (dy == 1)], axes["z"][1 + (dz == 1)])
            @pl.when(has)
            def _():
                pl.semaphore_signal(barrier, inc=1, device_id=(me + NBZ * dy + dz,), device_id_type=MESH)
            total = total + has.astype(jnp.int32)
    def copies(axis, ident, up, down):
        stride = axes[axis][0]
        out = []
        for d, (pair, there) in enumerate(((up, me + stride), (down, me - stride))):
            out.append(pltpu.make_async_remote_copy(
                src_ref=pair[0], dst_ref=pair[1], send_sem=send_sem.at[2 * ident + d],
                recv_sem=recv_sem.at[2 * ident + d], device_id=(there,), device_id_type=MESH))
        return axis, out

    def start(c):
        axis, (up, down) = c
        _, low, high = axes[axis]
        pl.when(high)(lambda: up.start())
        pl.when(low)(lambda: down.start())

    def recv(c):
        axis, (up, down) = c
        _, low, high = axes[axis]
        pl.when(low)(lambda: up.wait_recv())
        pl.when(high)(lambda: down.wait_recv())

    def sent(c):
        axis, (up, down) = c
        _, low, high = axes[axis]
        pl.when(high)(lambda: up.wait_send())
        pl.when(low)(lambda: down.wait_send())

    x_f = copies("x", 0, (raw_f.at[:, cx - 1:cx], xr_f.at[0]), (raw_f.at[:, 0:1], xr_f.at[1]))
    x_e = copies("x", 1, (xs_e.at[1], xr_e.at[0]), (xs_e.at[0], xr_e.at[1]))
    y_e = copies("y", 2, (ys_e.at[0], yr_e.at[0]), (ys_e.at[1], yr_e.at[1]))
    y_f = copies("y", 3, (ys_f.at[0], yr_f.at[0]), (ys_f.at[1], yr_f.at[1]))
    c_e = copies("x", 4, (yr_e.at[:, cx - 2:cx], cr_e.at[0]), (yr_e.at[:, 0:2], cr_e.at[1]))
    c_f = copies("x", 5, (yr_f.at[:, :, cx - 1:cx], cr_f.at[0]), (yr_f.at[:, :, 0:1], cr_f.at[1]))
    z_e = [copies("z", 6 + t, (zs_e.at[1], zr_e.at[t, 0]), (zs_e.at[0], zr_e.at[t, 1])) for t in (0, 1)]
    z_f = [copies("z", 8 + t, (zs_f.at[1], zr_f.at[t, 0]), (zs_f.at[0], zr_f.at[t, 1])) for t in (0, 1)]

    loads[0].wait()
    loads[1].wait()

    diagonal = []
    for d, dy in enumerate((1, -1)):
        for side, dz in enumerate((-1, 1)):
            to = jnp.logical_and(axes["y"][1 + (dy == 1)], axes["z"][1 + (dz == 1)])
            frm = jnp.logical_and(axes["y"][1 + (dy == -1)], axes["z"][1 + (dz == -1)])
            for ts, tr in ((ts_e, tr_e), (ts_f, tr_f)):
                at = 20 + len(diagonal)
                diagonal.append((to, frm, pltpu.make_async_remote_copy(
                    src_ref=ts.at[d, side], dst_ref=tr.at[d, 1 - side], send_sem=send_sem.at[at],
                    recv_sem=recv_sem.at[at], device_id=(me + NBZ * dy + dz,), device_id_type=MESH)))

    def row_of(p, y):
        return PAD + pitch * (p + 2) + 8 + y

    _, x_low, x_high = axes["x"]
    _, y_low, y_high = axes["y"]
    _, z_low, z_high = axes["z"]
    clear = lambda has, bits: jnp.where(has, 0, bits)
    row2 = lax.broadcasted_iota(jnp.int32, (cy, cz), 0)
    lane2 = lax.broadcasted_iota(jnp.int32, (cy, cz), 1)
    drop = (jnp.where(row2 == 0, clear(y_low, YM), 0) + jnp.where(row2 == cy - 1, clear(y_high, YP), 0)
            + jnp.where(lane2 == 0, clear(z_low, ZM + (1 << DOWN)), 0)
            + jnp.where(lane2 == cz - 1, clear(z_high, ZP + (1 << UP)), 0))
    keep = ~drop

    def encode(p, _):
        c = raw_c[p]
        cut = raw_m[p] == 1
        third = (c * 171) >> 9
        sz = c - 3 * third
        ninth = (third * 171) >> 9
        sy = third - 3 * ninth
        bit = lambda test, value: jnp.where(test, value, 0)
        e = (bit(ninth == 2, XP) + bit(ninth == 0, XM) + bit(sy == 2, YP) + bit(sy == 0, YM)
             + bit(sz == 2, ZP + (1 << UP)) + bit(sz == 0, ZM + (1 << DOWN)))
        off = jnp.where(p == 0, clear(x_low, XM), 0) + jnp.where(p == cx - 1, clear(x_high, XP), 0)
        ee[pl.ds(row_of(p, 0), cy), :] = (jnp.where(cut, e, 0) & keep & ~off) + NONE
        ys_e[0, p] = ee[pl.ds(row_of(p, cy - 2), 2), :]
        ys_e[1, p] = ee[pl.ds(row_of(p, 0), 2), :]
        return 0

    lax.fori_loop(0, cx, encode, 0)
    loads[2].wait()
    loads[3].wait()
    for c in range(chans):
        ys_f[0, c] = raw_f[c, :, cy - 1:cy, :]
        ys_f[1, c] = raw_f[c, :, 0:1, :]
    pl.semaphore_wait(barrier, total)
    start(y_e)
    start(y_f)

    def turn(v, amount):
        if isinstance(amount, int):
            return pltpu.roll(v, amount % cz, 1) if amount % cz else v
        return pltpu.roll(v, lax.rem(amount + cz, cz), 1)

    shifts = ((0, 1), (-1, -2))

    def pack(ks, e_of, f_of):
        at = [{d: lane == (k + d) % cz if isinstance(k, int) else lane == k + d for d in (-2, -1, 0, 1)} for k in ks]
        acc = {(side, j): zs_e[side, j] for side in (0, 1) for j in (0, 1)}
        for i, k in enumerate(ks):
            e = turn(e_of(i), k)
            for side, j in acc:
                acc[side, j] = jnp.where(at[i][shifts[side][j]], e, acc[side, j])
        for side, j in acc:
            zs_e[side, j] = acc[side, j]
        for c in range(chans):
            acc = [zs_f[side, c] for side in (0, 1)]
            for i, k in enumerate(ks):
                f = turn(f_of(i, c), k)
                acc = [jnp.where(at[i][shifts[side][0]], f, acc[side]) for side in (0, 1)]
            for side in (0, 1):
                zs_f[side, c] = acc[side]

    def settle(t, merge):
        for side, beside in enumerate((z_low, z_high)):
            at = []
            for has, rows_of in ((y_low, sub >= 4), (y_high, sub < 4)):
                both = jnp.full((8, cz), jnp.logical_and(has, beside).astype(jnp.int32), jnp.int32) == 1
                at.append(jnp.logical_and(jnp.logical_and(slot == 0, rows_of), both))
            for j in (0, 1):
                e = turn(zr_e[t, side, j], -shifts[1 - side][j])
                for i in (0, 1) if merge else ():
                    e = jnp.where(at[i], turn(tr_e[i, side], nb * i - j), e)
                zr_e[t, side, j] = e
            for c in range(chans):
                f = turn(zr_f[t, side, c], -shifts[1 - side][0])
                for i in (0, 1) if merge else ():
                    v = turn(tr_f[i, side], nb * i - c % 4)
                    f = jnp.where(at[i], v if c < 4 else pltpu.roll(v, 4, 0), f)
                zr_f[t, side, c] = f

    def pack_flat(ks):
        pack(ks, lambda i: ee[PAD + 8 * ks[i]:PAD + 8 * ks[i] + 8, :],
             lambda i, c: ff[c, PAD + 8 * ks[i]:PAD + 8 * ks[i] + 8, :])

    zs_e[...] = jnp.full(zs_e.shape, NONE, jnp.int32)
    zs_f[...] = jnp.zeros(zs_f.shape, jnp.float32)
    group = 4 if cx % 4 == 0 else 1

    def pack_own(group, places):
        def step(i, _):
            ks, where = [], []
            for j in range(group):
                p = i * group + j
                for c in range(chans):
                    for b in places:
                        ff[c, pl.ds(row_of(p, 8 * b), 8), :] = raw_f[c, p, 8 * b:8 * b + 8, :]
                for b in places:
                    ks.append((p + 2) * nb + 1 + b)
                    where.append((p, b))
            pack(ks, lambda i: ee[pl.ds(PAD + 8 * ks[i], 8), :],
                 lambda i, c: raw_f[c, where[i][0], 8 * where[i][1]:8 * where[i][1] + 8, :])
            return 0

        lax.fori_loop(0, cx // group, step, 0)

    pack_own(8 if cx % 8 == 0 else 1, (0, nb - 2))
    for d, source, direct in ((0, nb - 1, sub >= 4), (1, 1, sub < 4)):
        for side in (0, 1):
            back = [shift + source for shift in shifts[side]]
            ts_e[d, side] = jnp.where(slot == 0, turn(zs_e[side, 0], -back[0]), turn(zs_e[side, 1], 1 - back[1]))
            line = [None, None]
            for c in range(chans):
                v = turn(zs_f[side, c], c % 4 - back[0])
                line[c // 4] = v if c % 4 == 0 else jnp.where(slot == c % 4, v, line[c // 4])
            ts_f[d, side] = jnp.where(direct, line[0], pltpu.roll(line[1], 4, 0))
    for to, _, copy in diagonal:
        pl.when(to)(lambda: copy.start())
    pack_own(8 if cx % 8 == 0 else 1, range(1, nb - 2))
    start(z_e[0])
    start(z_f[0])
    for i in range(2):
        xs_e[0, i] = ee[row_of(i, 0):row_of(i, cy), :]
        xs_e[1, i] = ee[row_of(cx - 2 + i, 0):row_of(cx - 2 + i, cy), :]
    start(x_f)
    start(x_e)

    @pl.when(jnp.logical_not(x_low))
    def _():
        a, b = PAD, row_of(-1, cy + 2)
        ee[a:b, :] = jnp.full((b - a, cz), NONE, jnp.int32)

    @pl.when(jnp.logical_not(x_high))
    def _():
        a, b = row_of(cx, -2), row_of(cx + 1, cy + 8)
        ee[a:b, :] = jnp.full((b - a, cz), NONE, jnp.int32)

    for side, has in enumerate((y_low, y_high)):
        @pl.when(jnp.logical_not(has))
        def _():
            yr_e[side] = jnp.full(yr_e.shape[1:], NONE, jnp.int32)
            yr_f[side] = jnp.zeros(yr_f.shape[1:], jnp.float32)
    for side, has in enumerate((z_low, z_high)):
        @pl.when(jnp.logical_not(has))
        def _():
            for t in (0, 1):
                zr_e[t, side] = jnp.full(zr_e.shape[2:], NONE, jnp.int32)
                zr_f[t, side] = jnp.zeros(zr_f.shape[2:], jnp.float32)

    def rotate(ks):
        for k in ks:
            r = PAD + 8 * k
            for c in range(chans):
                v = ff[c, pl.ds(r, 8), :]
                fp[c, pl.ds(r, 8), :] = pltpu.roll(v, cz - 1, 1)
                fm[c, pl.ds(r, 8), :] = pltpu.roll(v, 1, 1)

    def rotate_own(i, _):
        rotate([(i * group + j + 2) * nb + 1 + b for j in range(group) for b in range(nb - 1)])
        return 0

    lax.fori_loop(0, cx // group, rotate_own, 0)

    zero = me // n
    low, high = x_low.astype(jnp.int32), x_high.astype(jnp.int32)

    def blocks(p0, p1, chunk, body):
        k0 = (p0 + 2) * nb
        steps = ((p1 - p0) * nb + chunk) // chunk

        def step(i, _):
            for j in range(chunk):
                k = k0 + i * chunk + j
                body(k, PAD + 8 * k)
            return 0

        lax.fori_loop(0, steps, step, 0)

    def rows(ref, lead, r):
        return ref[lead + (pl.ds(r, 8), slice(None))]

    def count_body(k, r):
        acc = rows(ee, (), r)
        for ax, ay in PAIRS[1:]:
            e = rows(ee, (), r - pitch * ax - ay)
            acc = acc + jnp.where(holds(e, flag(ax, ay)), e, 0)
        here = (acc >> ONE) & 15
        here = here + pltpu.roll((acc >> UP) & 15, 1, 1) + pltpu.roll((acc >> DOWN) & 15, cz - 1, 1)
        inv[pl.ds(r, 8), :] = 1.0 / here.astype(jnp.float32)

    def plane_blocks(p0, p1, places, body):
        def step(i, _):
            for j in (0, 1):
                for b in places:
                    k = (p0 + 2 * i + j + 2) * nb + b
                    body(k, PAD + 8 * k)
            return 0

        lax.fori_loop(0, (p1 - p0 + 1) // 2, step, 0)

    plane_blocks(low, cx - high, range(2, nb - 1), count_body)
    recv(y_e)
    start(c_e)
    for p in range(cx):
        ee[row_of(p, -2):row_of(p, 0), :] = yr_e[0, p]
        ee[row_of(p, cy):row_of(p, cy + 2), :] = yr_e[1, p]

    def edge(ref, lead, k):
        return turn(ref[(lax.rem(k, 2),) + lead], cz - k)

    def inverse_body(k, r):
        inv[pl.ds(r, 8), :] = jnp.where(ends, edge(inj_c, (), k), rows(inv, (), r))

    def weight_body(k, r):
        i = rows(inv, (), r)
        up, down = pltpu.roll(i, cz - 1, 1), pltpu.roll(i, 1, 1)
        w, up, down = i * rows(ff, (0,), r), up * rows(fp, (0,), r), down * rows(fm, (0,), r)
        for c in range(chans):
            g = edge(inj_w, (c,), k)
            v, a, b = (w, up, down) if c == 0 else (
                w * rows(ff, (c,), r), up * rows(fp, (c,), r), down * rows(fm, (c,), r))
            w0[c, pl.ds(r, 8), :] = v
            wp[c, pl.ds(r, 8), :] = v + jnp.where(final, g, a)
            wm[c, pl.ds(r, 8), :] = v + jnp.where(first, g, b)

    def weights(p0, p1, chunk):
        k0 = (p0 + 2) * nb
        steps = ((p1 - p0) * nb + chunk) // chunk

        def step(i, _):
            before = k0 + jnp.maximum(i - 1, 0) * chunk
            for j in range(chunk):
                weight_body(before + j, PAD + 8 * (before + j))
            for j in range(chunk):
                k = k0 + i * chunk + j
                inverse_body(k, PAD + 8 * k)
            return 0

        lax.fori_loop(0, steps + 1, step, 0)

    def average_body(k, r):
        e = rows(ee, (), r)
        m = {b: holds(e, b) for b in (XP, XM, YP, YM, ZP, ZM)}

        def along_z(c, q):
            return jnp.where(m[ZP], rows(wp, (c,), q), jnp.where(m[ZM], rows(wm, (c,), q), rows(w0, (c,), q)))

        def along_y(c, q):
            side = jnp.where(m[YP], along_z(c, q + 1), jnp.where(m[YM], along_z(c, q - 1), 0.0))
            return along_z(c, q) + side

        def whole(c):
            side = jnp.where(m[XP], along_y(c, r + pitch), jnp.where(m[XM], along_y(c, r - pitch), 0.0))
            return along_y(c, r) + side

        inverse = 1.0 / whole(0)
        for c in range(1, chans):
            avg[c - 1, pl.ds(r, 8), :] = whole(c) * inverse

    def deposit_body(p, b):
        k = (p + 2) * nb + 1 + b
        r = PAD + 8 * k
        acc = [[None] * 3 for _ in range(fields)]
        for ax, ay in PAIRS:
            s = r - pitch * ax - ay
            e = rows(ee, (), s)
            ms = [holds(e, flag(ax, ay, az)) for az in (0, 1, -1)]
            for f in range(fields):
                v = rows(avg, (f,), s)
                for i in range(3):
                    term = v if (ax, ay, i) == (0, 0, 0) else jnp.where(ms[i], v, 0.0)
                    acc[f][i] = term if acc[f][i] is None else acc[f][i] + term
        i = rows(inv, (), r)
        for f in range(fields):
            here, up, down = acc[f]
            g = edge(inj_d, (f,), k)
            here = here + jnp.where(first, g, pltpu.roll(up, 1, 1))
            here = here + jnp.where(final, g, pltpu.roll(down, cz - 1, 1))
            out_ref[0, f, p, 8 * b:8 * b + 8, :] = here * i

    def deposit(p0, p1):
        def plane(i, _):
            for b in range(nb - 1):
                deposit_body(p0 + i, b)
            return 0

        lax.fori_loop(0, p1 - p0, plane, 0)

    def shift_y(v, dy):
        if dy == 0:
            return v
        w = pltpu.roll(v, 7 if dy == 1 else 1, 0)
        return jnp.where(sub == (7 if dy == 1 else 0), turn(w, -dy), w)

    def shift_x(v, dx):
        return turn(v, -nb * dx) if dx else v

    def spread(t):
        lines = {ax: t[ax, 0] + shift_y(t[ax, 1], -1) + shift_y(t[ax, -1], 1) for ax in (0, 1, -1)}
        return lines[0] + shift_x(lines[1], -1) + shift_x(lines[-1], 1)

    def ghost(t, side):
        toward, away = (ZP, ZM) if side == 0 else (ZM, ZP)
        e0, e1 = (turn(zs_e[side, j], -shifts[side][j]) for j in (0, 1))
        g0, g1 = zr_e[t, side, 0], zr_e[t, side, 1]
        own = [turn(zs_f[side, c], -shifts[side][0]) for c in range(chans)]
        from_g0 = jnp.where(holds(g0, toward), 257, 1)
        from_e0 = jnp.where(holds(e0, away), 257, 256)
        found = {}
        for ax, ay in PAIRS:
            b = flag(ax, ay)
            found[ax, ay] = (jnp.where(holds(g1, b | toward), 1, 0) + jnp.where(holds(g0, b), from_g0, 0)
                             + jnp.where(holds(e0, b), from_e0, 0) + jnp.where(holds(e1, b | away), 256, 0))
        found = spread(found)
        i_ghost = 1.0 / (found & 255).astype(jnp.float32)
        i_own = 1.0 / (found >> 8).astype(jnp.float32)
        two_c[side] = i_own
        w_ghost, w_own = zr_f[t, side, 0] * i_ghost, own[0] * i_own
        m = {b: holds(g0, b) for b in (XP, XM, YP, YM)}
        mine = holds(g0, toward)
        inverse = None
        for c in range(chans):
            v = w_ghost if c == 0 else w_ghost * zr_f[t, side, c]
            two_w[side, c] = v
            v = v + (w_own if c == 0 else w_own * own[c])
            above, below = shift_y(v, 1), shift_y(v, -1)
            line = {dx: shift_x(v, dx) + jnp.where(m[YP], shift_x(above, dx), jnp.where(m[YM], shift_x(below, dx), 0.0))
                    for dx in (0, 1, -1)}
            whole = line[0] + jnp.where(m[XP], line[1], jnp.where(m[XM], line[-1], 0.0))
            if c == 0:
                inverse = 1.0 / whole
                continue
            a = jnp.where(mine, whole * inverse, 0.0)
            two_d[side, c - 1] = spread({
                (ax, ay): jnp.where(holds(g0, flag(ax, ay)), a, 0.0) if (ax, ay) != (0, 0) else a
                for ax, ay in PAIRS})

    def ghosts(t):
        for side in (0, 1):
            ghost(t, side)
        pairs = [(two_c, inj_c, ())] + [(two_w, inj_w, (c,)) for c in range(chans)]
        for two, inj, lead in pairs + [(two_d, inj_d, (f,)) for f in range(fields)]:
            below, above = two[(0,) + lead], turn(two[(1,) + lead], -1)
            inj[(0,) + lead] = jnp.where(odd, above, below)
            inj[(1,) + lead] = jnp.where(odd, below, above)

    plane_blocks(low, cx - high + 1, (0, 1, nb - 1), count_body)
    recv(y_f)
    start(c_f)
    for c in (z_e[0], z_f[0]):
        recv(c)
        sent(c)
    for _, frm, copy in diagonal:
        pl.when(frm)(lambda: copy.wait_recv())
    for p in range(cx):
        for c in range(chans):
            ff[c, row_of(p, -1):row_of(p, 0), :] = yr_f[0, c, p]
            ff[c, row_of(p, cy):row_of(p, cy + 1), :] = yr_f[1, c, p]
    pack_flat([(p + 2) * nb for p in range(cx + 1)])
    rotate([(p + 2) * nb for p in range(cx + 1)])
    settle(0, True)
    ghosts(0)
    weights(low, cx - high, 10)
    blocks(2 * low, cx - 2 * high, 5, average_body)

    for c in (x_f, x_e, c_e, c_f):
        recv(c)
    for side, has in enumerate((x_low, x_high)):
        @pl.when(has)
        def _():
            for i in range(2):
                p = (i - 2, cx + i)[side]
                ee[row_of(p, 0):row_of(p, cy), :] = xr_e[side, i]
                ee[row_of(p, -2):row_of(p, 0), :] = cr_e[side, 0, i]
                ee[row_of(p, cy):row_of(p, cy + 2), :] = cr_e[side, 1, i]
            p = (-1, cx)[side]
            for c in range(chans):
                ff[c, row_of(p, 0):row_of(p, cy), :] = xr_f[side, c, 0]
                ff[c, row_of(p, -1):row_of(p, 0), :] = cr_f[side, 0, c, 0]
                ff[c, row_of(p, cy):row_of(p, cy + 1), :] = cr_f[side, 1, c, 0]
            k = (0, (cx + 2) * nb)[side]
            pack_flat(list(range(k, k + 2 * nb + 1)))
            k = (nb, (cx + 2) * nb)[side]
            rotate(range(k, k + nb + 1))
    start(z_e[1])
    start(z_f[1])
    edges = ((low, -1, 1), (high, cx - 1, cx + 1))
    for has, a, b in edges:
        @pl.when(has == 1)
        def _():
            blocks(zero + a, b, (b - a) * nb + 1, count_body)
    beside = 2
    last = cx - 3 * high - beside
    deposit(3 * low, last)

    recv(z_e[1])
    recv(z_f[1])
    for j in range(beside):
        for b in range(nb - 1):
            deposit_body(last + j, b)
    settle(1, False)
    ghosts(1)
    for has, a, b in edges:
        @pl.when(has == 1)
        def _():
            k0 = (zero + a + 2) * nb
            for body in (inverse_body, weight_body):
                for j in range((b - a) * nb + 1):
                    body(k0 + j, PAD + 8 * (k0 + j))
            a2, b2 = (a, b + 1) if a < 0 else (a - 1, b)
            blocks(zero + a2, b2, 4, average_body)
            a3, b3 = (0, 3) if a < 0 else (cx - 3, cx)
            deposit(zero + a3, b3)
    for c in [x_f, x_e, y_e, y_f, c_e, c_f, z_e[1], z_f[1]]:
        sent(c)
    for to, _, copy in diagonal:
        pl.when(to)(lambda: copy.wait_send())


def per_device(n, conserved, volume_fraction, cut_mask, merge_code):
    fields, cx, cy, cz = conserved.shape[1:]
    chans = fields + 1
    flat = pl.cdiv(PAD + (cx + 6) * (cy + 8) + 64, 32) * 32
    f32, i32 = jnp.float32, jnp.int32
    V = pltpu.VMEM
    scratch = [
        V((flat, cz), i32), V((chans, flat, cz), f32), V((chans, flat, cz), f32), V((chans, flat, cz), f32),
        V((flat, cz), f32),
        V((chans, flat, cz), f32), V((chans, flat, cz), f32), V((chans, flat, cz), f32),
        V((fields, flat, cz), f32),
        V((cx, cy, cz), i32), V((cx, cy, cz), i32), V((chans, cx, cy, cz), f32),
        V((2, cx, 2, cz), i32), V((2, chans, cx, 1, cz), f32),
        V((2, cx, 2, cz), i32), V((2, chans, cx, 1, cz), f32),
        V((2, 2, cy, cz), i32), V((2, 2, cy, cz), i32), V((2, chans, 1, cy, cz), f32),
        V((2, 2, 2, 2, cz), i32), V((2, 2, chans, 1, 1, cz), f32),
        V((2, 2, 8, cz), i32), V((2, chans, 8, cz), f32),
        V((2, 2, 2, 8, cz), i32), V((2, 2, chans, 8, cz), f32),
        V((2, 2, 8, cz), i32), V((2, 2, 8, cz), f32), V((2, 2, 8, cz), i32), V((2, 2, 8, cz), f32),
        V((2, 8, cz), f32), V((2, chans, 8, cz), f32), V((2, fields, 8, cz), f32),
        V((2, 8, cz), f32), V((2, chans, 8, cz), f32), V((2, fields, 8, cz), f32),
        pltpu.SemaphoreType.DMA((4,)), pltpu.SemaphoreType.DMA((28,)), pltpu.SemaphoreType.DMA((28,)),
    ]
    return pl.pallas_call(
        functools.partial(kernel, n, (fields, cx, cy, cz)),
        out_shape=pltpu.VMEM(conserved.shape, f32),
        in_specs=[pl.BlockSpec(memory_space=pl.ANY)] * 4,
        out_specs=pl.BlockSpec(memory_space=pltpu.VMEM),
        scratch_shapes=scratch,
        compiler_params=pltpu.CompilerParams(
            collective_id=0, has_side_effects=True, vmem_limit_bytes=60 * 1024 * 1024),
        name="redistribute",
    )(conserved, volume_fraction, cut_mask, merge_code)


def solution(mesh):
    return jax.shard_map(
        functools.partial(per_device, mesh.shape["boxes"]),
        mesh=mesh,
        in_specs=(
            P("boxes", None, None, None, None),
            P("boxes", None, None, None),
            P("boxes", None, None, None),
            P("boxes", None, None, None),
        ),
        out_specs=P("boxes", None, None, None, None),
        check_vma=False,
    )
```

```python
import functools

import jax
import jax.numpy as jnp
from jax import lax
from jax.experimental import pallas as pl
from jax.experimental.pallas import tpu as pltpu
from jax.sharding import PartitionSpec as P

NBY = 4
NBZ = 4
MESH = pl.DeviceIdType.MESH
XP, XM, YP, YM, ZP, ZM = 1, 2, 4, 8, 16, 32
ONE, UP, DOWN = 10, 14, 18
NONE = 1 << ONE
PAD = 8
PAIRS = [(ax, ay) for ax in (0, 1, -1) for ay in (0, 1, -1)]


def flag(ax, ay, az=0):
    return (
        {1: XP, -1: XM, 0: 0}[ax] | {1: YP, -1: YM, 0: 0}[ay] | {1: ZP, -1: ZM, 0: 0}[az]
    )


def holds(e, bits):
    return (e & bits) == bits


def kernel(n, dims, u_ref, vf_ref, mask_ref, code_ref, out_ref, ee, ff, fp, fm, inv, w0, wp, wm, avg,
           raw_m, raw_c, raw_f, ys_e, ys_f, yr_e, yr_f, xs_e, xr_e, xr_f, cr_e, cr_f,
           zs_e, zs_f, zr_e, zr_f, ts_e, ts_f, tr_e, tr_f, two_c, two_w, two_d, inj_c, inj_w, inj_d, load_sem, send_sem, recv_sem):
    fields, cx, cy, cz = dims
    chans = fields + 1
    nb = cy // 8 + 1
    pitch = 8 * nb
    me = lax.axis_index("boxes")
    bx, by, bz = me // (NBY * NBZ), me // NBZ % NBY, me % NBZ
    axes = {
        "x": (NBY * NBZ, bx > 0, bx < n // (NBY * NBZ) - 1),
        "y": (NBZ, by > 0, by < NBY - 1),
        "z": (1, bz > 0, bz < NBZ - 1),
    }
    lane = lax.broadcasted_iota(jnp.int32, (8, cz), 1)
    sub = lax.broadcasted_iota(jnp.int32, (8, cz), 0)
    first, final = lane == 0, lane == cz - 1
    ends = jnp.logical_or(first, final)
    odd = (lane & 1) == 1
    slot = lane - nb * ((lane * (4096 // nb + 1)) >> 12)

    loads = [
        pltpu.make_async_copy(mask_ref.at[0], raw_m, load_sem.at[0]),
        pltpu.make_async_copy(code_ref.at[0], raw_c, load_sem.at[1]),
        pltpu.make_async_copy(u_ref.at[0], raw_f.at[1:chans], load_sem.at[2]),
        pltpu.make_async_copy(vf_ref.at[0], raw_f.at[0], load_sem.at[3]),
    ]
    for copy in loads:
        copy.start()

    barrier = pltpu.get_barrier_semaphore()
    total = jnp.int32(0)
    for stride, low, high in axes.values():
        for has, there in ((low, me - stride), (high, me + stride)):
            @pl.when(has)
            def _():
                pl.semaphore_signal(barrier, inc=1, device_id=(there,), device_id_type=MESH)
            total = total + has.astype(jnp.int32)
    for dy in (1, -1):
        for dz in (-1, 1):
            has = jnp.logical_and(axes["y"][1 + (dy == 1)], axes["z"][1 + (dz == 1)])
            @pl.when(has)
            def _():
                pl.semaphore_signal(barrier, inc=1, device_id=(me + NBZ * dy + dz,), device_id_type=MESH)
            total = total + has.astype(jnp.int32)
    def copies(axis, ident, up, down):
        stride = axes[axis][0]
        out = []
        for d, (pair, there) in enumerate(((up, me + stride), (down, me - stride))):
            out.append(pltpu.make_async_remote_copy(
                src_ref=pair[0], dst_ref=pair[1], send_sem=send_sem.at[2 * ident + d],
                recv_sem=recv_sem.at[2 * ident + d], device_id=(there,), device_id_type=MESH))
        return axis, out

    def start(c):
        axis, (up, down) = c
        _, low, high = axes[axis]
        pl.when(high)(lambda: up.start())
        pl.when(low)(lambda: down.start())

    def recv(c):
        axis, (up, down) = c
        _, low, high = axes[axis]
        pl.when(low)(lambda: up.wait_recv())
        pl.when(high)(lambda: down.wait_recv())

    def sent(c):
        axis, (up, down) = c
        _, low, high = axes[axis]
        pl.when(high)(lambda: up.wait_send())
        pl.when(low)(lambda: down.wait_send())

    x_f = copies("x", 0, (raw_f.at[:, cx - 1:cx], xr_f.at[0]), (raw_f.at[:, 0:1], xr_f.at[1]))
    x_e = copies("x", 1, (xs_e.at[1], xr_e.at[0]), (xs_e.at[0], xr_e.at[1]))
    y_e = copies("y", 2, (ys_e.at[0], yr_e.at[0]), (ys_e.at[1], yr_e.at[1]))
    y_f = copies("y", 3, (ys_f.at[0], yr_f.at[0]), (ys_f.at[1], yr_f.at[1]))
    c_e = copies("x", 4, (yr_e.at[:, cx - 2:cx], cr_e.at[0]), (yr_e.at[:, 0:2], cr_e.at[1]))
    c_f = copies("x", 5, (yr_f.at[:, :, cx - 1:cx], cr_f.at[0]), (yr_f.at[:, :, 0:1], cr_f.at[1]))
    z_e = [copies("z", 6 + t, (zs_e.at[1], zr_e.at[t, 0]), (zs_e.at[0], zr_e.at[t, 1])) for t in (0, 1)]
    z_f = [copies("z", 8 + t, (zs_f.at[1], zr_f.at[t, 0]), (zs_f.at[0], zr_f.at[t, 1])) for t in (0, 1)]

    loads[0].wait()
    loads[1].wait()

    diagonal = []
    for d, dy in enumerate((1, -1)):
        for side, dz in enumerate((-1, 1)):
            to = jnp.logical_and(axes["y"][1 + (dy == 1)], axes["z"][1 + (dz == 1)])
            frm = jnp.logical_and(axes["y"][1 + (dy == -1)], axes["z"][1 + (dz == -1)])
            for ts, tr in ((ts_e, tr_e), (ts_f, tr_f)):
                at = 20 + len(diagonal)
                diagonal.append((to, frm, pltpu.make_async_remote_copy(
                    src_ref=ts.at[d, side], dst_ref=tr.at[d, 1 - side], send_sem=send_sem.at[at],
                    recv_sem=recv_sem.at[at], device_id=(me + NBZ * dy + dz,), device_id_type=MESH)))

    def row_of(p, y):
        return PAD + pitch * (p + 2) + 8 + y

    _, x_low, x_high = axes["x"]
    _, y_low, y_high = axes["y"]
    _, z_low, z_high = axes["z"]
    clear = lambda has, bits: jnp.where(has, 0, bits)
    row2 = lax.broadcasted_iota(jnp.int32, (cy, cz), 0)
    lane2 = lax.broadcasted_iota(jnp.int32, (cy, cz), 1)
    drop = (jnp.where(row2 == 0, clear(y_low, YM), 0) + jnp.where(row2 == cy - 1, clear(y_high, YP), 0)
            + jnp.where(lane2 == 0, clear(z_low, ZM + (1 << DOWN)), 0)
            + jnp.where(lane2 == cz - 1, clear(z_high, ZP + (1 << UP)), 0))
    keep = ~drop

    def encode(p, _):
        c = raw_c[p]
        cut = raw_m[p] == 1
        third = (c * 171) >> 9
        sz = c - 3 * third
        ninth = (third * 171) >> 9
        sy = third - 3 * ninth
        bit = lambda test, value: jnp.where(test, value, 0)
        e = (bit(ninth == 2, XP) + bit(ninth == 0, XM) + bit(sy == 2, YP) + bit(sy == 0, YM)
             + bit(sz == 2, ZP + (1 << UP)) + bit(sz == 0, ZM + (1 << DOWN)))
        off = jnp.where(p == 0, clear(x_low, XM), 0) + jnp.where(p == cx - 1, clear(x_high, XP), 0)
        ee[pl.ds(row_of(p, 0), cy), :] = (jnp.where(cut, e, 0) & keep & ~off) + NONE
        ys_e[0, p] = ee[pl.ds(row_of(p, cy - 2), 2), :]
        ys_e[1, p] = ee[pl.ds(row_of(p, 0), 2), :]
        return 0

    lax.fori_loop(0, cx, encode, 0)
    loads[2].wait()
    loads[3].wait()
    for c in range(chans):
        ys_f[0, c] = raw_f[c, :, cy - 1:cy, :]
        ys_f[1, c] = raw_f[c, :, 0:1, :]
    pl.semaphore_wait(barrier, total)
    start(y_e)
    start(y_f)

    def turn(v, amount):
        if isinstance(amount, int):
            return pltpu.roll(v, amount % cz, 1) if amount % cz else v
        return pltpu.roll(v, lax.rem(amount + cz, cz), 1)

    shifts = ((0, 1), (-1, -2))

    def pack(ks, e_of, f_of):
        at = [{d: lane == (k + d) % cz if isinstance(k, int) else lane == k + d for d in (-2, -1, 0, 1)} for k in ks]
        acc = {(side, j): zs_e[side, j] for side in (0, 1) for j in (0, 1)}
        for i, k in enumerate(ks):
            e = turn(e_of(i), k)
            for side, j in acc:
                acc[side, j] = jnp.where(at[i][shifts[side][j]], e, acc[side, j])
        for side, j in acc:
            zs_e[side, j] = acc[side, j]
        for c in range(chans):
            acc = [zs_f[side, c] for side in (0, 1)]
            for i, k in enumerate(ks):
                f = turn(f_of(i, c), k)
                acc = [jnp.where(at[i][shifts[side][0]], f, acc[side]) for side in (0, 1)]
            for side in (0, 1):
                zs_f[side, c] = acc[side]

    def settle(t, merge):
        for side, beside in enumerate((z_low, z_high)):
            at = []
            for has, rows_of in ((y_low, sub >= 4), (y_high, sub < 4)):
                both = jnp.full((8, cz), jnp.logical_and(has, beside).astype(jnp.int32), jnp.int32) == 1
                at.append(jnp.logical_and(jnp.logical_and(slot == 0, rows_of), both))
            for j in (0, 1):
                e = turn(zr_e[t, side, j], -shifts[1 - side][j])
                for i in (0, 1) if merge else ():
                    e = jnp.where(at[i], turn(tr_e[i, side], nb * i - j), e)
                zr_e[t, side, j] = e
            for c in range(chans):
                f = turn(zr_f[t, side, c], -shifts[1 - side][0])
                for i in (0, 1) if merge else ():
                    v = turn(tr_f[i, side], nb * i - c % 4)
                    f = jnp.where(at[i], v if c < 4 else pltpu.roll(v, 4, 0), f)
                zr_f[t, side, c] = f

    def pack_flat(ks):
        pack(ks, lambda i: ee[PAD + 8 * ks[i]:PAD + 8 * ks[i] + 8, :],
             lambda i, c: ff[c, PAD + 8 * ks[i]:PAD + 8 * ks[i] + 8, :])

    zs_e[...] = jnp.full(zs_e.shape, NONE, jnp.int32)
    zs_f[...] = jnp.zeros(zs_f.shape, jnp.float32)
    group = 4 if cx % 4 == 0 else 1

    def pack_own(group, places):
        def step(i, _):
            ks, where = [], []
            for j in range(group):
                p = i * group + j
                for c in range(chans):
                    for b in places:
                        ff[c, pl.ds(row_of(p, 8 * b), 8), :] = raw_f[c, p, 8 * b:8 * b + 8, :]
                for b in places:
                    ks.append((p + 2) * nb + 1 + b)
                    where.append((p, b))
            pack(ks, lambda i: ee[pl.ds(PAD + 8 * ks[i], 8), :],
                 lambda i, c: raw_f[c, where[i][0], 8 * where[i][1]:8 * where[i][1] + 8, :])
            return 0

        lax.fori_loop(0, cx // group, step, 0)

    pack_own(8 if cx % 8 == 0 else 1, (0, nb - 2))
    for d, source, direct in ((0, nb - 1, sub >= 4), (1, 1, sub < 4)):
        for side in (0, 1):
            back = [shift + source for shift in shifts[side]]
            ts_e[d, side] = jnp.where(slot == 0, turn(zs_e[side, 0], -back[0]), turn(zs_e[side, 1], 1 - back[1]))
            line = [None, None]
            for c in range(chans):
                v = turn(zs_f[side, c], c % 4 - back[0])
                line[c // 4] = v if c % 4 == 0 else jnp.where(slot == c % 4, v, line[c // 4])
            ts_f[d, side] = jnp.where(direct, line[0], pltpu.roll(line[1], 4, 0))
    for to, _, copy in diagonal:
        pl.when(to)(lambda: copy.start())
    pack_own(8 if cx % 8 == 0 else 1, range(1, nb - 2))
    start(z_e[0])
    start(z_f[0])
    for i in range(2):
        xs_e[0, i] = ee[row_of(i, 0):row_of(i, cy), :]
        xs_e[1, i] = ee[row_of(cx - 2 + i, 0):row_of(cx - 2 + i, cy), :]
    start(x_f)
    start(x_e)

    @pl.when(jnp.logical_not(x_low))
    def _():
        a, b = PAD, row_of(-1, cy + 2)
        ee[a:b, :] = jnp.full((b - a, cz), NONE, jnp.int32)

    @pl.when(jnp.logical_not(x_high))
    def _():
        a, b = row_of(cx, -2), row_of(cx + 1, cy + 8)
        ee[a:b, :] = jnp.full((b - a, cz), NONE, jnp.int32)

    for side, has in enumerate((y_low, y_high)):
        @pl.when(jnp.logical_not(has))
        def _():
            yr_e[side] = jnp.full(yr_e.shape[1:], NONE, jnp.int32)
            yr_f[side] = jnp.zeros(yr_f.shape[1:], jnp.float32)
    for side, has in enumerate((z_low, z_high)):
        @pl.when(jnp.logical_not(has))
        def _():
            for t in (0, 1):
                zr_e[t, side] = jnp.full(zr_e.shape[2:], NONE, jnp.int32)
                zr_f[t, side] = jnp.zeros(zr_f.shape[2:], jnp.float32)

    def rotate(ks):
        for k in ks:
            r = PAD + 8 * k
            for c in range(chans):
                v = ff[c, pl.ds(r, 8), :]
                fp[c, pl.ds(r, 8), :] = pltpu.roll(v, cz - 1, 1)
                fm[c, pl.ds(r, 8), :] = pltpu.roll(v, 1, 1)

    def rotate_own(i, _):
        rotate([(i * group + j + 2) * nb + 1 + b for j in range(group) for b in range(nb - 1)])
        return 0

    lax.fori_loop(0, cx // group, rotate_own, 0)

    zero = me // n
    low, high = x_low.astype(jnp.int32), x_high.astype(jnp.int32)

    def blocks(p0, p1, chunk, body):
        k0 = (p0 + 2) * nb
        steps = ((p1 - p0) * nb + chunk) // chunk

        def step(i, _):
            for j in range(chunk):
                k = k0 + i * chunk + j
                body(k, PAD + 8 * k)
            return 0

        lax.fori_loop(0, steps, step, 0)

    def rows(ref, lead, r):
        return ref[lead + (pl.ds(r, 8), slice(None))]

    def count_body(k, r):
        acc = rows(ee, (), r)
        for ax, ay in PAIRS[1:]:
            e = rows(ee, (), r - pitch * ax - ay)
            acc = acc + jnp.where(holds(e, flag(ax, ay)), e, 0)
        here = (acc >> ONE) & 15
        here = here + pltpu.roll((acc >> UP) & 15, 1, 1) + pltpu.roll((acc >> DOWN) & 15, cz - 1, 1)
        inv[pl.ds(r, 8), :] = 1.0 / here.astype(jnp.float32)

    def plane_blocks(p0, p1, places, body):
        def step(i, _):
            for j in (0, 1):
                for b in places:
                    k = (p0 + 2 * i + j + 2) * nb + b
                    body(k, PAD + 8 * k)
            return 0

        lax.fori_loop(0, (p1 - p0 + 1) // 2, step, 0)

    plane_blocks(low, cx - high, range(2, nb - 1), count_body)
    recv(y_e)
    start(c_e)
    for p in range(cx):
        ee[row_of(p, -2):row_of(p, 0), :] = yr_e[0, p]
        ee[row_of(p, cy):row_of(p, cy + 2), :] = yr_e[1, p]

    def edge(ref, lead, k):
        return turn(ref[(lax.rem(k, 2),) + lead], cz - k)

    def inverse_body(k, r):
        inv[pl.ds(r, 8), :] = jnp.where(ends, edge(inj_c, (), k), rows(inv, (), r))

    def weight_body(k, r):
        i = rows(inv, (), r)
        up, down = pltpu.roll(i, cz - 1, 1), pltpu.roll(i, 1, 1)
        w, up, down = i * rows(ff, (0,), r), up * rows(fp, (0,), r), down * rows(fm, (0,), r)
        for c in range(chans):
            g = edge(inj_w, (c,), k)
            v, a, b = (w, up, down) if c == 0 else (
                w * rows(ff, (c,), r), up * rows(fp, (c,), r), down * rows(fm, (c,), r))
            w0[c, pl.ds(r, 8), :] = v
            wp[c, pl.ds(r, 8), :] = v + jnp.where(final, g, a)
            wm[c, pl.ds(r, 8), :] = v + jnp.where(first, g, b)

    def weights(p0, p1, chunk):
        k0 = (p0 + 2) * nb
        steps = ((p1 - p0) * nb + chunk) // chunk

        def step(i, _):
            before = k0 + jnp.maximum(i - 1, 0) * chunk
            for j in range(chunk):
                weight_body(before + j, PAD + 8 * (before + j))
            for j in range(chunk):
                k = k0 + i * chunk + j
                inverse_body(k, PAD + 8 * k)
            return 0

        lax.fori_loop(0, steps + 1, step, 0)

    def average_body(k, r):
        e = rows(ee, (), r)
        m = {b: holds(e, b) for b in (XP, XM, YP, YM, ZP, ZM)}

        def along_z(c, q):
            return jnp.where(m[ZP], rows(wp, (c,), q), jnp.where(m[ZM], rows(wm, (c,), q), rows(w0, (c,), q)))

        def along_y(c, q):
            side = jnp.where(m[YP], along_z(c, q + 1), jnp.where(m[YM], along_z(c, q - 1), 0.0))
            return along_z(c, q) + side

        def whole(c):
            side = jnp.where(m[XP], along_y(c, r + pitch), jnp.where(m[XM], along_y(c, r - pitch), 0.0))
            return along_y(c, r) + side

        inverse = 1.0 / whole(0)
        for c in range(1, chans):
            avg[c - 1, pl.ds(r, 8), :] = whole(c) * inverse

    def deposit_body(p, b):
        k = (p + 2) * nb + 1 + b
        r = PAD + 8 * k
        acc = [[None] * 3 for _ in range(fields)]
        for ax, ay in PAIRS:
            s = r - pitch * ax - ay
            e = rows(ee, (), s)
            ms = [holds(e, flag(ax, ay, az)) for az in (0, 1, -1)]
            for f in range(fields):
                v = rows(avg, (f,), s)
                for i in range(3):
                    term = v if (ax, ay, i) == (0, 0, 0) else jnp.where(ms[i], v, 0.0)
                    acc[f][i] = term if acc[f][i] is None else acc[f][i] + term
        i = rows(inv, (), r)
        for f in range(fields):
            here, up, down = acc[f]
            g = edge(inj_d, (f,), k)
            here = here + jnp.where(first, g, pltpu.roll(up, 1, 1))
            here = here + jnp.where(final, g, pltpu.roll(down, cz - 1, 1))
            out_ref[0, f, p, 8 * b:8 * b + 8, :] = here * i

    def deposit(p0, p1):
        def plane(i, _):
            for b in range(nb - 1):
                deposit_body(p0 + i, b)
            return 0

        lax.fori_loop(0, p1 - p0, plane, 0)

    def shift_y(v, dy):
        if dy == 0:
            return v
        w = pltpu.roll(v, 7 if dy == 1 else 1, 0)
        return jnp.where(sub == (7 if dy == 1 else 0), turn(w, -dy), w)

    def shift_x(v, dx):
        return turn(v, -nb * dx) if dx else v

    def spread(t):
        lines = {ax: t[ax, 0] + shift_y(t[ax, 1], -1) + shift_y(t[ax, -1], 1) for ax in (0, 1, -1)}
        return lines[0] + shift_x(lines[1], -1) + shift_x(lines[-1], 1)

    def ghost(t, side):
        toward, away = (ZP, ZM) if side == 0 else (ZM, ZP)
        e0, e1 = (turn(zs_e[side, j], -shifts[side][j]) for j in (0, 1))
        g0, g1 = zr_e[t, side, 0], zr_e[t, side, 1]
        own = [turn(zs_f[side, c], -shifts[side][0]) for c in range(chans)]
        from_g0 = jnp.where(holds(g0, toward), 257, 1)
        from_e0 = jnp.where(holds(e0, away), 257, 256)
        found = {}
        for ax, ay in PAIRS:
            b = flag(ax, ay)
            found[ax, ay] = (jnp.where(holds(g1, b | toward), 1, 0) + jnp.where(holds(g0, b), from_g0, 0)
                             + jnp.where(holds(e0, b), from_e0, 0) + jnp.where(holds(e1, b | away), 256, 0))
        found = spread(found)
        i_ghost = 1.0 / (found & 255).astype(jnp.float32)
        i_own = 1.0 / (found >> 8).astype(jnp.float32)
        two_c[side] = i_own
        w_ghost, w_own = zr_f[t, side, 0] * i_ghost, own[0] * i_own
        m = {b: holds(g0, b) for b in (XP, XM, YP, YM)}
        mine = holds(g0, toward)
        inverse = None
        for c in range(chans):
            v = w_ghost if c == 0 else w_ghost * zr_f[t, side, c]
            two_w[side, c] = v
            v = v + (w_own if c == 0 else w_own * own[c])
            above, below = shift_y(v, 1), shift_y(v, -1)
            line = {dx: shift_x(v, dx) + jnp.where(m[YP], shift_x(above, dx), jnp.where(m[YM], shift_x(below, dx), 0.0))
                    for dx in (0, 1, -1)}
            whole = line[0] + jnp.where(m[XP], line[1], jnp.where(m[XM], line[-1], 0.0))
            if c == 0:
                inverse = 1.0 / whole
                continue
            a = jnp.where(mine, whole * inverse, 0.0)
            two_d[side, c - 1] = spread({
                (ax, ay): jnp.where(holds(g0, flag(ax, ay)), a, 0.0) if (ax, ay) != (0, 0) else a
                for ax, ay in PAIRS})

    def ghosts(t):
        for side in (0, 1):
            ghost(t, side)
        pairs = [(two_c, inj_c, ())] + [(two_w, inj_w, (c,)) for c in range(chans)]
        for two, inj, lead in pairs + [(two_d, inj_d, (f,)) for f in range(fields)]:
            below, above = two[(0,) + lead], turn(two[(1,) + lead], -1)
            inj[(0,) + lead] = jnp.where(odd, above, below)
            inj[(1,) + lead] = jnp.where(odd, below, above)

    plane_blocks(low, cx - high + 1, (0, 1, nb - 1), count_body)
    recv(y_f)
    start(c_f)
    for c in (z_e[0], z_f[0]):
        recv(c)
        sent(c)
    for _, frm, copy in diagonal:
        pl.when(frm)(lambda: copy.wait_recv())
    for p in range(cx):
        for c in range(chans):
            ff[c, row_of(p, -1):row_of(p, 0), :] = yr_f[0, c, p]
            ff[c, row_of(p, cy):row_of(p, cy + 1), :] = yr_f[1, c, p]
    pack_flat([(p + 2) * nb for p in range(cx + 1)])
    rotate([(p + 2) * nb for p in range(cx + 1)])
    settle(0, True)
    ghosts(0)
    weights(low, cx - high, 13)
    blocks(2 * low, cx - 2 * high, 5, average_body)

    for c in (x_f, x_e, c_e, c_f):
        recv(c)
    for side, has in enumerate((x_low, x_high)):
        @pl.when(has)
        def _():
            for i in range(2):
                p = (i - 2, cx + i)[side]
                ee[row_of(p, 0):row_of(p, cy), :] = xr_e[side, i]
                ee[row_of(p, -2):row_of(p, 0), :] = cr_e[side, 0, i]
                ee[row_of(p, cy):row_of(p, cy + 2), :] = cr_e[side, 1, i]
            p = (-1, cx)[side]
            for c in range(chans):
                ff[c, row_of(p, 0):row_of(p, cy), :] = xr_f[side, c, 0]
                ff[c, row_of(p, -1):row_of(p, 0), :] = cr_f[side, 0, c, 0]
                ff[c, row_of(p, cy):row_of(p, cy + 1), :] = cr_f[side, 1, c, 0]
            k = (0, (cx + 2) * nb)[side]
            pack_flat(list(range(k, k + 2 * nb + 1)))
            k = (nb, (cx + 2) * nb)[side]
            rotate(range(k, k + nb + 1))
    start(z_e[1])
    start(z_f[1])
    edges = ((low, -1, 1), (high, cx - 1, cx + 1))
    for has, a, b in edges:
        @pl.when(has == 1)
        def _():
            blocks(zero + a, b, (b - a) * nb + 1, count_body)
    beside = 2
    last = cx - 3 * high - beside
    deposit(3 * low, last)

    recv(z_e[1])
    recv(z_f[1])
    for j in range(beside):
        for b in range(nb - 1):
            deposit_body(last + j, b)
    settle(1, False)
    ghosts(1)
    for has, a, b in edges:
        @pl.when(has == 1)
        def _():
            k0 = (zero + a + 2) * nb
            for body in (inverse_body, weight_body):
                for j in range((b - a) * nb + 1):
                    body(k0 + j, PAD + 8 * (k0 + j))
            a2, b2 = (a, b + 1) if a < 0 else (a - 1, b)
            blocks(zero + a2, b2, 4, average_body)
            a3, b3 = (0, 3) if a < 0 else (cx - 3, cx)
            deposit(zero + a3, b3)
    for c in [x_f, x_e, y_e, y_f, c_e, c_f, z_e[1], z_f[1]]:
        sent(c)
    for to, _, copy in diagonal:
        pl.when(to)(lambda: copy.wait_send())


def per_device(n, conserved, volume_fraction, cut_mask, merge_code):
    fields, cx, cy, cz = conserved.shape[1:]
    chans = fields + 1
    flat = pl.cdiv(PAD + (cx + 6) * (cy + 8) + 64, 32) * 32
    f32, i32 = jnp.float32, jnp.int32
    V = pltpu.VMEM
    scratch = [
        V((flat, cz), i32), V((chans, flat, cz), f32), V((chans, flat, cz), f32), V((chans, flat, cz), f32),
        V((flat, cz), f32),
        V((chans, flat, cz), f32), V((chans, flat, cz), f32), V((chans, flat, cz), f32),
        V((fields, flat, cz), f32),
        V((cx, cy, cz), i32), V((cx, cy, cz), i32), V((chans, cx, cy, cz), f32),
        V((2, cx, 2, cz), i32), V((2, chans, cx, 1, cz), f32),
        V((2, cx, 2, cz), i32), V((2, chans, cx, 1, cz), f32),
        V((2, 2, cy, cz), i32), V((2, 2, cy, cz), i32), V((2, chans, 1, cy, cz), f32),
        V((2, 2, 2, 2, cz), i32), V((2, 2, chans, 1, 1, cz), f32),
        V((2, 2, 8, cz), i32), V((2, chans, 8, cz), f32),
        V((2, 2, 2, 8, cz), i32), V((2, 2, chans, 8, cz), f32),
        V((2, 2, 8, cz), i32), V((2, 2, 8, cz), f32), V((2, 2, 8, cz), i32), V((2, 2, 8, cz), f32),
        V((2, 8, cz), f32), V((2, chans, 8, cz), f32), V((2, fields, 8, cz), f32),
        V((2, 8, cz), f32), V((2, chans, 8, cz), f32), V((2, fields, 8, cz), f32),
        pltpu.SemaphoreType.DMA((4,)), pltpu.SemaphoreType.DMA((28,)), pltpu.SemaphoreType.DMA((28,)),
    ]
    return pl.pallas_call(
        functools.partial(kernel, n, (fields, cx, cy, cz)),
        out_shape=pltpu.VMEM(conserved.shape, f32),
        in_specs=[pl.BlockSpec(memory_space=pl.ANY)] * 4,
        out_specs=pl.BlockSpec(memory_space=pltpu.VMEM),
        scratch_shapes=scratch,
        compiler_params=pltpu.CompilerParams(
            collective_id=0, has_side_effects=True, vmem_limit_bytes=60 * 1024 * 1024),
        name="redistribute",
    )(conserved, volume_fraction, cut_mask, merge_code)


def solution(mesh):
    return jax.shard_map(
        functools.partial(per_device, mesh.shape["boxes"]),
        mesh=mesh,
        in_specs=(
            P("boxes", None, None, None, None),
            P("boxes", None, None, None),
            P("boxes", None, None, None),
            P("boxes", None, None, None),
        ),
        out_specs=P("boxes", None, None, None, None),
        check_vma=False,
    )
```
